16 devices in a mesh: dp: 4 (over z, y), tp: 4 (over x, core).
Axes of the slice: x: 2, y: 2, z: 2, core: 2. Of those that a mesh axis runs over, the one named last changes fastest.
Arguments:
- x: bfloat16 [4, 128, 2560], P('dp', 'tp'), parts along dimension 0
- ln1_gamma: float32 [2560], replicated
- ln1_beta: float32 [2560], replicated
- w_qkv: bfloat16 [2560, 32, 3, 80], P(None, 'tp')
- b_qkv: float32 [32, 3, 80], P('tp')
- w_out: bfloat16 [2560, 2560], P('tp')
- b_out: float32 [2560], replicated
- ln2_gamma: float32 [2560], replicated
- ln2_beta: float32 [2560], replicated
- w_up: bfloat16 [2560, 10240], P(None, 'tp')
- b_up: float32 [10240], P('tp')
- w_down: bfloat16 [10240, 2560], P('tp')
- b_down: float32 [2560], replicated
- grad_y: bfloat16 [4, 128, 2560], P('dp', 'tp'), parts along dimension 0
Outputs:
- output 1: bfloat16 [4, 128, 2560], P('dp', 'tp'), parts along dimension 0
- output 2: bfloat16 [4, 128, 2560], P('dp', 'tp'), parts along dimension 0
- output 3: float32 [10240], P('dp'), parts along dimension 0
- output 4: float32 [10240], P('dp'), parts along dimension 0
- output 5: bfloat16 [10240, 32, 3, 80], P('dp', 'tp'), parts along dimension 0
- output 6: float32 [128, 3, 80], P(('dp', 'tp')), parts along dimension 0
- output 7: bfloat16 [10240, 2560], P(('dp', 'tp')), parts along dimension 0
- output 8: float32 [10240], P('dp'), parts along dimension 0
- output 9: float32 [10240], P('dp'), parts along dimension 0
- output 10: float32 [10240], P('dp'), parts along dimension 0
- output 11: bfloat16 [10240, 10240], P('dp', 'tp'), parts along dimension 0
- output 12: float32 [40960], P(('dp', 'tp')), parts along dimension 0
- output 13: bfloat16 [40960, 2560], P(('dp', 'tp')), parts along dimension 0
- output 14: float32 [10240], P('dp'), parts along dimension 0
There are 4 independent parts. The reference program is written for one: setup_inputs(seed, part) draws one part's arguments, and reference() takes and returns one part's arrays. A program takes and returns all parts, laid end to end along the dimension named above; an argument that names none is the same for every part.
All inputs are finite; a program needn't handle non-finite values.
Results may differ from the reference program's by a relative error of at most 0.0174444.
Values are sent between devices in bfloat16 or wider.
A program may use at most 1 GiB of HBM per device.

```python
import math
import jax
import jax.numpy as jnp
from jax import lax

BATCH = 1
SEQ = 128
D = 2560
HEADS = 32
HEAD = 80
FF = 10240
EPS = 1e-5
MASK_VALUE = -1e30


def alibi_slopes(n_heads):
    closest = 2 ** int(math.floor(math.log2(n_heads)))
    base_ratio = 2.0 ** (-8.0 / closest)
    extra_ratio = 2.0 ** (-4.0 / closest)
    remaining = min(closest, n_heads - closest)
    slopes = [base_ratio ** (i + 1) for i in range(closest)]
    slopes = slopes + [extra_ratio ** (2 * i + 1) for i in range(remaining)]
    return jnp.array(slopes, dtype=jnp.float32)


def layer_norm(values, ln_gain, ln_bias):
    row_mean = jnp.mean(values, axis=-1, keepdims=True)
    centered = values - row_mean
    variance = jnp.mean(centered * centered, axis=-1, keepdims=True)
    return centered * lax.rsqrt(variance + EPS) * ln_gain + ln_bias


def layer_forward(x, ln1_gamma, ln1_beta, w_qkv, b_qkv, w_out, b_out, ln2_gamma, ln2_beta, w_up, b_up, w_down, b_down):
    positions = jnp.arange(SEQ)
    causal = positions[None, :] <= positions[:, None]
    key_pos = positions.astype(jnp.float32)
    x_f = x.astype(jnp.float32)
    h_norm = layer_norm(x_f, ln1_gamma, ln1_beta).astype(jnp.bfloat16)
    qkv_vals = (jnp.einsum('bsd,dhte->bshte', h_norm.astype(jnp.float32), w_qkv.astype(jnp.float32)) + b_qkv).astype(jnp.bfloat16)
    per_head = jnp.moveaxis(qkv_vals, 2, 0)

    def head_attention(operands):
        head_qkv, head_slope = operands
        q_one = head_qkv[:, :, 0].astype(jnp.float32)
        k_one = head_qkv[:, :, 1].astype(jnp.float32)
        v_one = head_qkv[:, :, 2].astype(jnp.float32)
        scores = jnp.einsum('bie,bje->bij', q_one, k_one) * (HEAD ** -0.5) + head_slope * key_pos
        scores = jnp.where(causal, scores, MASK_VALUE)
        prob_bf = jax.nn.softmax(scores, axis=-1).astype(jnp.bfloat16)
        return jnp.einsum('bij,bje->bie', prob_bf.astype(jnp.float32), v_one).astype(jnp.bfloat16)

    context = lax.map(jax.checkpoint(head_attention), (per_head, alibi_slopes(HEADS)))
    context_flat = jnp.moveaxis(context, 0, 2).reshape(BATCH, SEQ, D)
    attn_out = jnp.einsum('bsc,cd->bsd', context_flat.astype(jnp.float32), w_out.astype(jnp.float32)).astype(jnp.bfloat16)
    x_mid = x_f + attn_out.astype(jnp.float32) + b_out
    g_norm = layer_norm(x_mid, ln2_gamma, ln2_beta).astype(jnp.bfloat16)
    pre_act = jnp.einsum('bsd,df->bsf', g_norm.astype(jnp.float32), w_up.astype(jnp.float32)) + b_up
    activated = jax.nn.gelu(pre_act, approximate=True).astype(jnp.bfloat16)
    mlp_out = jnp.einsum('bsf,fd->bsd', activated.astype(jnp.float32), w_down.astype(jnp.float32)).astype(jnp.bfloat16)
    return (x_mid + mlp_out.astype(jnp.float32) + b_down).astype(jnp.bfloat16)


def setup_inputs(seed: int = 0, part: int = 0) -> dict:
    key_list = jax.random.split(jax.random.key(seed), 14)

    def normal(rng_key, out_shape, std_dev):
        return std_dev * jax.random.normal(rng_key, out_shape, jnp.float32)

    return {
        'x': normal(jax.random.fold_in(key_list[0], part), (BATCH, SEQ, D), 1.0).astype(jnp.bfloat16),
        'ln1_gamma': 1.0 + normal(key_list[1], (D,), 0.2),
        'ln1_beta': normal(key_list[2], (D,), 0.2),
        'w_qkv': normal(key_list[3], (D, HEADS, 3, HEAD), D ** -0.5).astype(jnp.bfloat16),
        'b_qkv': normal(key_list[4], (HEADS, 3, HEAD), 0.5),
        'w_out': normal(key_list[5], (D, D), D ** -0.5).astype(jnp.bfloat16),
        'b_out': normal(key_list[6], (D,), 0.5),
        'ln2_gamma': 1.0 + normal(key_list[7], (D,), 0.2),
        'ln2_beta': normal(key_list[8], (D,), 0.2),
        'w_up': normal(key_list[9], (D, FF), D ** -0.5).astype(jnp.bfloat16),
        'b_up': normal(key_list[10], (FF,), 0.5),
        'w_down': normal(key_list[11], (FF, D), FF ** -0.5).astype(jnp.bfloat16),
        'b_down': normal(key_list[12], (D,), 0.5),
        'grad_y': normal(jax.random.fold_in(key_list[13], part), (BATCH, SEQ, D), 1.0).astype(jnp.bfloat16),
    }


def reference(x, ln1_gamma, ln1_beta, w_qkv, b_qkv, w_out, b_out, ln2_gamma, ln2_beta, w_up, b_up, w_down, b_down, grad_y):
    y, pullback = jax.vjp(layer_forward, x, ln1_gamma, ln1_beta, w_qkv, b_qkv, w_out, b_out, ln2_gamma, ln2_beta, w_up, b_up, w_down, b_down)
    (grad_x, grad_ln1_gamma, grad_ln1_beta, grad_w_qkv, grad_b_qkv, grad_w_out, grad_b_out,
     grad_ln2_gamma, grad_ln2_beta, grad_w_up, grad_b_up, grad_w_down, grad_b_down) = pullback(grad_y)
    return (y, grad_x, grad_ln1_gamma, grad_ln1_beta, grad_w_qkv, grad_b_qkv, grad_w_out, grad_b_out,
            grad_ln2_gamma, grad_ln2_beta, grad_w_up, grad_b_up, grad_w_down, grad_b_down)
```

```python
import jax
import jax.numpy as jnp
from jax import lax
from jax.experimental import pallas as pl
from jax.experimental.pallas import tpu as pltpu
from jax.sharding import PartitionSpec as P

EPS = 1e-5
MASK_VALUE = -1e30
MESH = pl.DeviceIdType.MESH
F32 = jnp.float32
BF16 = jnp.bfloat16

D = 2560
SEQ = 128
TP = 4
ROWS = SEQ // TP
NH = 8
HD = 80
QKV = NH * 3 * HD
CTX = NH * HD
FF = 2560
AGC = 4
AGW = D // AGC
RSC = 5
RSW = D // RSC
OFF_G, OFF_ACT, OFF_QKV, OFF_O = 0, D, D + FF, D + FF + QKV
LROWS = D + FF + QKV + CTX
SLOPES = [2.0 ** (-(h + 1) / 4.0) for h in range(NH)]
NT = (((1,), (1,)), ((), ()))
NN = (((1,), (0,)), ((), ()))
TN = (((0,), (0,)), ((), ()))


def dot(a, b, dims):
    return lax.dot_general(a, b, dims, preferred_element_type=F32)


def ln_stats(v):
    mean = jnp.mean(v, axis=-1, keepdims=True)
    cen = v - mean
    var = jnp.mean(cen * cen, axis=-1, keepdims=True)
    rstd = lax.rsqrt(var + EPS)
    return cen * rstd, rstd


def ln_grad(dy, xhat, rstd, gain):
    dxh = dy * gain
    m1 = jnp.mean(dxh, axis=-1, keepdims=True)
    m2 = jnp.mean(dxh * xhat, axis=-1, keepdims=True)
    return rstd * (dxh - m1 - xhat * m2)


def block_kernel(x_hbm, gy_hbm, wq_hbm, wo_hbm, wu_hbm, wd_hbm, g1_hbm, b1_hbm, bq_hbm, bo_hbm, g2_hbm, b2_hbm, bu_hbm,
                 bd_hbm, y_hbm, gx_hbm, vec_hbm, gbu_hbm, l_hbm, r_hbm,
                 wq, wo, wu, wd, xv, gyv, g1, b1, bq, bo, g2, b2, bu, bd,
                 rbuf, lbuf, gbuf, qkvt, dqkv, ctx, dctxt, prob, act, dact, x1, dmid, outb, gbu, va, vb, vo,
                 pb, rx1, sb, rx2, wsem, lsem, osem, ssem, rsem):
    me = lax.axis_index('tp')
    ax = lax.div(me, 2)
    ak = lax.rem(me, 2)
    partner = 2 * ax + (1 - ak)
    cross = 2 * (1 - ax) + ak
    diag = 2 * (1 - ax) + (1 - ak)

    def rows(i):
        return pl.ds(pl.multiple_of(i * ROWS, ROWS), ROWS)

    sent = []
    count = {'s': 0, 'r': 0}

    def alloc(kind, n=1):
        base = count[kind]
        count[kind] += n
        return base

    def remote(src, dst, si, ri, dev):
        return pltpu.make_async_remote_copy(src_ref=src, dst_ref=dst, send_sem=ssem.at[si], recv_sem=rsem.at[ri],
                                            device_id={'tp': dev}, device_id_type=MESH)

    small = [(x_hbm, xv), (g1_hbm, g1), (b1_hbm, b1), (bq_hbm, bq), (bo_hbm, bo), (g2_hbm, g2), (b2_hbm, b2),
             (bu_hbm, bu), (bd_hbm, bd)]
    loads = [pltpu.make_async_copy(s, d, lsem.at[i]) for i, (s, d) in enumerate(small)]
    for c in loads:
        c.start()
    gm = rbuf.at[1]
    gy_full = pltpu.make_async_copy(gy_hbm, gm.at[rows(me)], lsem.at[len(small)])
    gy_full.start()
    gy_loc = pltpu.make_async_copy(gy_hbm, gyv, lsem.at[len(small) + 1])
    gy_loc.start()
    wcopies = [pltpu.make_async_copy(s, d, wsem.at[i])
               for i, (s, d) in enumerate([(wq_hbm, wq), (wo_hbm, wo), (wd_hbm, wd), (wu_hbm, wu)])]
    wcopies[0].start()
    wcopies[1].start()

    bar = pltpu.get_barrier_semaphore()
    for dev in (partner, cross, diag):
        pl.semaphore_signal(bar, inc=1, device_id={'tp': dev}, device_id_type=MESH)

    class Gather:
        def __init__(self, full):
            self.full = full
            self.s = alloc('s', 2 * AGC + 1)
            self.r = alloc('r', 2 * AGC + 1)

        def chunk(self, dev, c):
            return self.full.at[rows(dev), pl.ds(c * AGW, AGW)]

        def cross_copy(self, dev, c):
            ref = self.chunk(dev, c)
            return remote(ref, ref, self.s + c, self.r + c, cross)

        def fwd_copy(self, dev, c):
            ref = self.chunk(dev, c)
            return remote(ref, ref, self.s + AGC + c, self.r + AGC + c, partner)

        def own_copy(self, dev):
            ref = self.full.at[rows(dev)]
            return remote(ref, ref, self.s + 2 * AGC, self.r + 2 * AGC, partner)

        def start(self):
            for c in range(AGC):
                self.cross_copy(me, c).start()
            self.own_copy(me).start()

        def forward(self, c):
            self.cross_copy(cross, c).wait_recv()
            self.fwd_copy(cross, c).start()

        def finish(self):
            self.own_copy(partner).wait_recv()
            for c in range(AGC):
                self.fwd_copy(diag, c).wait_recv()

        def drain(self):
            for c in range(AGC):
                self.cross_copy(me, c).wait_send()
                self.fwd_copy(cross, c).wait_send()
            self.own_copy(me).wait_send()

    class Scatter:
        def __init__(self, i):
            self.p, self.x1, self.sb, self.x2 = pb.at[i], rx1.at[i], sb.at[i], rx2.at[i]
            self.s = alloc('s', 2 * RSC)
            self.r = alloc('r', 2 * RSC)

        def cols(self, n):
            if isinstance(n, int):
                return pl.ds(n * RSW, RSW)
            return pl.ds(pl.multiple_of(n * RSW, RSW), RSW)

        def pair(self, n):
            return remote(self.p.at[:, 1 - ak, :, self.cols(n)], self.x1.at[:, :, self.cols(n)], self.s + n, self.r + n, partner)

        def over(self, n):
            return remote(self.sb.at[:, self.cols(n)], self.x2.at[:, self.cols(n)], self.s + RSC + n, self.r + RSC + n, cross)

        def produce(self, n, val):
            self.p[:, :, :, self.cols(n)] = val.astype(BF16).reshape(2, 2, ROWS, RSW)
            self.pair(n).start()

        def relay(self, n):
            self.pair(n).wait_recv()
            self.sb[:, self.cols(n)] = (self.p[1 - ax, ak, :, self.cols(n)].astype(F32)
                                        + self.x1[1 - ax, :, self.cols(n)].astype(F32)).astype(BF16)
            self.over(n).start()

        def run(self, fn, relay=True):
            def body(n, carry):
                self.produce(n, fn(self.cols(n)))
                if relay:
                    @pl.when(n > 0)
                    def _():
                        self.relay(n - 1)
                return carry
            lax.fori_loop(0, RSC, body, 0)

        def relay_all(self):
            def body(n, carry):
                self.relay(n)
                return carry
            lax.fori_loop(0, RSC, body, 0)

        def result(self):
            for n in range(RSC):
                self.over(n).wait_recv()
            return (self.p[ax, ak].astype(F32) + self.x1[ax].astype(F32) + self.x2[...].astype(F32))

        def drain(self):
            for n in range(RSC):
                self.pair(n).wait_send()
                self.over(n).wait_send()

    gat_h, gat_m, gat_g, gat_a = Gather(rbuf.at[2]), Gather(rbuf.at[1]), Gather(gbuf), Gather(rbuf.at[3])
    sc_a, sc_g, sc_y, sc_h = Scatter(0), Scatter(1), Scatter(2), Scatter(3)
    outs = []

    def emit(src, dst):
        c = pltpu.make_async_copy(src, dst, osem.at[len(outs)])
        c.start()
        outs.append(c)

    for c in loads:
        c.wait()
    xhat1, _ = ln_stats(xv[...].astype(F32))
    rbuf[2, rows(me), :] = (xhat1 * g1[...] + b1[...]).astype(BF16)
    gy_full.wait()
    pl.semaphore_wait(bar, 3)
    gat_h.start()
    wcopies[2].start()
    wcopies[3].start()
    for c in range(AGC):
        gat_h.forward(c)
    wcopies[0].wait()
    gat_h.finish()
    gat_m.start()
    emit(rbuf.at[2], r_hbm.at[2])

    QC = 384

    def qkv_body(n, carry):
        r0 = pl.multiple_of(n * QC, QC)
        v = dot(rbuf[2], wq[pl.ds(r0, QC), :], NT) + bq[:, pl.ds(r0, QC)]
        qkvt[pl.ds(r0, QC), :] = v.astype(BF16).T
        return carry
    lax.fori_loop(0, QKV // QC, qkv_body, 0)

    scale = HD ** -0.5
    jpos = lax.broadcasted_iota(jnp.int32, (SEQ, SEQ), 0)
    ipos = lax.broadcasted_iota(jnp.int32, (SEQ, SEQ), 1)
    causal = jpos <= ipos
    jf = jpos.astype(F32)
    base = jnp.where(me == 0, 1.0, jnp.where(me == 1, 0.25, jnp.where(me == 2, 0.0625, 0.015625))).astype(F32)

    def head(h, t):
        r0 = h * 3 * HD + t * HD
        return qkvt[r0:r0 + HD, :]

    for h in range(NH):
        s = dot(head(h, 1), head(h, 0), TN) * scale + (base * SLOPES[h]) * jf
        s = jnp.where(causal, s, MASK_VALUE)
        e = jnp.exp(s - jnp.max(s, axis=0, keepdims=True))
        p = e * (1.0 / jnp.sum(e, axis=0, keepdims=True))
        prob[h] = p
        lbuf[OFF_O + h * HD:OFF_O + (h + 1) * HD, :] = dot(head(h, 2), p.astype(BF16), NN).astype(BF16)
    for t in range(CTX // 128):
        ctx[:, t * 128:(t + 1) * 128] = lbuf[OFF_O + t * 128:OFF_O + (t + 1) * 128, :].T

    wcopies[1].wait()
    sc_a.run(lambda cols: dot(ctx[...], wo[:, cols], NN))
    sc_a.relay(RSC - 1)

    for c in range(AGC):
        gat_m.forward(c)
    wcopies[2].wait()
    gat_m.finish()
    emit(rbuf.at[1], r_hbm.at[1])
    FC = 256

    def dact_body(n, carry):
        f0 = pl.multiple_of(n * FC, FC)
        dact[:, pl.ds(f0, FC)] = dot(rbuf[1], wd[pl.ds(f0, FC), :], NT).astype(BF16)
        return carry
    lax.fori_loop(0, 5, dact_body, 0)

    a = sc_a.result().astype(BF16).astype(F32)
    x1[...] = xv[...].astype(F32) + a + bo[...]
    xhat2, rstd2 = ln_stats(x1[...])
    gbuf[rows(me), :] = (xhat2 * g2[...] + b2[...]).astype(BF16)
    gat_g.start()
    lax.fori_loop(5, 10, dact_body, 0)
    for c in range(AGC):
        gat_g.forward(c)
    wcopies[3].wait()
    gat_g.finish()

    UC = 512
    k0 = 0.7978845608028654
    k1 = 0.044715

    def up_body(n, carry):
        f0 = pl.multiple_of(n * UC, UC)
        cols = pl.ds(f0, UC)
        v = dot(gbuf[...], wu[:, cols], NN) + bu[:, cols]
        v2 = v * v
        t = jnp.tanh(k0 * (v + k1 * (v2 * v)))
        hp = 0.5 * (1.0 + t)
        act[:, cols] = (v * hp).astype(BF16)
        dg = hp + (0.5 * k0) * v * (1.0 - t * t) * (1.0 + (3.0 * k1) * v2)
        dpre = dact[:, cols].astype(F32) * dg
        gbu[:, cols] = jnp.sum(dpre, axis=0, keepdims=True)
        rbuf[0, :, cols] = dpre.astype(BF16)
        return carry
    lax.fori_loop(0, FF // UC, up_body, 0)
    emit(rbuf.at[0], r_hbm.at[0])
    emit(gbu, gbu_hbm)

    def dg_chunk(cols):
        return dot(rbuf[0], wu[cols, :], NT)
    sc_g.run(dg_chunk)
    sc_g.relay(RSC - 1)

    sc_y.run(lambda cols: dot(act[...], wd[:, cols], NN), relay=False)

    def tr_body(src, off):
        def body(n, carry):
            r0 = pl.multiple_of(n * 128, 128)
            lbuf[pl.ds(off + r0, 128), :] = src[:, pl.ds(r0, 128)].T
            return carry
        return body
    lax.fori_loop(0, FF // 128, tr_body(act, OFF_ACT), 0)

    gy_loc.wait()
    dgl = sc_g.result().astype(BF16).astype(F32)
    xhat2, rstd2 = ln_stats(x1[...])
    gyf = gyv[...].astype(F32)
    dm = gyf + ln_grad(dgl, xhat2, rstd2, g2[...])
    dmid[...] = dm
    rbuf[3, rows(me), :] = dm.astype(BF16)
    gat_a.start()
    va[me, 0:1, :] = jnp.sum(dgl * xhat2, axis=0, keepdims=True)
    va[me, 1:2, :] = jnp.sum(dgl, axis=0, keepdims=True)
    va[me, 2:3, :] = jnp.sum(dm, axis=0, keepdims=True)
    va[me, 3:4, :] = jnp.sum(gyf, axis=0, keepdims=True)
    lax.fori_loop(0, D // 128, tr_body(gbuf, OFF_G), 0)
    for c in range(AGC):
        gat_a.forward(c)
    gat_a.finish()
    emit(rbuf.at[3], r_hbm.at[3])

    sva, rva = alloc('s', 3), alloc('r', 3)

    def vec_copy(buf, s, r, i, owner, dev):
        return remote(buf.at[owner], buf.at[owner], s + i, r + i, dev)
    peers = (partner, cross, diag)
    sc_y.relay_all()
    for i, dev in enumerate(peers):
        vec_copy(va, sva, rva, i, me, dev).start()

    ctx[...] = dot(rbuf[3], wo[...], NT).astype(BF16)
    for t in range(CTX // 128):
        dctxt[t * 128:(t + 1) * 128, :] = ctx[:, t * 128:(t + 1) * 128].T

    for h in range(NH):
        dot_h = dctxt[h * HD:(h + 1) * HD, :]
        p = prob[h]
        dp = dot(head(h, 2), dot_h, TN).astype(BF16).astype(F32)
        ds = (p * (dp - jnp.sum(dp * p, axis=0, keepdims=True))).astype(BF16)
        r0 = OFF_QKV + h * 3 * HD
        lbuf[r0:r0 + HD, :] = (dot(head(h, 1), ds, NN) * scale).astype(BF16)
        lbuf[r0 + HD:r0 + 2 * HD, :] = (dot(head(h, 0), ds, NT) * scale).astype(BF16)
        lbuf[r0 + 2 * HD:r0 + 3 * HD, :] = dot(dot_h, p.astype(BF16), NT).astype(BF16)
    for t in range(QKV // 128):
        dqkv[:, t * 128:(t + 1) * 128] = lbuf[OFF_QKV + t * 128:OFF_QKV + (t + 1) * 128, :].T
    emit(lbuf, l_hbm)

    sc_h.run(lambda cols: dot(dqkv[...], wq[:, cols], NN))
    sc_h.relay(RSC - 1)

    m = sc_y.result().astype(BF16).astype(F32)
    outb[0] = (x1[...] + m + bd[...]).astype(BF16)
    emit(outb.at[0], y_hbm)
    vec_copy(va, sva, rva, 0, partner, partner).wait_recv()
    vec_copy(va, sva, rva, 1, cross, cross).wait_recv()
    vec_copy(va, sva, rva, 2, diag, diag).wait_recv()
    tot = (va[0] + va[1]) + (va[2] + va[3])
    for i in range(4):
        vo[i] = tot[i:i + 1]

    dhl = sc_h.result().astype(BF16).astype(F32)
    xhat1, rstd1 = ln_stats(xv[...].astype(F32))
    vb[me, 0:1, :] = jnp.sum(dhl * xhat1, axis=0, keepdims=True)
    vb[me, 1:2, :] = jnp.sum(dhl, axis=0, keepdims=True)
    svb, rvb = alloc('s', 3), alloc('r', 3)
    for i, dev in enumerate(peers):
        vec_copy(vb, svb, rvb, i, me, dev).start()
    outb[1] = (dmid[...] + ln_grad(dhl, xhat1, rstd1, g1[...])).astype(BF16)
    emit(outb.at[1], gx_hbm)
    vec_copy(vb, svb, rvb, 0, partner, partner).wait_recv()
    vec_copy(vb, svb, rvb, 1, cross, cross).wait_recv()
    vec_copy(vb, svb, rvb, 2, diag, diag).wait_recv()
    tot = (vb[0] + vb[1]) + (vb[2] + vb[3])
    for i in range(2):
        vo[4 + i] = tot[i:i + 1]
    emit(vo, vec_hbm)

    for g in (gat_h, gat_m, gat_g, gat_a):
        g.drain()
    for s in (sc_a, sc_g, sc_y, sc_h):
        s.drain()
    for i, dev in enumerate(peers):
        vec_copy(va, sva, rva, i, me, dev).wait_send()
        vec_copy(vb, svb, rvb, i, me, dev).wait_send()
    for c in outs:
        c.wait()


GR = 320
SECTIONS = ((OFF_ACT, FF, 1), (OFF_G, D, 0), (OFF_QKV, QKV, 2), (OFF_O, CTX, 3))


def grad_kernel(y_in, gx_in, vec_in, gbu_in, l_hbm, r_hbm, y_out, gx_out, v0, v1, v2, v3, v4, v5, gbq_hbm, gbu_out,
                dwq, dwo, dwu, dwd, lv, rv, st, yv, gxv, vv, gv, gbq, isem, ssem, psem, osem):
    loads = []
    for i, (off, n, r) in enumerate(SECTIONS):
        cl = pltpu.make_async_copy(l_hbm.at[pl.ds(off, n)], lv.at[pl.ds(off, n)], isem.at[2 * i])
        cr = pltpu.make_async_copy(r_hbm.at[r], rv.at[r], isem.at[2 * i + 1])
        cl.start()
        cr.start()
        loads.append((cl, cr))
    passes = [(y_in, yv, y_out), (gx_in, gxv, gx_out), (gbu_in, gv, gbu_out)]
    pin = [pltpu.make_async_copy(a, b, psem.at[i]) for i, (a, b, _) in enumerate(passes)]
    pin.append(pltpu.make_async_copy(vec_in, vv, psem.at[3]))
    for c in pin:
        c.start()
    douts = (dwd, dwu, dwq, dwo)
    step = 0
    for i, (off, n, r) in enumerate(SECTIONS):
        loads[i][0].wait()
        loads[i][1].wait()
        dst = douts[i]

        def body(m, carry, off=off, r=r, dst=dst, step=step):
            slot = lax.rem(m + step, 3)
            out = pltpu.make_async_copy(st.at[slot], dst.at[pl.ds(pl.multiple_of(m * GR, GR), GR)], ssem.at[slot])

            @pl.when(m + step >= 3)
            def _():
                out.wait()
            st[slot] = dot(lv[pl.ds(pl.multiple_of(off + m * GR, 64), GR), :], rv[r], NN).astype(BF16)
            out.start()
            return carry
        lax.fori_loop(0, n // GR, body, 0)
        step += n // GR
    for c in pin:
        c.wait()
    done = []
    for i, (_, b, o) in enumerate(passes):
        done.append(pltpu.make_async_copy(b, o, osem.at[i]))
    for i, o in enumerate((v0, v1, v2, v3, v4, v5)):
        done.append(pltpu.make_async_copy(vv.at[i], o, osem.at[3 + i]))
    ones = jnp.ones((16, SEQ), BF16)
    for h in range(NH):
        for t in range(3):
            r0 = OFF_QKV + h * 3 * HD + t * HD
            gbq[t, h:h + 1, :] = dot(ones, lv[r0:r0 + HD, :], NT)[0:1]
    done.append(pltpu.make_async_copy(gbq, gbq_hbm, osem.at[9]))
    for c in done:
        c.start()
    for i in range(3):
        pltpu.make_async_copy(st.at[i], dwo.at[pl.ds(0, GR)], ssem.at[i]).wait()
    for c in done:
        c.wait()


def solution(mesh):
    def local_step(x, ln1_gamma, ln1_beta, w_qkv, b_qkv, w_out, b_out, ln2_gamma, ln2_beta, w_up, b_up, w_down, b_down, grad_y):
        row = lambda v: v.reshape(1, -1)
        wqt = jnp.transpose(w_qkv, (1, 2, 3, 0)).reshape(QKV, D)
        any_spec = pl.BlockSpec(memory_space=pl.ANY)
        sds = jax.ShapeDtypeStruct
        y, gx, vec, gbu, lmat, rmat = pl.pallas_call(
            block_kernel,
            name='block',
            out_shape=(sds((ROWS, D), BF16), sds((ROWS, D), BF16), sds((6, 1, D), F32), sds((1, FF), F32),
                       sds((LROWS, SEQ), BF16), sds((4, SEQ, D), BF16)),
            in_specs=[any_spec] * 14,
            out_specs=(any_spec,) * 6,
            scratch_shapes=[
                pltpu.VMEM((QKV, D), BF16), pltpu.VMEM((CTX, D), BF16), pltpu.VMEM((D, FF), BF16), pltpu.VMEM((FF, D), BF16),
                pltpu.VMEM((ROWS, D), BF16), pltpu.VMEM((ROWS, D), BF16),
                pltpu.VMEM((1, D), F32), pltpu.VMEM((1, D), F32), pltpu.VMEM((1, QKV), F32), pltpu.VMEM((1, D), F32),
                pltpu.VMEM((1, D), F32), pltpu.VMEM((1, D), F32), pltpu.VMEM((1, FF), F32), pltpu.VMEM((1, D), F32),
                pltpu.VMEM((4, SEQ, D), BF16), pltpu.VMEM((LROWS, SEQ), BF16), pltpu.VMEM((SEQ, D), BF16),
                pltpu.VMEM((QKV, SEQ), BF16), pltpu.VMEM((SEQ, QKV), BF16), pltpu.VMEM((SEQ, CTX), BF16),
                pltpu.VMEM((CTX, SEQ), BF16), pltpu.VMEM((NH, SEQ, SEQ), F32),
                pltpu.VMEM((SEQ, FF), BF16), pltpu.VMEM((SEQ, FF), BF16),
                pltpu.VMEM((ROWS, D), F32), pltpu.VMEM((ROWS, D), F32), pltpu.VMEM((2, ROWS, D), BF16),
                pltpu.VMEM((1, FF), F32),
                pltpu.VMEM((TP, 4, D), F32), pltpu.VMEM((TP, 2, D), F32), pltpu.VMEM((6, 1, D), F32),
                pltpu.VMEM((4, 2, 2, ROWS, D), BF16), pltpu.VMEM((4, 2, ROWS, D), BF16),
                pltpu.VMEM((4, ROWS, D), BF16), pltpu.VMEM((4, ROWS, D), BF16),
                pltpu.SemaphoreType.DMA((4,)), pltpu.SemaphoreType.DMA((11,)), pltpu.SemaphoreType.DMA((10,)),
                pltpu.SemaphoreType.DMA((82,)), pltpu.SemaphoreType.DMA((82,)),
            ],
            compiler_params=pltpu.CompilerParams(collective_id=0, has_side_effects=True, vmem_limit_bytes=66_000_000),
            cost_estimate=pl.CostEstimate(flops=10_000_000_000, bytes_accessed=45_000_000, transcendentals=1_000_000),
        )(x[0], grad_y[0], wqt, w_out, w_up, w_down, row(ln1_gamma), row(ln1_beta), b_qkv.reshape(1, QKV), row(b_out),
          row(ln2_gamma), row(ln2_beta), row(b_up), row(b_down))
        y, gx, v0, v1, v2, v3, v4, v5, gbq, gbu, dwq, dwo, dwu, dwd = pl.pallas_call(
            grad_kernel,
            name='weight_grads',
            out_shape=(sds((ROWS, D), BF16), sds((ROWS, D), BF16)) + (sds((1, D), F32),) * 6 + (
                sds((3, NH, HD), F32), sds((1, FF), F32), sds((QKV, D), BF16), sds((CTX, D), BF16), sds((D, FF), BF16), sds((FF, D), BF16)),
            in_specs=[any_spec] * 6,
            out_specs=(any_spec,) * 14,
            scratch_shapes=[
                pltpu.VMEM((LROWS, SEQ), BF16), pltpu.VMEM((4, SEQ, D), BF16), pltpu.VMEM((3, GR, D), BF16),
                pltpu.VMEM((ROWS, D), BF16), pltpu.VMEM((ROWS, D), BF16), pltpu.VMEM((6, 1, D), F32), pltpu.VMEM((1, FF), F32),
                pltpu.VMEM((3, NH, HD), F32),
                pltpu.SemaphoreType.DMA((8,)), pltpu.SemaphoreType.DMA((3,)), pltpu.SemaphoreType.DMA((4,)), pltpu.SemaphoreType.DMA((10,)),
            ],
            compiler_params=pltpu.CompilerParams(vmem_limit_bytes=40_000_000),
            cost_estimate=pl.CostEstimate(flops=5_000_000_000, bytes_accessed=44_000_000, transcendentals=0),
        )(y, gx, vec, gbu, lmat, rmat)
        g_wqkv = jnp.transpose(dwq.reshape(NH, 3, HD, D), (3, 0, 1, 2))
        vecs = [v.reshape(D) for v in (v0, v1, v2, v3, v4, v5)]
        g_ln2g, g_ln2b, g_bo, g_bd, g_ln1g, g_ln1b = vecs
        return (y[None], gx[None], g_ln1g, g_ln1b, g_wqkv, jnp.transpose(gbq, (1, 0, 2)), dwo, g_bo,
                g_ln2g, g_ln2b, dwu, gbu.reshape(FF), dwd, g_bd)

    row_spec = P('dp', 'tp', None)
    in_specs = (row_spec, P(), P(), P(None, 'tp', None, None), P('tp', None, None), P('tp', None), P(), P(), P(),
                P(None, 'tp'), P('tp'), P('tp', None), P(), row_spec)
    out_specs = (row_spec, row_spec, P('dp'), P('dp'), P('dp', 'tp', None, None), P(('dp', 'tp'), None, None),
                 P(('dp', 'tp'), None), P('dp'), P('dp'), P('dp'), P('dp', 'tp'), P(('dp', 'tp')), P(('dp', 'tp'), None), P('dp'))
    return jax.shard_map(local_step, mesh=mesh, in_specs=in_specs, out_specs=out_specs, check_vma=False)
```

```python
import jax
import jax.numpy as jnp
from jax import lax
from jax.experimental import pallas as pl
from jax.experimental.pallas import tpu as pltpu
from jax.sharding import PartitionSpec as P

EPS = 1e-5
MASK_VALUE = -1e30
MESH = pl.DeviceIdType.MESH
F32 = jnp.float32
BF16 = jnp.bfloat16

D = 2560
SEQ = 128
TP = 4
ROWS = SEQ // TP
NH = 8
HD = 80
QKV = NH * 3 * HD
CTX = NH * HD
FF = 2560
AGC = 4
NSEM = 64
AGW = D // AGC
RSC = 5
RSW = D // RSC
OFF_G, OFF_ACT, OFF_QKV, OFF_O = 0, D, D + FF, D + FF + QKV
LROWS = D + FF + QKV + CTX
SLOPES = [2.0 ** (-(h + 1) / 4.0) for h in range(NH)]
NT = (((1,), (1,)), ((), ()))
NN = (((1,), (0,)), ((), ()))
TN = (((0,), (0,)), ((), ()))


def dot(a, b, dims):
    return lax.dot_general(a, b, dims, preferred_element_type=F32)


def ln_stats(v):
    mean = jnp.mean(v, axis=-1, keepdims=True)
    cen = v - mean
    var = jnp.mean(cen * cen, axis=-1, keepdims=True)
    rstd = lax.rsqrt(var + EPS)
    return cen * rstd, rstd


def ln_grad(dy, xhat, rstd, gain):
    dxh = dy * gain
    m1 = jnp.mean(dxh, axis=-1, keepdims=True)
    m2 = jnp.mean(dxh * xhat, axis=-1, keepdims=True)
    return rstd * (dxh - m1 - xhat * m2)


def block_kernel(x_hbm, gy_hbm, wq_hbm, wo_hbm, wu_hbm, wd_hbm, g1_hbm, b1_hbm, bq_hbm, bo_hbm, g2_hbm, b2_hbm, bu_hbm,
                 bd_hbm, y_hbm, gx_hbm, vec_hbm, gbu_hbm, l_hbm, r_hbm,
                 wq, wo, wu, wd, xh, g1, b1, bqv, bq, bo, g2, b2, bu, bd,
                 rbuf, lbuf, gbuf, qkvt, dqkv, ctx, dctxt, prob, act, dact, x1, dmid, outb, gbu, va, vb, vo,
                 pb, rx1, sb, rx2, wsem, lsem, osem, ssem, rsem):
    me = lax.axis_index('tp')
    ax = lax.div(me, 2)
    ak = lax.rem(me, 2)
    partner = 2 * ax + (1 - ak)
    cross = 2 * (1 - ax) + ak
    diag = 2 * (1 - ax) + (1 - ak)
    peers = (partner, cross, diag)

    def rows(i):
        return pl.ds(pl.multiple_of(i * ROWS, ROWS), ROWS)

    def block_rows(b):
        return rows(2 * b + ak)

    count = {'s': 0, 'r': 0}

    def alloc(kind, n=1):
        base = count[kind]
        count[kind] += n
        return base

    def remote(src, dst, si, ri, dev):
        return pltpu.make_async_remote_copy(src_ref=src, dst_ref=dst, send_sem=ssem.at[si], recv_sem=rsem.at[ri],
                                            device_id={'tp': dev}, device_id_type=MESH)

    x_load = pltpu.make_async_copy(x_hbm, xh.at[ax], lsem.at[0])
    x_load.start()
    small = [(g1_hbm, g1.at[0]), (b1_hbm, b1.at[0]), (bq_hbm, bqv), (bo_hbm, bo.at[0]), (g2_hbm, g2.at[0]), (b2_hbm, b2.at[0]),
             (bu_hbm, bu.at[0]), (bd_hbm, bd.at[0])]
    loads = [pltpu.make_async_copy(s, d, lsem.at[1 + i]) for i, (s, d) in enumerate(small)]
    for c in loads:
        c.start()
    gy_load = pltpu.make_async_copy(gy_hbm, rbuf.at[1, rows(me)], lsem.at[1 + len(small)])
    gy_load.start()
    wcopies = [pltpu.make_async_copy(s, d, wsem.at[i])
               for i, (s, d) in enumerate([(wq_hbm, wq), (wo_hbm, wo), (wd_hbm, wd), (wu_hbm, wu)])]

    bar = pltpu.get_barrier_semaphore()
    for dev in peers:
        pl.semaphore_signal(bar, inc=1, device_id={'tp': dev}, device_id_type=MESH)
    wcopies[0].start()
    wcopies[1].start()

    class Gather:
        def __init__(self, full):
            self.full = full
            self.s = alloc('s', 2 * AGC + 1)
            self.r = alloc('r', 2 * AGC + 1)

        def chunk(self, dev, c):
            return self.full.at[rows(dev), pl.ds(c * AGW, AGW)]

        def cross_copy(self, dev, c):
            ref = self.chunk(dev, c)
            return remote(ref, ref, self.s + c, self.r + c, cross)

        def fwd_copy(self, dev, c):
            ref = self.chunk(dev, c)
            return remote(ref, ref, self.s + AGC + c, self.r + AGC + c, partner)

        def own_copy(self, dev):
            ref = self.full.at[rows(dev)]
            return remote(ref, ref, self.s + 2 * AGC, self.r + 2 * AGC, partner)

        def start(self):
            for c in range(AGC):
                self.cross_copy(me, c).start()
            self.own_copy(me).start()

        def forward(self, c):
            self.cross_copy(cross, c).wait_recv()
            self.fwd_copy(cross, c).start()

        def finish(self):
            self.own_copy(partner).wait_recv()
            for c in range(AGC):
                self.fwd_copy(diag, c).wait_recv()

        def drain(self):
            for c in range(AGC):
                self.cross_copy(me, c).wait_send()
                self.fwd_copy(cross, c).wait_send()
            self.own_copy(me).wait_send()

    class Share:
        def __init__(self, full):
            self.full = full
            self.s = alloc('s', 2)
            self.r = alloc('r', 2)

        def copy(self, b, k, i):
            ref = self.full.at[rows(2 * b + k)]
            return remote(ref, ref, self.s + i, self.r + i, partner)

        def send(self, b, i):
            self.copy(b, ak, i).start()

        def finish(self, b, i):
            self.copy(b, 1 - ak, i).wait_recv()

        def drain(self):
            self.copy(ax, ak, 0).wait_send()
            self.copy(1 - ax, ak, 1).wait_send()

    class Reduce:
        def __init__(self, i, both):
            self.p, self.x1, self.sb, self.x2 = pb.at[i], rx1.at[i], sb.at[i], rx2.at[i]
            self.both = both
            self.s = alloc('s', 2 * RSC)
            self.r = alloc('r', 2 * RSC)

        def cols(self, n):
            if isinstance(n, int):
                return pl.ds(n * RSW, RSW)
            return pl.ds(pl.multiple_of(n * RSW, RSW), RSW)

        def pair(self, n):
            return remote(self.p.at[:, 1 - ak, :, self.cols(n)], self.x1.at[:, :, self.cols(n)], self.s + n, self.r + n, partner)

        def over(self, n):
            if self.both:
                src, dst = self.sb.at[:, :, self.cols(n)], self.x2.at[:, :, self.cols(n)]
            else:
                src, dst = self.sb.at[0, :, self.cols(n)], self.x2.at[0, :, self.cols(n)]
            return remote(src, dst, self.s + RSC + n, self.r + RSC + n, cross)

        def produce(self, n, val):
            self.p[:, :, :, self.cols(n)] = val.astype(BF16).reshape(2, 2, ROWS, RSW)
            self.pair(n).start()

        def relay(self, n):
            self.pair(n).wait_recv()
            c = self.cols(n)
            if self.both:
                self.sb[:, :, c] = (self.p[:, ak, :, c].astype(F32) + self.x1[:, :, c].astype(F32)).astype(BF16)
            else:
                self.sb[0, :, c] = (self.p[1 - ax, ak, :, c].astype(F32) + self.x1[1 - ax, :, c].astype(F32)).astype(BF16)
            self.over(n).start()

        def run(self, fn, relay=True):
            def body(n, carry):
                self.produce(n, fn(self.cols(n)))
                if relay:
                    @pl.when(n > 0)
                    def _():
                        self.relay(n - 1)
                return carry
            lax.fori_loop(0, RSC, body, 0)
            if relay:
                self.relay(RSC - 1)

        def relay_all(self):
            def body(n, carry):
                self.relay(n)
                return carry
            lax.fori_loop(0, RSC, body, 0)

        def arrive(self):
            for n in range(RSC):
                self.over(n).wait_recv()

        def block(self, b):
            return (self.sb[b].astype(F32) + self.x2[b].astype(F32)).astype(BF16).astype(F32)

        def own(self):
            v = self.p[ax, ak].astype(F32) + self.x1[ax].astype(F32) + self.x2[0].astype(F32)
            return v.astype(BF16).astype(F32)

        def drain(self):
            for n in range(RSC):
                self.pair(n).wait_send()
                self.over(n).wait_send()

    gat_m = Gather(rbuf.at[1])
    sh_h, sh_g, sh_a = Share(rbuf.at[2]), Share(gbuf), Share(rbuf.at[3])
    sc_a, sc_g, sc_y, sc_h = Reduce(0, True), Reduce(1, True), Reduce(2, False), Reduce(3, False)
    blocks = ((ax, 0), (1 - ax, 1))
    outs = []

    def emit(src, dst):
        c = pltpu.make_async_copy(src, dst, osem.at[len(outs)])
        c.start()
        outs.append(c)

    sx, rx = alloc('s'), alloc('r')
    x_load.wait()
    pl.semaphore_wait(bar, 3)
    remote(xh.at[ax], xh.at[ax], sx, rx, cross).start()
    for c in loads:
        c.wait()
    bq[...] = jnp.concatenate([bqv[t, h:h + 1, :] for h in range(NH) for t in range(3)], axis=1)
    for b, i in blocks:
        if i == 1:
            remote(xh.at[1 - ax], xh.at[1 - ax], sx, rx, cross).wait_recv()
        xhat, _ = ln_stats(xh[b].astype(F32))
        rbuf[2, block_rows(b), :] = (xhat * g1[...] + b1[...]).astype(BF16)
        sh_h.send(b, i)
    gy_load.wait()
    gat_m.start()
    wcopies[2].start()
    wcopies[3].start()
    wcopies[0].wait()
    for b, i in blocks:
        sh_h.finish(b, i)
    emit(rbuf.at[2], r_hbm.at[2])

    QC = 384

    def qkv_body(n, carry):
        r0 = pl.multiple_of(n * QC, QC)
        v = dot(rbuf[2], wq[pl.ds(r0, QC), :], NT) + bq[:, pl.ds(r0, QC)]
        qkvt[pl.ds(r0, QC), :] = v.astype(BF16).T
        return carry
    lax.fori_loop(0, QKV // QC, qkv_body, 0)

    scale = HD ** -0.5
    jpos = lax.broadcasted_iota(jnp.int32, (SEQ, SEQ), 0)
    ipos = lax.broadcasted_iota(jnp.int32, (SEQ, SEQ), 1)
    causal = jpos <= ipos
    jf = jpos.astype(F32)
    base = jnp.where(me == 0, 1.0, jnp.where(me == 1, 0.25, jnp.where(me == 2, 0.0625, 0.015625))).astype(F32)

    def head(h, t):
        r0 = h * 3 * HD + t * HD
        return qkvt[r0:r0 + HD, :]

    for h in range(NH):
        s = dot(head(h, 1), head(h, 0), TN) * scale + (base * SLOPES[h]) * jf
        s = jnp.where(causal, s, MASK_VALUE)
        e = jnp.exp(s - jnp.max(s, axis=0, keepdims=True))
        p = e * (1.0 / jnp.sum(e, axis=0, keepdims=True))
        prob[h] = p
        lbuf[OFF_O + h * HD:OFF_O + (h + 1) * HD, :] = dot(head(h, 2), p.astype(BF16), NN).astype(BF16)
    for t in range(CTX // 128):
        ctx[:, t * 128:(t + 1) * 128] = lbuf[OFF_O + t * 128:OFF_O + (t + 1) * 128, :].T

    wcopies[1].wait()
    sc_a.run(lambda cols: dot(ctx[...], wo[:, cols], NN))

    for c in range(AGC):
        gat_m.forward(c)
    wcopies[2].wait()
    gat_m.finish()
    emit(rbuf.at[1], r_hbm.at[1])
    FC = 256

    def dact_body(n, carry):
        f0 = pl.multiple_of(n * FC, FC)
        dact[:, pl.ds(f0, FC)] = dot(rbuf[1], wd[pl.ds(f0, FC), :], NT).astype(BF16)
        return carry
    lax.fori_loop(0, FF // FC, dact_body, 0)

    sc_a.arrive()
    for b, i in blocks:
        x1[b] = xh[b].astype(F32) + sc_a.block(b) + bo[...]
        xhat, _ = ln_stats(x1[b])
        gbuf[block_rows(b), :] = (xhat * g2[...] + b2[...]).astype(BF16)
        sh_g.send(b, i)
    wcopies[3].wait()
    for b, i in blocks:
        sh_g.finish(b, i)

    UC = 512
    k0 = 0.7978845608028654
    k1 = 0.044715

    def up_body(n, carry):
        f0 = pl.multiple_of(n * UC, UC)
        cols = pl.ds(f0, UC)
        v = dot(gbuf[...], wu[:, cols], NN) + bu[:, cols]
        v2 = v * v
        t = jnp.tanh(k0 * (v + k1 * (v2 * v)))
        hp = 0.5 * (1.0 + t)
        act[:, cols] = (v * hp).astype(BF16)
        dg = hp + (0.5 * k0) * v * (1.0 - t * t) * (1.0 + (3.0 * k1) * v2)
        dpre = dact[:, cols].astype(F32) * dg
        gbu[:, cols] = jnp.sum(dpre, axis=0, keepdims=True)
        rbuf[0, :, cols] = dpre.astype(BF16)
        return carry
    lax.fori_loop(0, FF // UC, up_body, 0)
    emit(rbuf.at[0], r_hbm.at[0])
    emit(gbu, gbu_hbm)

    def dg_chunk(cols):
        return dot(rbuf[0], wu[cols, :], NT)
    sc_g.run(dg_chunk)

    sc_y.run(lambda cols: dot(act[...], wd[:, cols], NN))

    def tr_body(src, off):
        def body(n, carry):
            r0 = pl.multiple_of(n * 128, 128)
            lbuf[pl.ds(off + r0, 128), :] = src[:, pl.ds(r0, 128)].T
            return carry
        return body
    lax.fori_loop(0, FF // 128, tr_body(act, OFF_ACT), 0)
    lax.fori_loop(0, D // 128, tr_body(gbuf, OFF_G), 0)
    va[me, 3:4, :] = jnp.sum(rbuf[1, rows(me), :].astype(F32), axis=0, keepdims=True)

    sc_g.arrive()
    for b, i in blocks:
        dgl = sc_g.block(b)
        xhat, rstd = ln_stats(x1[b])
        dm = rbuf[1, block_rows(b), :].astype(F32) + ln_grad(dgl, xhat, rstd, g2[...])
        rbuf[3, block_rows(b), :] = dm.astype(BF16)
        sh_a.send(b, i)
        if i == 0:
            dmid[...] = dm
    va[me, 2:3, :] = jnp.sum(dmid[...], axis=0, keepdims=True)
    dgl = sc_g.block(ax)
    xhat, _ = ln_stats(x1[ax])
    va[me, 0:1, :] = jnp.sum(dgl * xhat, axis=0, keepdims=True)
    va[me, 1:2, :] = jnp.sum(dgl, axis=0, keepdims=True)

    sva, rva = alloc('s', 3), alloc('r', 3)

    def vec_copy(buf, s, r, i, owner, dev):
        return remote(buf.at[owner], buf.at[owner], s + i, r + i, dev)
    for i, dev in enumerate(peers):
        vec_copy(va, sva, rva, i, me, dev).start()
    for b, i in blocks:
        sh_a.finish(b, i)
    emit(rbuf.at[3], r_hbm.at[3])

    ctx[...] = dot(rbuf[3], wo[...], NT).astype(BF16)
    for t in range(CTX // 128):
        dctxt[t * 128:(t + 1) * 128, :] = ctx[:, t * 128:(t + 1) * 128].T

    for h in range(NH):
        dot_h = dctxt[h * HD:(h + 1) * HD, :]
        p = prob[h]
        dp = dot(head(h, 2), dot_h, TN).astype(BF16).astype(F32)
        ds = (p * (dp - jnp.sum(dp * p, axis=0, keepdims=True))).astype(BF16)
        r0 = OFF_QKV + h * 3 * HD
        lbuf[r0:r0 + HD, :] = (dot(head(h, 1), ds, NN) * scale).astype(BF16)
        lbuf[r0 + HD:r0 + 2 * HD, :] = (dot(head(h, 0), ds, NT) * scale).astype(BF16)
        lbuf[r0 + 2 * HD:r0 + 3 * HD, :] = dot(dot_h, p.astype(BF16), NT).astype(BF16)
    for t in range(QKV // 128):
        dqkv[:, t * 128:(t + 1) * 128] = lbuf[OFF_QKV + t * 128:OFF_QKV + (t + 1) * 128, :].T
    emit(lbuf, l_hbm)

    sc_h.run(lambda cols: dot(dqkv[...], wq[:, cols], NN))

    sc_y.arrive()
    outb[0] = (x1[ax] + sc_y.own() + bd[...]).astype(BF16)
    emit(outb.at[0], y_hbm)
    for i, dev in enumerate(peers):
        vec_copy(va, sva, rva, i, dev, dev).wait_recv()
    tot = (va[0] + va[1]) + (va[2] + va[3])
    for i in range(4):
        vo[i] = tot[i:i + 1]

    sc_h.arrive()
    dhl = sc_h.own()
    xhat1, rstd1 = ln_stats(xh[ax].astype(F32))
    vb[me, 0:1, :] = jnp.sum(dhl * xhat1, axis=0, keepdims=True)
    vb[me, 1:2, :] = jnp.sum(dhl, axis=0, keepdims=True)
    svb, rvb = alloc('s', 3), alloc('r', 3)
    for i, dev in enumerate(peers):
        vec_copy(vb, svb, rvb, i, me, dev).start()
    outb[1] = (dmid[...] + ln_grad(dhl, xhat1, rstd1, g1[...])).astype(BF16)
    emit(outb.at[1], gx_hbm)
    remote(xh.at[ax], xh.at[ax], sx, rx, cross).wait_send()
    gat_m.drain()
    for g in (sh_h, sh_g, sh_a, sc_a, sc_g, sc_y, sc_h):
        g.drain()
    for i, dev in enumerate(peers):
        vec_copy(va, sva, rva, i, me, dev).wait_send()
    for i, dev in enumerate(peers):
        vec_copy(vb, svb, rvb, i, dev, dev).wait_recv()
    tot = (vb[0] + vb[1]) + (vb[2] + vb[3])
    for i in range(2):
        vo[4 + i] = tot[i:i + 1]
    emit(vo, vec_hbm)
    for i, dev in enumerate(peers):
        vec_copy(vb, svb, rvb, i, me, dev).wait_send()
    for c in outs:
        c.wait()
    assert max(count.values()) <= NSEM


GR = 320
SECTIONS = ((OFF_ACT, FF, 1), (OFF_G, D, 0), (OFF_QKV, QKV, 2), (OFF_O, CTX, 3))


def grad_kernel(y_in, gx_in, vec_in, gbu_in, l_hbm, r_hbm, y_out, gx_out, v0, v1, v2, v3, v4, v5, gbq_hbm, gbu_out,
                dwq, dwo, dwu, dwd, lv, rv, st, yv, gxv, vv, gv, gbq, isem, ssem, psem, osem):
    loads = []
    for i, (off, n, r) in enumerate(SECTIONS):
        cl = pltpu.make_async_copy(l_hbm.at[pl.ds(off, n)], lv.at[pl.ds(off, n)], isem.at[2 * i])
        cr = pltpu.make_async_copy(r_hbm.at[r], rv.at[r], isem.at[2 * i + 1])
        cl.start()
        cr.start()
        loads.append((cl, cr))
    passes = [(y_in, yv, y_out), (gx_in, gxv, gx_out), (gbu_in, gv, gbu_out)]
    srcs = (yv, gxv, gv.at[0])
    pin = [pltpu.make_async_copy(a, b, psem.at[i]) for i, (a, b, _) in enumerate(passes)]
    pin.append(pltpu.make_async_copy(vec_in, vv, psem.at[3]))
    for c in pin:
        c.start()
    douts = (dwd, dwu, dwq, dwo)
    step = 0
    for i, (off, n, r) in enumerate(SECTIONS):
        loads[i][0].wait()
        loads[i][1].wait()
        dst = douts[i]

        def body(m, carry, off=off, r=r, dst=dst, step=step):
            slot = lax.rem(m + step, 4)
            out = pltpu.make_async_copy(st.at[slot], dst.at[pl.ds(pl.multiple_of(m * GR, GR), GR)], ssem.at[slot])

            @pl.when(m + step >= 4)
            def _():
                out.wait()
            st[slot] = dot(lv[pl.ds(pl.multiple_of(off + m * GR, 64), GR), :], rv[r], NN).astype(BF16)
            out.start()
            return carry
        lax.fori_loop(0, n // GR, body, 0)
        step += n // GR
    for c in pin:
        c.wait()
    done = []
    for i, (_, _, o) in enumerate(passes):
        done.append(pltpu.make_async_copy(srcs[i], o, osem.at[i]))
    for i, o in enumerate((v0, v1, v2, v3, v4, v5)):
        done.append(pltpu.make_async_copy(vv.at[i, 0], o, osem.at[3 + i]))
    ones = jnp.ones((16, SEQ), BF16)
    for h in range(NH):
        for t in range(3):
            r0 = OFF_QKV + h * 3 * HD + t * HD
            gbq[t, h:h + 1, :] = dot(ones, lv[r0:r0 + HD, :], NT)[0:1]
    done.append(pltpu.make_async_copy(gbq, gbq_hbm, osem.at[9]))
    for c in done:
        c.start()
    for i in range(4):
        pltpu.make_async_copy(st.at[i], dwo.at[pl.ds(0, GR)], ssem.at[i]).wait()
    for c in done:
        c.wait()


def solution(mesh):
    def local_step(x, ln1_gamma, ln1_beta, w_qkv, b_qkv, w_out, b_out, ln2_gamma, ln2_beta, w_up, b_up, w_down, b_down, grad_y):
        wqt = jnp.transpose(w_qkv, (1, 2, 3, 0)).reshape(QKV, D)
        any_spec = pl.BlockSpec(memory_space=pl.ANY)
        sds = jax.ShapeDtypeStruct
        y, gx, vec, gbu, lmat, rmat = pl.pallas_call(
            block_kernel,
            name='block',
            out_shape=(sds((ROWS, D), BF16), sds((ROWS, D), BF16), sds((6, 1, D), F32), sds((1, FF), F32),
                       sds((LROWS, SEQ), BF16), sds((4, SEQ, D), BF16)),
            in_specs=[any_spec] * 14,
            out_specs=(any_spec,) * 6,
            scratch_shapes=[
                pltpu.VMEM((QKV, D), BF16), pltpu.VMEM((CTX, D), BF16), pltpu.VMEM((D, FF), BF16), pltpu.VMEM((FF, D), BF16),
                pltpu.VMEM((2, ROWS, D), BF16),
                pltpu.VMEM((1, D), F32), pltpu.VMEM((1, D), F32), pltpu.VMEM((3, NH, HD), F32), pltpu.VMEM((1, QKV), F32),
                pltpu.VMEM((1, D), F32), pltpu.VMEM((1, D), F32), pltpu.VMEM((1, D), F32), pltpu.VMEM((1, FF), F32), pltpu.VMEM((1, D), F32),
                pltpu.VMEM((4, SEQ, D), BF16), pltpu.VMEM((LROWS, SEQ), BF16), pltpu.VMEM((SEQ, D), BF16),
                pltpu.VMEM((QKV, SEQ), BF16), pltpu.VMEM((SEQ, QKV), BF16), pltpu.VMEM((SEQ, CTX), BF16),
                pltpu.VMEM((CTX, SEQ), BF16), pltpu.VMEM((NH, SEQ, SEQ), F32),
                pltpu.VMEM((SEQ, FF), BF16), pltpu.VMEM((SEQ, FF), BF16),
                pltpu.VMEM((2, ROWS, D), F32), pltpu.VMEM((ROWS, D), F32), pltpu.VMEM((2, ROWS, D), BF16),
                pltpu.VMEM((1, FF), F32),
                pltpu.VMEM((TP, 4, D), F32), pltpu.VMEM((TP, 2, D), F32), pltpu.VMEM((6, 1, D), F32),
                pltpu.VMEM((4, 2, 2, ROWS, D), BF16), pltpu.VMEM((4, 2, ROWS, D), BF16),
                pltpu.VMEM((4, 2, ROWS, D), BF16), pltpu.VMEM((4, 2, ROWS, D), BF16),
                pltpu.SemaphoreType.DMA((4,)), pltpu.SemaphoreType.DMA((10,)), pltpu.SemaphoreType.DMA((9,)),
                pltpu.SemaphoreType.DMA((NSEM,)), pltpu.SemaphoreType.DMA((NSEM,)),
            ],
            compiler_params=pltpu.CompilerParams(collective_id=0, has_side_effects=True, vmem_limit_bytes=66_000_000),
            cost_estimate=pl.CostEstimate(flops=10_000_000_000, bytes_accessed=45_000_000, transcendentals=1_000_000),
        )(x[0], grad_y[0], wqt, w_out, w_up, w_down, ln1_gamma, ln1_beta, jnp.transpose(b_qkv, (1, 0, 2)), b_out,
          ln2_gamma, ln2_beta, b_up, b_down)
        y, gx, v0, v1, v2, v3, v4, v5, gbq, gbu, dwq, dwo, dwu, dwd = pl.pallas_call(
            grad_kernel,
            name='weight_grads',
            out_shape=(sds((ROWS, D), BF16), sds((ROWS, D), BF16)) + (sds((D,), F32),) * 6 + (
                sds((3, NH, HD), F32), sds((FF,), F32), sds((QKV, D), BF16), sds((CTX, D), BF16), sds((D, FF), BF16), sds((FF, D), BF16)),
            in_specs=[any_spec] * 6,
            out_specs=(any_spec,) * 14,
            scratch_shapes=[
                pltpu.VMEM((LROWS, SEQ), BF16), pltpu.VMEM((4, SEQ, D), BF16), pltpu.VMEM((4, GR, D), BF16),
                pltpu.VMEM((ROWS, D), BF16), pltpu.VMEM((ROWS, D), BF16), pltpu.VMEM((6, 1, D), F32), pltpu.VMEM((1, FF), F32),
                pltpu.VMEM((3, NH, HD), F32),
                pltpu.SemaphoreType.DMA((8,)), pltpu.SemaphoreType.DMA((4,)), pltpu.SemaphoreType.DMA((4,)), pltpu.SemaphoreType.DMA((10,)),
            ],
            compiler_params=pltpu.CompilerParams(vmem_limit_bytes=66_000_000),
            cost_estimate=pl.CostEstimate(flops=5_000_000_000, bytes_accessed=44_000_000, transcendentals=0),
        )(y, gx, vec, gbu, lmat, rmat)
        g_wqkv = jnp.transpose(dwq.reshape(NH, 3, HD, D), (3, 0, 1, 2))
        g_ln2g, g_ln2b, g_bo, g_bd, g_ln1g, g_ln1b = v0, v1, v2, v3, v4, v5
        return (y[None], gx[None], g_ln1g, g_ln1b, g_wqkv, jnp.transpose(gbq, (1, 0, 2)), dwo, g_bo,
                g_ln2g, g_ln2b, dwu, gbu, dwd, g_bd)

    row_spec = P('dp', 'tp', None)
    in_specs = (row_spec, P(), P(), P(None, 'tp', None, None), P('tp', None, None), P('tp', None), P(), P(), P(),
                P(None, 'tp'), P('tp'), P('tp', None), P(), row_spec)
    out_specs = (row_spec, row_spec, P('dp'), P('dp'), P('dp', 'tp', None, None), P(('dp', 'tp'), None, None),
                 P(('dp', 'tp'), None), P('dp'), P('dp'), P('dp'), P('dp', 'tp'), P(('dp', 'tp')), P(('dp', 'tp'), None), P('dp'))
    return jax.shard_map(local_step, mesh=mesh, in_specs=in_specs, out_specs=out_specs, check_vma=False)
```

```python
import jax
import jax.numpy as jnp
from jax import lax
from jax.experimental import pallas as pl
from jax.experimental.pallas import tpu as pltpu
from jax.sharding import PartitionSpec as P

EPS = 1e-5
MASK_VALUE = -1e30
MESH = pl.DeviceIdType.MESH
F32 = jnp.float32
BF16 = jnp.bfloat16

D = 2560
SEQ = 128
TP = 4
ROWS = SEQ // TP
NH = 8
HD = 80
QKV = NH * 3 * HD
CTX = NH * HD
FF = 2560
AGC = 4
NSEM = 64
AGW = D // AGC
RSC = 5
RSW = D // RSC
OFF_G, OFF_ACT, OFF_QKV, OFF_O = 0, D, D + FF, D + FF + QKV
LROWS = D + FF + QKV + CTX
SLOPES = [2.0 ** (-(h + 1) / 4.0) for h in range(NH)]
NT = (((1,), (1,)), ((), ()))
NN = (((1,), (0,)), ((), ()))
TN = (((0,), (0,)), ((), ()))


def dot(a, b, dims):
    return lax.dot_general(a, b, dims, preferred_element_type=F32)


def ln_stats(v):
    mean = jnp.mean(v, axis=-1, keepdims=True)
    cen = v - mean
    var = jnp.mean(cen * cen, axis=-1, keepdims=True)
    rstd = lax.rsqrt(var + EPS)
    return cen * rstd, rstd


def ln_grad(dy, xhat, rstd, gain):
    dxh = dy * gain
    m1 = jnp.mean(dxh, axis=-1, keepdims=True)
    m2 = jnp.mean(dxh * xhat, axis=-1, keepdims=True)
    return rstd * (dxh - m1 - xhat * m2)


def block_kernel(x_hbm, gy_hbm, wq_hbm, wo_hbm, wu_hbm, wd_hbm, g1_hbm, b1_hbm, bq_hbm, bo_hbm, g2_hbm, b2_hbm, bu_hbm,
                 bd_hbm, y_hbm, gx_hbm, vec_hbm, gbu_hbm, l_hbm, r_hbm,
                 wq, wo, wu, wd, xh, g1, b1, bqv, bq, bo, g2, b2, bu, bd,
                 rbuf, lbuf, gbuf, qkvt, dqkv, ctx, dctxt, prob, act, dact, x1, dmid, outb, gbu, va, vb, vo,
                 pb, rx1, sb, rx2, wsem, lsem, osem, ssem, rsem):
    me = lax.axis_index('tp')
    ax = lax.div(me, 2)
    ak = lax.rem(me, 2)
    partner = 2 * ax + (1 - ak)
    cross = 2 * (1 - ax) + ak
    diag = 2 * (1 - ax) + (1 - ak)
    peers = (partner, cross, diag)

    def rows(i):
        return pl.ds(pl.multiple_of(i * ROWS, ROWS), ROWS)

    def block_rows(b):
        return rows(2 * b + ak)

    count = {'s': 0, 'r': 0}

    def alloc(kind, n=1):
        base = count[kind]
        count[kind] += n
        return base

    def remote(src, dst, si, ri, dev):
        return pltpu.make_async_remote_copy(src_ref=src, dst_ref=dst, send_sem=ssem.at[si], recv_sem=rsem.at[ri],
                                            device_id={'tp': dev}, device_id_type=MESH)

    x_load = pltpu.make_async_copy(x_hbm, xh.at[ax], lsem.at[0])
    x_load.start()
    small = [(g1_hbm, g1.at[0]), (b1_hbm, b1.at[0]), (bq_hbm, bqv), (bo_hbm, bo.at[0]), (g2_hbm, g2.at[0]), (b2_hbm, b2.at[0]),
             (bu_hbm, bu.at[0]), (bd_hbm, bd.at[0])]
    loads = [pltpu.make_async_copy(s, d, lsem.at[1 + i]) for i, (s, d) in enumerate(small)]
    for c in loads:
        c.start()
    gy_load = pltpu.make_async_copy(gy_hbm, rbuf.at[1, rows(me)], lsem.at[1 + len(small)])
    gy_load.start()
    wcopies = [pltpu.make_async_copy(s, d, wsem.at[i])
               for i, (s, d) in enumerate([(wq_hbm, wq), (wo_hbm, wo), (wd_hbm, wd), (wu_hbm, wu)])]

    bar = pltpu.get_barrier_semaphore()
    for dev in peers:
        pl.semaphore_signal(bar, inc=1, device_id={'tp': dev}, device_id_type=MESH)
    wcopies[0].start()
    wcopies[1].start()

    class Gather:
        def __init__(self, full):
            self.full = full
            self.s = alloc('s', 2 * AGC + 1)
            self.r = alloc('r', 2 * AGC + 1)

        def chunk(self, dev, c):
            return self.full.at[rows(dev), pl.ds(c * AGW, AGW)]

        def cross_copy(self, dev, c):
            ref = self.chunk(dev, c)
            return remote(ref, ref, self.s + c, self.r + c, cross)

        def fwd_copy(self, dev, c):
            ref = self.chunk(dev, c)
            return remote(ref, ref, self.s + AGC + c, self.r + AGC + c, partner)

        def own_copy(self, dev):
            ref = self.full.at[rows(dev)]
            return remote(ref, ref, self.s + 2 * AGC, self.r + 2 * AGC, partner)

        def start(self):
            for c in range(AGC):
                self.cross_copy(me, c).start()
            self.own_copy(me).start()

        def forward(self, c):
            self.cross_copy(cross, c).wait_recv()
            self.fwd_copy(cross, c).start()

        def finish(self):
            self.own_copy(partner).wait_recv()
            for c in range(AGC):
                self.fwd_copy(diag, c).wait_recv()

        def drain(self):
            for c in range(AGC):
                self.cross_copy(me, c).wait_send()
                self.fwd_copy(cross, c).wait_send()
            self.own_copy(me).wait_send()

    class Share:
        def __init__(self, full):
            self.full = full
            self.s = alloc('s', 2)
            self.r = alloc('r', 2)

        def copy(self, b, k, i):
            ref = self.full.at[rows(2 * b + k)]
            return remote(ref, ref, self.s + i, self.r + i, partner)

        def send(self, b, i):
            self.copy(b, ak, i).start()

        def finish(self, b, i):
            self.copy(b, 1 - ak, i).wait_recv()

        def drain(self):
            self.copy(ax, ak, 0).wait_send()
            self.copy(1 - ax, ak, 1).wait_send()

    class Reduce:
        def __init__(self, i, both):
            self.p, self.x1, self.sb, self.x2 = pb.at[i], rx1.at[i], sb.at[i], rx2.at[i]
            self.both = both
            self.s = alloc('s', 2 * RSC)
            self.r = alloc('r', 2 * RSC)

        def cols(self, n):
            if isinstance(n, int):
                return pl.ds(n * RSW, RSW)
            return pl.ds(pl.multiple_of(n * RSW, RSW), RSW)

        def pair(self, n):
            return remote(self.p.at[:, 1 - ak, :, self.cols(n)], self.x1.at[:, :, self.cols(n)], self.s + n, self.r + n, partner)

        def over(self, n):
            if self.both:
                src, dst = self.sb.at[:, :, self.cols(n)], self.x2.at[:, :, self.cols(n)]
            else:
                src, dst = self.sb.at[0, :, self.cols(n)], self.x2.at[0, :, self.cols(n)]
            return remote(src, dst, self.s + RSC + n, self.r + RSC + n, cross)

        def produce(self, n, val):
            self.p[:, :, :, self.cols(n)] = val.astype(BF16).reshape(2, 2, ROWS, RSW)
            self.pair(n).start()

        def relay(self, n):
            self.pair(n).wait_recv()
            c = self.cols(n)
            if self.both:
                self.sb[:, :, c] = (self.p[:, ak, :, c].astype(F32) + self.x1[:, :, c].astype(F32)).astype(BF16)
            else:
                self.sb[0, :, c] = (self.p[1 - ax, ak, :, c].astype(F32) + self.x1[1 - ax, :, c].astype(F32)).astype(BF16)
            self.over(n).start()

        def run(self, fn, lag, also=None):
            def body(n, carry):
                self.produce(n, fn(self.cols(n)))
                if lag < RSC:
                    @pl.when(n >= lag)
                    def _():
                        self.relay(n - lag)
                if also is not None:
                    also(n)
                return carry
            lax.fori_loop(0, RSC, body, 0)

        def relay_from(self, first):
            def body(n, carry):
                self.relay(n)
                return carry
            lax.fori_loop(first, RSC, body, 0)

        def arrive(self):
            for n in range(RSC):
                self.over(n).wait_recv()

        def block(self, b):
            return (self.sb[b].astype(F32) + self.x2[b].astype(F32)).astype(BF16).astype(F32)

        def own(self):
            v = self.p[ax, ak].astype(F32) + self.x1[ax].astype(F32) + self.x2[0].astype(F32)
            return v.astype(BF16).astype(F32)

        def drain(self):
            for n in range(RSC):
                self.pair(n).wait_send()
                self.over(n).wait_send()

    gat_m = Gather(rbuf.at[1])
    sh_h, sh_g, sh_a = Share(rbuf.at[2]), Share(gbuf), Share(rbuf.at[3])
    sc_a, sc_g, sc_y, sc_h = Reduce(0, True), Reduce(1, True), Reduce(2, False), Reduce(3, False)
    blocks = ((ax, 0), (1 - ax, 1))
    outs = []

    def emit(src, dst):
        c = pltpu.make_async_copy(src, dst, osem.at[len(outs)])
        c.start()
        outs.append(c)

    sx, rx = alloc('s'), alloc('r')
    x_load.wait()
    pl.semaphore_wait(bar, 3)
    remote(xh.at[ax], xh.at[ax], sx, rx, cross).start()
    for c in loads:
        c.wait()
    bq[...] = jnp.concatenate([bqv[t, h:h + 1, :] for h in range(NH) for t in range(3)], axis=1)
    for b, i in blocks:
        if i == 1:
            remote(xh.at[1 - ax], xh.at[1 - ax], sx, rx, cross).wait_recv()
        xhat, _ = ln_stats(xh[b].astype(F32))
        rbuf[2, block_rows(b), :] = (xhat * g1[...] + b1[...]).astype(BF16)
        sh_h.send(b, i)
    gy_load.wait()
    gat_m.start()
    wcopies[2].start()
    wcopies[3].start()
    wcopies[0].wait()
    for b, i in blocks:
        sh_h.finish(b, i)
    emit(rbuf.at[2], r_hbm.at[2])

    QC = 640

    def qkv_body(n, carry):
        r0 = pl.multiple_of(n * QC, QC)
        v = dot(rbuf[2], wq[pl.ds(r0, QC), :], NT) + bq[:, pl.ds(r0, QC)]
        qkvt[pl.ds(r0, QC), :] = v.astype(BF16).T
        return carry
    lax.fori_loop(0, QKV // QC, qkv_body, 0)

    scale = HD ** -0.5
    jpos = lax.broadcasted_iota(jnp.int32, (SEQ, SEQ), 0)
    ipos = lax.broadcasted_iota(jnp.int32, (SEQ, SEQ), 1)
    causal = jpos <= ipos
    jf = jpos.astype(F32)
    base = jnp.where(me == 0, 1.0, jnp.where(me == 1, 0.25, jnp.where(me == 2, 0.0625, 0.015625))).astype(F32)

    def head(h, t):
        r0 = h * 3 * HD + t * HD
        return qkvt[r0:r0 + HD, :]

    for h in range(NH):
        s = dot(head(h, 1), head(h, 0), TN) * scale + (base * SLOPES[h]) * jf
        s = jnp.where(causal, s, MASK_VALUE)
        e = jnp.exp(s - jnp.max(s, axis=0, keepdims=True))
        p = e * (1.0 / jnp.sum(e, axis=0, keepdims=True))
        prob[h] = p
        lbuf[OFF_O + h * HD:OFF_O + (h + 1) * HD, :] = dot(head(h, 2), p.astype(BF16), NN).astype(BF16)
    for t in range(CTX // 128):
        ctx[:, t * 128:(t + 1) * 128] = lbuf[OFF_O + t * 128:OFF_O + (t + 1) * 128, :].T

    wcopies[1].wait()
    sc_a.run(lambda cols: dot(ctx[...], wo[:, cols], NN), RSC)
    sc_a.relay_from(0)

    for c in range(AGC):
        gat_m.forward(c)
    wcopies[2].wait()
    gat_m.finish()
    emit(rbuf.at[1], r_hbm.at[1])
    FC = 512

    def dact_body(n, carry):
        f0 = pl.multiple_of(n * FC, FC)
        dact[:, pl.ds(f0, FC)] = dot(rbuf[1], wd[pl.ds(f0, FC), :], NT).astype(BF16)
        return carry
    lax.fori_loop(0, FF // FC, dact_body, 0)

    sc_a.arrive()
    for b, i in blocks:
        x1[b] = xh[b].astype(F32) + sc_a.block(b) + bo[...]
        xhat, _ = ln_stats(x1[b])
        gbuf[block_rows(b), :] = (xhat * g2[...] + b2[...]).astype(BF16)
        sh_g.send(b, i)
    wcopies[3].wait()
    for b, i in blocks:
        sh_g.finish(b, i)

    UC = 1280
    k0 = 0.7978845608028654
    k1 = 0.044715

    def up_body(n, carry):
        f0 = pl.multiple_of(n * UC, UC)
        cols = pl.ds(f0, UC)
        v = dot(gbuf[...], wu[:, cols], NN) + bu[:, cols]
        v2 = v * v
        t = jnp.tanh(k0 * (v + k1 * (v2 * v)))
        hp = 0.5 * (1.0 + t)
        act[:, cols] = (v * hp).astype(BF16)
        dg = hp + (0.5 * k0) * v * (1.0 - t * t) * (1.0 + (3.0 * k1) * v2)
        dpre = dact[:, cols].astype(F32) * dg
        gbu[:, cols] = jnp.sum(dpre, axis=0, keepdims=True)
        rbuf[0, :, cols] = dpre.astype(BF16)
        return carry
    lax.fori_loop(0, FF // UC, up_body, 0)
    emit(rbuf.at[0], r_hbm.at[0])
    emit(gbu, gbu_hbm)

    def dg_chunk(cols):
        return dot(rbuf[0], wu[cols, :], NT)
    sc_g.run(dg_chunk, 2)

    def rest(n):
        @pl.when(n < 2)
        def _():
            sc_g.relay(n + RSC - 2)
    sc_y.run(lambda cols: dot(act[...], wd[:, cols], NN), RSC, rest)
    sc_y.relay_from(0)

    va[me, 3:4, :] = jnp.sum(rbuf[1, rows(me), :].astype(F32), axis=0, keepdims=True)

    sc_g.arrive()
    for b, i in blocks:
        dgl = sc_g.block(b)
        xhat, rstd = ln_stats(x1[b])
        dm = rbuf[1, block_rows(b), :].astype(F32) + ln_grad(dgl, xhat, rstd, g2[...])
        rbuf[3, block_rows(b), :] = dm.astype(BF16)
        sh_a.send(b, i)
        if i == 0:
            dmid[...] = dm
    va[me, 2:3, :] = jnp.sum(dmid[...], axis=0, keepdims=True)
    dgl = sc_g.block(ax)
    xhat, _ = ln_stats(x1[ax])
    va[me, 0:1, :] = jnp.sum(dgl * xhat, axis=0, keepdims=True)
    va[me, 1:2, :] = jnp.sum(dgl, axis=0, keepdims=True)

    sva, rva = alloc('s', 3), alloc('r', 3)

    def vec_copy(buf, s, r, i, owner, dev):
        return remote(buf.at[owner], buf.at[owner], s + i, r + i, dev)
    for i, dev in enumerate(peers):
        vec_copy(va, sva, rva, i, me, dev).start()
    for b, i in blocks:
        sh_a.finish(b, i)
    emit(rbuf.at[3], r_hbm.at[3])

    ctx[...] = dot(rbuf[3], wo[...], NT).astype(BF16)
    for t in range(CTX // 128):
        dctxt[t * 128:(t + 1) * 128, :] = ctx[:, t * 128:(t + 1) * 128].T

    for h in range(NH):
        dot_h = dctxt[h * HD:(h + 1) * HD, :]
        p = prob[h]
        dp = dot(head(h, 2), dot_h, TN).astype(BF16).astype(F32)
        ds = (p * (dp - jnp.sum(dp * p, axis=0, keepdims=True))).astype(BF16)
        r0 = OFF_QKV + h * 3 * HD
        lbuf[r0:r0 + HD, :] = (dot(head(h, 1), ds, NN) * scale).astype(BF16)
        lbuf[r0 + HD:r0 + 2 * HD, :] = (dot(head(h, 0), ds, NT) * scale).astype(BF16)
        lbuf[r0 + 2 * HD:r0 + 3 * HD, :] = dot(dot_h, p.astype(BF16), NT).astype(BF16)
    for t in range(QKV // 128):
        dqkv[:, t * 128:(t + 1) * 128] = lbuf[OFF_QKV + t * 128:OFF_QKV + (t + 1) * 128, :].T
    emit(lbuf.at[pl.ds(OFF_QKV, QKV + CTX)], l_hbm.at[pl.ds(OFF_QKV, QKV + CTX)])

    sc_h.run(lambda cols: dot(dqkv[...], wq[:, cols], NN), 3)
    sc_h.relay_from(RSC - 3)

    sc_y.arrive()
    outb[0] = (x1[ax] + sc_y.own() + bd[...]).astype(BF16)
    emit(outb.at[0], y_hbm)
    for i, dev in enumerate(peers):
        vec_copy(va, sva, rva, i, dev, dev).wait_recv()
    tot = (va[0] + va[1]) + (va[2] + va[3])
    for i in range(4):
        vo[i] = tot[i:i + 1]

    def tr_body(src, off):
        def body(n, carry):
            r0 = pl.multiple_of(n * 128, 128)
            lbuf[pl.ds(off + r0, 128), :] = src[:, pl.ds(r0, 128)].T
            return carry
        return body
    lax.fori_loop(0, FF // 128, tr_body(act, OFF_ACT), 0)
    lax.fori_loop(0, D // 128, tr_body(gbuf, OFF_G), 0)
    emit(lbuf.at[pl.ds(0, OFF_QKV)], l_hbm.at[pl.ds(0, OFF_QKV)])

    sc_h.arrive()
    dhl = sc_h.own()
    xhat1, rstd1 = ln_stats(xh[ax].astype(F32))
    vb[me, 0:1, :] = jnp.sum(dhl * xhat1, axis=0, keepdims=True)
    vb[me, 1:2, :] = jnp.sum(dhl, axis=0, keepdims=True)
    svb, rvb = alloc('s', 3), alloc('r', 3)
    for i, dev in enumerate(peers):
        vec_copy(vb, svb, rvb, i, me, dev).start()
    outb[1] = (dmid[...] + ln_grad(dhl, xhat1, rstd1, g1[...])).astype(BF16)
    emit(outb.at[1], gx_hbm)
    remote(xh.at[ax], xh.at[ax], sx, rx, cross).wait_send()
    gat_m.drain()
    for g in (sh_h, sh_g, sh_a, sc_a, sc_g, sc_y, sc_h):
        g.drain()
    for i, dev in enumerate(peers):
        vec_copy(va, sva, rva, i, me, dev).wait_send()
    for i, dev in enumerate(peers):
        vec_copy(vb, svb, rvb, i, dev, dev).wait_recv()
    tot = (vb[0] + vb[1]) + (vb[2] + vb[3])
    for i in range(2):
        vo[4 + i] = tot[i:i + 1]
    emit(vo, vec_hbm)
    for i, dev in enumerate(peers):
        vec_copy(vb, svb, rvb, i, me, dev).wait_send()
    for c in outs:
        c.wait()
    assert max(count.values()) <= NSEM


SECTIONS = ((OFF_ACT, FF, 1, 640), (OFF_G, D, 0, 640), (OFF_QKV, QKV, 2, 640), (OFF_O, CTX, 3, 320))
GR = 640
SLOTS = 4


def grad_kernel(y_in, gx_in, vec_in, gbu_in, l_hbm, r_hbm, y_out, gx_out, v0, v1, v2, v3, v4, v5, gbq_hbm, gbu_out,
                dwq, dwo, dwu, dwd, lv, rv, st, yv, gxv, vv, gv, gbq, isem, ssem, psem, osem):
    loads = []
    for i, (off, n, r, _) in enumerate(SECTIONS):
        cl = pltpu.make_async_copy(l_hbm.at[pl.ds(off, n)], lv.at[pl.ds(off, n)], isem.at[2 * i])
        cr = pltpu.make_async_copy(r_hbm.at[r], rv.at[r], isem.at[2 * i + 1])
        cl.start()
        cr.start()
        loads.append((cl, cr))
    passes = [(y_in, yv, y_out), (gx_in, gxv, gx_out), (gbu_in, gv, gbu_out)]
    srcs = (yv, gxv, gv.at[0])
    pin = [pltpu.make_async_copy(a, b, psem.at[i]) for i, (a, b, _) in enumerate(passes)]
    pin.append(pltpu.make_async_copy(vec_in, vv, psem.at[3]))
    for c in pin:
        c.start()
    douts = (dwd, dwu, dwq, dwo)
    step = 0
    last = []

    def out_copy(slot, dst, r0, gr):
        return pltpu.make_async_copy(st.at[slot, pl.ds(0, gr)], dst.at[pl.ds(r0, gr)], ssem.at[slot])
    for i, (off, n, r, gr) in enumerate(SECTIONS):
        loads[i][0].wait()
        loads[i][1].wait()
        dst = douts[i]

        def body(m, carry, off=off, r=r, dst=dst, step=step, gr=gr):
            slot = lax.rem(m + step, SLOTS)

            @pl.when(m + step >= SLOTS)
            def _():
                out_copy(slot, dwd, 0, GR).wait()
            st[slot, 0:gr] = dot(lv[pl.ds(pl.multiple_of(off + m * gr, 64), gr), :], rv[r], NN).astype(BF16)
            out_copy(slot, dst, pl.multiple_of(m * gr, gr), gr).start()
            return carry
        lax.fori_loop(0, n // gr, body, 0)
        last += [((step + m) % SLOTS, gr) for m in range(n // gr)]
        step += n // gr
    for c in pin:
        c.wait()
    done = []
    for i, (_, _, o) in enumerate(passes):
        done.append(pltpu.make_async_copy(srcs[i], o, osem.at[i]))
    for i, o in enumerate((v0, v1, v2, v3, v4, v5)):
        done.append(pltpu.make_async_copy(vv.at[i, 0], o, osem.at[3 + i]))
    ones = jnp.ones((16, SEQ), BF16)
    for h in range(NH):
        for t in range(3):
            r0 = OFF_QKV + h * 3 * HD + t * HD
            gbq[t, h:h + 1, :] = dot(ones, lv[r0:r0 + HD, :], NT)[0:1]
    done.append(pltpu.make_async_copy(gbq, gbq_hbm, osem.at[9]))
    for c in done:
        c.start()
    for slot, gr in last[-SLOTS:]:
        out_copy(slot, dwo, 0, gr).wait()
    for c in done:
        c.wait()


def solution(mesh):
    def local_step(x, ln1_gamma, ln1_beta, w_qkv, b_qkv, w_out, b_out, ln2_gamma, ln2_beta, w_up, b_up, w_down, b_down, grad_y):
        wqt = jnp.transpose(w_qkv, (1, 2, 3, 0)).reshape(QKV, D)
        any_spec = pl.BlockSpec(memory_space=pl.ANY)
        sds = jax.ShapeDtypeStruct
        y, gx, vec, gbu, lmat, rmat = pl.pallas_call(
            block_kernel,
            name='block',
            out_shape=(sds((ROWS, D), BF16), sds((ROWS, D), BF16), sds((6, 1, D), F32), sds((1, FF), F32),
                       sds((LROWS, SEQ), BF16), sds((4, SEQ, D), BF16)),
            in_specs=[any_spec] * 14,
            out_specs=(any_spec,) * 6,
            scratch_shapes=[
                pltpu.VMEM((QKV, D), BF16), pltpu.VMEM((CTX, D), BF16), pltpu.VMEM((D, FF), BF16), pltpu.VMEM((FF, D), BF16),
                pltpu.VMEM((2, ROWS, D), BF16),
                pltpu.VMEM((1, D), F32), pltpu.VMEM((1, D), F32), pltpu.VMEM((3, NH, HD), F32), pltpu.VMEM((1, QKV), F32),
                pltpu.VMEM((1, D), F32), pltpu.VMEM((1, D), F32), pltpu.VMEM((1, D), F32), pltpu.VMEM((1, FF), F32), pltpu.VMEM((1, D), F32),
                pltpu.VMEM((4, SEQ, D), BF16), pltpu.VMEM((LROWS, SEQ), BF16), pltpu.VMEM((SEQ, D), BF16),
                pltpu.VMEM((QKV, SEQ), BF16), pltpu.VMEM((SEQ, QKV), BF16), pltpu.VMEM((SEQ, CTX), BF16),
                pltpu.VMEM((CTX, SEQ), BF16), pltpu.VMEM((NH, SEQ, SEQ), F32),
                pltpu.VMEM((SEQ, FF), BF16), pltpu.VMEM((SEQ, FF), BF16),
                pltpu.VMEM((2, ROWS, D), F32), pltpu.VMEM((ROWS, D), F32), pltpu.VMEM((2, ROWS, D), BF16),
                pltpu.VMEM((1, FF), F32),
                pltpu.VMEM((TP, 4, D), F32), pltpu.VMEM((TP, 2, D), F32), pltpu.VMEM((6, 1, D), F32),
                pltpu.VMEM((4, 2, 2, ROWS, D), BF16), pltpu.VMEM((4, 2, ROWS, D), BF16),
                pltpu.VMEM((4, 2, ROWS, D), BF16), pltpu.VMEM((4, 2, ROWS, D), BF16),
                pltpu.SemaphoreType.DMA((4,)), pltpu.SemaphoreType.DMA((10,)), pltpu.SemaphoreType.DMA((10,)),
                pltpu.SemaphoreType.DMA((NSEM,)), pltpu.SemaphoreType.DMA((NSEM,)),
            ],
            compiler_params=pltpu.CompilerParams(collective_id=0, has_side_effects=True, vmem_limit_bytes=66_000_000),
            cost_estimate=pl.CostEstimate(flops=10_000_000_000, bytes_accessed=45_000_000, transcendentals=1_000_000),
        )(x[0], grad_y[0], wqt, w_out, w_up, w_down, ln1_gamma, ln1_beta, jnp.transpose(b_qkv, (1, 0, 2)), b_out,
          ln2_gamma, ln2_beta, b_up, b_down)
        y, gx, v0, v1, v2, v3, v4, v5, gbq, gbu, dwq, dwo, dwu, dwd = pl.pallas_call(
            grad_kernel,
            name='weight_grads',
            out_shape=(sds((ROWS, D), BF16), sds((ROWS, D), BF16)) + (sds((D,), F32),) * 6 + (
                sds((3, NH, HD), F32), sds((FF,), F32), sds((QKV, D), BF16), sds((CTX, D), BF16), sds((D, FF), BF16), sds((FF, D), BF16)),
            in_specs=[any_spec] * 6,
            out_specs=(any_spec,) * 14,
            scratch_shapes=[
                pltpu.VMEM((LROWS, SEQ), BF16), pltpu.VMEM((4, SEQ, D), BF16), pltpu.VMEM((SLOTS, GR, D), BF16),
                pltpu.VMEM((ROWS, D), BF16), pltpu.VMEM((ROWS, D), BF16), pltpu.VMEM((6, 1, D), F32), pltpu.VMEM((1, FF), F32),
                pltpu.VMEM((3, NH, HD), F32),
                pltpu.SemaphoreType.DMA((8,)), pltpu.SemaphoreType.DMA((4,)), pltpu.SemaphoreType.DMA((4,)), pltpu.SemaphoreType.DMA((10,)),
            ],
            compiler_params=pltpu.CompilerParams(vmem_limit_bytes=66_000_000),
            cost_estimate=pl.CostEstimate(flops=5_000_000_000, bytes_accessed=44_000_000, transcendentals=0),
        )(y, gx, vec, gbu, lmat, rmat)
        g_wqkv = jnp.transpose(dwq.reshape(NH, 3, HD, D), (3, 0, 1, 2))
        g_ln2g, g_ln2b, g_bo, g_bd, g_ln1g, g_ln1b = v0, v1, v2, v3, v4, v5
        return (y[None], gx[None], g_ln1g, g_ln1b, g_wqkv, jnp.transpose(gbq, (1, 0, 2)), dwo, g_bo,
                g_ln2g, g_ln2b, dwu, gbu, dwd, g_bd)

    row_spec = P('dp', 'tp', None)
    in_specs = (row_spec, P(), P(), P(None, 'tp', None, None), P('tp', None, None), P('tp', None), P(), P(), P(),
                P(None, 'tp'), P('tp'), P('tp', None), P(), row_spec)
    out_specs = (row_spec, row_spec, P('dp'), P('dp'), P('dp', 'tp', None, None), P(('dp', 'tp'), None, None),
                 P(('dp', 'tp'), None), P('dp'), P('dp'), P('dp'), P('dp', 'tp'), P(('dp', 'tp')), P(('dp', 'tp'), None), P('dp'))
    return jax.shard_map(local_step, mesh=mesh, in_specs=in_specs, out_specs=out_specs, check_vma=False)
```

```python
import jax
import jax.numpy as jnp
from jax import lax
from jax.experimental import pallas as pl
from jax.experimental.pallas import tpu as pltpu
from jax.sharding import PartitionSpec as P

EPS = 1e-5
MASK_VALUE = -1e30
MESH = pl.DeviceIdType.MESH
F32 = jnp.float32
BF16 = jnp.bfloat16

D = 2560
SEQ = 128
TP = 4
ROWS = SEQ // TP
NH = 8
HD = 80
QKV = NH * 3 * HD
CTX = NH * HD
FF = 2560
AGC = 4
NSEM = 72
AGW = D // AGC
CHUNKS = (256, 256, 512, 512, 512, 512)
RSC = len(CHUNKS)
STARTS = tuple(sum(CHUNKS[:i]) for i in range(RSC))
OFF_G, OFF_ACT, OFF_QKV, OFF_O = 0, D, D + FF, D + FF + QKV
LROWS = D + FF + QKV + CTX
SLOPES = [2.0 ** (-(h + 1) / 4.0) for h in range(NH)]
NT = (((1,), (1,)), ((), ()))
NN = (((1,), (0,)), ((), ()))
TN = (((0,), (0,)), ((), ()))


def dot(a, b, dims):
    return lax.dot_general(a, b, dims, preferred_element_type=F32)


def ln_stats(v):
    mean = jnp.mean(v, axis=-1, keepdims=True)
    cen = v - mean
    var = jnp.mean(cen * cen, axis=-1, keepdims=True)
    rstd = lax.rsqrt(var + EPS)
    return cen * rstd, rstd


def ln_grad(dy, xhat, rstd, gain):
    dxh = dy * gain
    m1 = jnp.mean(dxh, axis=-1, keepdims=True)
    m2 = jnp.mean(dxh * xhat, axis=-1, keepdims=True)
    return rstd * (dxh - m1 - xhat * m2)


def block_kernel(x_hbm, gy_hbm, wq_hbm, wo_hbm, wu_hbm, wd_hbm, g1_hbm, b1_hbm, bq_hbm, bo_hbm, g2_hbm, b2_hbm, bu_hbm,
                 bd_hbm, y_hbm, gx_hbm, vec_hbm, gbu_hbm, l_hbm, r_hbm,
                 wq, wo, wu, wd, xh, g1, b1, bqv, bq, bo, g2, b2, bu, bd,
                 rbuf, lbuf, gbuf, qkvt, dqkv, ctx, dctxt, prob, act, dact, x1, xn1, xn2, rs, dmid, outb, gbu, va, vb, vo,
                 pb, rx1, sb, rx2, wsem, lsem, osem, ssem, rsem):
    me = lax.axis_index('tp')
    ax = lax.div(me, 2)
    ak = lax.rem(me, 2)
    partner = 2 * ax + (1 - ak)
    cross = 2 * (1 - ax) + ak
    diag = 2 * (1 - ax) + (1 - ak)
    peers = (partner, cross, diag)

    def rows(i):
        return pl.ds(pl.multiple_of(i * ROWS, ROWS), ROWS)

    def block_rows(b):
        return rows(2 * b + ak)

    count = {'s': 0, 'r': 0}
    _cur = []

    def _ns(name):
        if _cur:
            _cur.pop().__exit__(None, None, None)
        if name:
            _cur.append(jax.named_scope(name))
            _cur[-1].__enter__()
    _ns('start')

    def alloc(kind, n=1):
        base = count[kind]
        count[kind] += n
        return base

    def remote(src, dst, si, ri, dev):
        return pltpu.make_async_remote_copy(src_ref=src, dst_ref=dst, send_sem=ssem.at[si], recv_sem=rsem.at[ri],
                                            device_id={'tp': dev}, device_id_type=MESH)

    x_load = pltpu.make_async_copy(x_hbm, xh.at[ax], lsem.at[0])
    x_load.start()
    small = [(g1_hbm, g1.at[0]), (b1_hbm, b1.at[0]), (bq_hbm, bqv), (bo_hbm, bo.at[0]), (g2_hbm, g2.at[0]), (b2_hbm, b2.at[0]),
             (bu_hbm, bu.at[0]), (bd_hbm, bd.at[0])]
    loads = [pltpu.make_async_copy(s, d, lsem.at[1 + i]) for i, (s, d) in enumerate(small)]
    for c in loads:
        c.start()
    gy_load = pltpu.make_async_copy(gy_hbm, rbuf.at[1, rows(me)], lsem.at[1 + len(small)])
    gy_load.start()
    wcopies = [pltpu.make_async_copy(s, d, wsem.at[i])
               for i, (s, d) in enumerate([(wq_hbm, wq), (wo_hbm, wo), (wd_hbm, wd), (wu_hbm, wu)])]

    bar = pltpu.get_barrier_semaphore()
    for dev in peers:
        pl.semaphore_signal(bar, inc=1, device_id={'tp': dev}, device_id_type=MESH)
    wcopies[0].start()
    wcopies[1].start()

    class Gather:
        def __init__(self, full):
            self.full = full
            self.s = alloc('s', 2 * AGC + 1)
            self.r = alloc('r', 2 * AGC + 1)

        def chunk(self, dev, c):
            return self.full.at[rows(dev), pl.ds(c * AGW, AGW)]

        def cross_copy(self, dev, c):
            ref = self.chunk(dev, c)
            return remote(ref, ref, self.s + c, self.r + c, cross)

        def fwd_copy(self, dev, c):
            ref = self.chunk(dev, c)
            return remote(ref, ref, self.s + AGC + c, self.r + AGC + c, partner)

        def own_copy(self, dev):
            ref = self.full.at[rows(dev)]
            return remote(ref, ref, self.s + 2 * AGC, self.r + 2 * AGC, partner)

        def start(self):
            for c in range(AGC):
                self.cross_copy(me, c).start()
            self.own_copy(me).start()

        def forward(self, c):
            self.cross_copy(cross, c).wait_recv()
            self.fwd_copy(cross, c).start()

        def finish(self):
            self.own_copy(partner).wait_recv()
            for c in range(AGC):
                self.fwd_copy(diag, c).wait_recv()

        def drain(self):
            for c in range(AGC):
                self.cross_copy(me, c).wait_send()
                self.fwd_copy(cross, c).wait_send()
            self.own_copy(me).wait_send()

    class Share:
        def __init__(self, full):
            self.full = full
            self.s = alloc('s', 2)
            self.r = alloc('r', 2)

        def copy(self, b, k, i):
            ref = self.full.at[rows(2 * b + k)]
            return remote(ref, ref, self.s + i, self.r + i, partner)

        def send(self, b, i):
            self.copy(b, ak, i).start()

        def finish(self, b, i):
            self.copy(b, 1 - ak, i).wait_recv()

        def drain(self):
            self.copy(ax, ak, 0).wait_send()
            self.copy(1 - ax, ak, 1).wait_send()

    class Reduce:
        def __init__(self, i, both):
            self.p, self.x1, self.sb, self.x2 = pb.at[i], rx1.at[i], sb.at[i], rx2.at[i]
            self.both = both
            self.s = alloc('s', 2 * RSC)
            self.r = alloc('r', 2 * RSC)

        def cols(self, n):
            return pl.ds(STARTS[n], CHUNKS[n])

        def pair(self, n):
            return remote(self.p.at[:, 1 - ak, :, self.cols(n)], self.x1.at[:, :, self.cols(n)], self.s + n, self.r + n, partner)

        def over(self, n):
            if self.both:
                src, dst = self.sb.at[:, :, self.cols(n)], self.x2.at[:, :, self.cols(n)]
            else:
                src, dst = self.sb.at[0, :, self.cols(n)], self.x2.at[0, :, self.cols(n)]
            return remote(src, dst, self.s + RSC + n, self.r + RSC + n, cross)

        def produce(self, n, val):
            self.p[:, :, :, self.cols(n)] = val.astype(BF16).reshape(2, 2, ROWS, CHUNKS[n])
            self.pair(n).start()

        def relay(self, n):
            self.pair(n).wait_recv()
            c = self.cols(n)
            if self.both:
                self.sb[:, :, c] = (self.p[:, ak, :, c].astype(F32) + self.x1[:, :, c].astype(F32)).astype(BF16)
            else:
                self.sb[0, :, c] = (self.p[1 - ax, ak, :, c].astype(F32) + self.x1[1 - ax, :, c].astype(F32)).astype(BF16)
            self.over(n).start()

        def run(self, fn, lag, also=None):
            for n in range(RSC):
                self.produce(n, fn(self.cols(n)))
                if n >= lag:
                    self.relay(n - lag)
                if also is not None:
                    also(n)

        def relay_from(self, first):
            for n in range(first, RSC):
                self.relay(n)

        def arrive(self):
            for n in range(RSC):
                self.over(n).wait_recv()

        def block(self, b):
            return (self.sb[b].astype(F32) + self.x2[b].astype(F32)).astype(BF16).astype(F32)

        def own(self):
            v = self.p[ax, ak].astype(F32) + self.x1[ax].astype(F32) + self.x2[0].astype(F32)
            return v.astype(BF16).astype(F32)

        def drain(self):
            for n in range(RSC):
                self.pair(n).wait_send()
                self.over(n).wait_send()

    gat_m = Gather(rbuf.at[1])
    sh_h, sh_g, sh_a = Share(rbuf.at[2]), Share(gbuf), Share(rbuf.at[3])
    sc_a, sc_g, sc_y, sc_h = Reduce(0, True), Reduce(1, True), Reduce(2, False), Reduce(3, False)
    blocks = ((ax, 0), (1 - ax, 1))
    outs = []

    def emit(src, dst):
        c = pltpu.make_async_copy(src, dst, osem.at[len(outs)])
        c.start()
        outs.append(c)

    sx, rx = alloc('s'), alloc('r')
    _ns('barrier')
    x_load.wait()
    pl.semaphore_wait(bar, 3)
    _ns('xsend')
    remote(xh.at[ax], xh.at[ax], sx, rx, cross).start()
    for c in loads:
        c.wait()
    bq[...] = jnp.concatenate([bqv[t, h:h + 1, :] for h in range(NH) for t in range(3)], axis=1)
    for b, i in blocks:
        if i == 1:
            remote(xh.at[1 - ax], xh.at[1 - ax], sx, rx, cross).wait_recv()
        xhat, rstd = ln_stats(xh[b].astype(F32))
        if i == 0:
            xn1[...] = xhat
            rs[2] = jnp.broadcast_to(rstd, (ROWS, 128))
        rbuf[2, block_rows(b), :] = (xhat * g1[...] + b1[...]).astype(BF16)
        sh_h.send(b, i)
    _ns('hshare')
    gy_load.wait()
    gat_m.start()
    wcopies[2].start()
    wcopies[3].start()
    wcopies[0].wait()
    for b, i in blocks:
        sh_h.finish(b, i)
    emit(rbuf.at[2], r_hbm.at[2])

    _ns('qkv')
    QC = 640

    def qkv_body(n, carry):
        r0 = pl.multiple_of(n * QC, QC)
        v = dot(rbuf[2], wq[pl.ds(r0, QC), :], NT) + bq[:, pl.ds(r0, QC)]
        qkvt[pl.ds(r0, QC), :] = v.astype(BF16).T
        return carry
    lax.fori_loop(0, QKV // QC, qkv_body, 0)

    _ns('attn')
    scale = HD ** -0.5
    jpos = lax.broadcasted_iota(jnp.int32, (SEQ, SEQ), 0)
    ipos = lax.broadcasted_iota(jnp.int32, (SEQ, SEQ), 1)
    causal = jpos <= ipos
    jf = jpos.astype(F32)
    base = jnp.where(me == 0, 1.0, jnp.where(me == 1, 0.25, jnp.where(me == 2, 0.0625, 0.015625))).astype(F32)

    def head(h, t):
        r0 = h * 3 * HD + t * HD
        return qkvt[r0:r0 + HD, :]

    for h in range(NH):
        s = dot(head(h, 1), head(h, 0), TN) * scale + (base * SLOPES[h]) * jf
        s = jnp.where(causal, s, MASK_VALUE)
        e = jnp.exp(s - jnp.max(s, axis=0, keepdims=True))
        p = e * (1.0 / jnp.sum(e, axis=0, keepdims=True))
        prob[h] = p
        lbuf[OFF_O + h * HD:OFF_O + (h + 1) * HD, :] = dot(head(h, 2), p.astype(BF16), NN).astype(BF16)
    for t in range(CTX // 128):
        ctx[:, t * 128:(t + 1) * 128] = lbuf[OFF_O + t * 128:OFF_O + (t + 1) * 128, :].T

    _ns('outproj')
    wcopies[1].wait()
    sc_a.run(lambda cols: dot(ctx[...], wo[:, cols], NN), 4)
    _ns('arelay')
    sc_a.relay_from(RSC - 4)

    _ns('gm_fwd')
    for c in range(AGC):
        gat_m.forward(c)
    wcopies[2].wait()
    gat_m.finish()
    emit(rbuf.at[1], r_hbm.at[1])
    _ns('dact')
    FC = 512

    def dact_body(n, carry):
        f0 = pl.multiple_of(n * FC, FC)
        dact[:, pl.ds(f0, FC)] = dot(rbuf[1], wd[pl.ds(f0, FC), :], NT).astype(BF16)
        return carry
    lax.fori_loop(0, FF // FC, dact_body, 0)

    _ns('a_wait')
    sc_a.arrive()
    _ns('ln2')
    for b, i in blocks:
        xm = xh[b].astype(F32) + sc_a.block(b) + bo[...]
        if i == 0:
            x1[...] = xm
        xhat, rstd = ln_stats(xm)
        xn2[b] = xhat
        rs[b] = jnp.broadcast_to(rstd, (ROWS, 128))
        gbuf[block_rows(b), :] = (xhat * g2[...] + b2[...]).astype(BF16)
        sh_g.send(b, i)
    _ns('g_share')
    wcopies[3].wait()
    for b, i in blocks:
        sh_g.finish(b, i)

    _ns('up')
    UC = 1280
    k0 = 0.7978845608028654
    k1 = 0.044715

    def up_body(n, carry):
        f0 = pl.multiple_of(n * UC, UC)
        cols = pl.ds(f0, UC)
        v = dot(gbuf[...], wu[:, cols], NN) + bu[:, cols]
        v2 = v * v
        t = jnp.tanh(k0 * (v + k1 * (v2 * v)))
        hp = 0.5 * (1.0 + t)
        act[:, cols] = (v * hp).astype(BF16)
        dg = hp + (0.5 * k0) * v * (1.0 - t * t) * (1.0 + (3.0 * k1) * v2)
        dpre = dact[:, cols].astype(F32) * dg
        gbu[:, cols] = jnp.sum(dpre, axis=0, keepdims=True)
        rbuf[0, :, cols] = dpre.astype(BF16)
        return carry
    lax.fori_loop(0, FF // UC, up_body, 0)
    emit(rbuf.at[0], r_hbm.at[0])
    emit(gbu, gbu_hbm)

    _ns('dg')
    def dg_chunk(cols):
        return dot(rbuf[0], wu[cols, :], NT)
    sc_g.run(dg_chunk, 2)

    _ns('down')
    def rest(n):
        if n < 2:
            sc_g.relay(n + RSC - 2)
    sc_y.run(lambda cols: dot(act[...], wd[:, cols], NN), RSC, rest)
    _ns('yrelay')
    sc_y.relay_from(0)

    _ns('vecy')
    va[me, 3:4, :] = jnp.sum(rbuf[1, rows(me), :].astype(F32), axis=0, keepdims=True)

    _ns('g_wait')
    sc_g.arrive()
    _ns('ln2b')
    for b, i in blocks:
        dgl = sc_g.block(b)
        xhat, rstd = xn2[b], rs[b, :, 0:1]
        dm = rbuf[1, block_rows(b), :].astype(F32) + ln_grad(dgl, xhat, rstd, g2[...])
        rbuf[3, block_rows(b), :] = dm.astype(BF16)
        sh_a.send(b, i)
        if i == 0:
            dmid[...] = dm
    va[me, 2:3, :] = jnp.sum(dmid[...], axis=0, keepdims=True)
    dgl = sc_g.block(ax)
    va[me, 0:1, :] = jnp.sum(dgl * xn2[ax], axis=0, keepdims=True)
    va[me, 1:2, :] = jnp.sum(dgl, axis=0, keepdims=True)

    sva, rva = alloc('s', 3), alloc('r', 3)

    def vec_copy(buf, s, r, i, owner, dev):
        return remote(buf.at[owner], buf.at[owner], s + i, r + i, dev)
    for i, dev in enumerate(peers):
        vec_copy(va, sva, rva, i, me, dev).start()
    _ns('a_share')
    for b, i in blocks:
        sh_a.finish(b, i)
    emit(rbuf.at[3], r_hbm.at[3])

    _ns('attnb')
    ctx[...] = dot(rbuf[3], wo[...], NT).astype(BF16)
    for t in range(CTX // 128):
        dctxt[t * 128:(t + 1) * 128, :] = ctx[:, t * 128:(t + 1) * 128].T

    for h in range(NH):
        dot_h = dctxt[h * HD:(h + 1) * HD, :]
        p = prob[h]
        dp = dot(head(h, 2), dot_h, TN).astype(BF16).astype(F32)
        ds = (p * (dp - jnp.sum(dp * p, axis=0, keepdims=True))).astype(BF16)
        r0 = OFF_QKV + h * 3 * HD
        lbuf[r0:r0 + HD, :] = (dot(head(h, 1), ds, NN) * scale).astype(BF16)
        lbuf[r0 + HD:r0 + 2 * HD, :] = (dot(head(h, 0), ds, NT) * scale).astype(BF16)
        lbuf[r0 + 2 * HD:r0 + 3 * HD, :] = dot(dot_h, p.astype(BF16), NT).astype(BF16)
    for t in range(QKV // 128):
        dqkv[:, t * 128:(t + 1) * 128] = lbuf[OFF_QKV + t * 128:OFF_QKV + (t + 1) * 128, :].T
    emit(lbuf.at[pl.ds(OFF_QKV, QKV + CTX)], l_hbm.at[pl.ds(OFF_QKV, QKV + CTX)])

    _ns('dh')
    sc_h.run(lambda cols: dot(dqkv[...], wq[:, cols], NN), 3)
    _ns('hrelay')
    sc_h.relay_from(RSC - 3)

    _ns('y')
    sc_y.arrive()
    outb[0] = (x1[...] + sc_y.own() + bd[...]).astype(BF16)
    emit(outb.at[0], y_hbm)
    for i, dev in enumerate(peers):
        vec_copy(va, sva, rva, i, dev, dev).wait_recv()
    tot = (va[0] + va[1]) + (va[2] + va[3])
    for i in range(4):
        vo[i] = tot[i:i + 1]

    _ns('transp')
    def tr_body(src, off):
        def body(n, carry):
            r0 = pl.multiple_of(n * 128, 128)
            lbuf[pl.ds(off + r0, 128), :] = src[:, pl.ds(r0, 128)].T
            return carry
        return body
    lax.fori_loop(0, FF // 128, tr_body(act, OFF_ACT), 0)
    lax.fori_loop(0, D // 128, tr_body(gbuf, OFF_G), 0)
    emit(lbuf.at[pl.ds(0, OFF_QKV)], l_hbm.at[pl.ds(0, OFF_QKV)])

    _ns('h_wait')
    sc_h.arrive()
    _ns('ln1b')
    dhl = sc_h.own()
    xhat1, rstd1 = xn1[...], rs[2, :, 0:1]
    vb[me, 0:1, :] = jnp.sum(dhl * xhat1, axis=0, keepdims=True)
    vb[me, 1:2, :] = jnp.sum(dhl, axis=0, keepdims=True)
    svb, rvb = alloc('s', 3), alloc('r', 3)
    for i, dev in enumerate(peers):
        vec_copy(vb, svb, rvb, i, me, dev).start()
    outb[1] = (dmid[...] + ln_grad(dhl, xhat1, rstd1, g1[...])).astype(BF16)
    emit(outb.at[1], gx_hbm)
    _ns('drain')
    remote(xh.at[ax], xh.at[ax], sx, rx, cross).wait_send()
    gat_m.drain()
    for g in (sh_h, sh_g, sh_a, sc_a, sc_g, sc_y, sc_h):
        g.drain()
    for i, dev in enumerate(peers):
        vec_copy(va, sva, rva, i, me, dev).wait_send()
    _ns('vecwait')
    for i, dev in enumerate(peers):
        vec_copy(vb, svb, rvb, i, dev, dev).wait_recv()
    tot = (vb[0] + vb[1]) + (vb[2] + vb[3])
    for i in range(2):
        vo[4 + i] = tot[i:i + 1]
    _ns('final')
    emit(vo, vec_hbm)
    for i, dev in enumerate(peers):
        vec_copy(vb, svb, rvb, i, me, dev).wait_send()
    for c in outs:
        c.wait()
    _ns(None)
    assert max(count.values()) <= NSEM


GR = 640
SLOTS = 4
SECTIONS = ((OFF_ACT, FF, 1), (OFF_G, D, 0), (OFF_QKV, QKV, 2), (OFF_O, CTX, 3))
PIECES = (((160, 1), (160, 1), (320, 1), (GR, 3)), ((GR, 4),), ((GR, 3),), ((320, 1), (160, 1), (160, 1)))
SMALL = 6


def grad_kernel(y_in, gx_in, vec_in, gbu_in, l_hbm, r_hbm, y_out, gx_out, v0, v1, v2, v3, v4, v5, gbq_hbm, gbu_out,
                dwq, dwo, dwu, dwd, lv, rv, st, st2, yv, gxv, vv, gv, gbq, isem, ssem, ssem2, psem, osem):
    _cur = []

    def _ns(name):
        if _cur:
            _cur.pop().__exit__(None, None, None)
        if name:
            _cur.append(jax.named_scope(name))
            _cur[-1].__enter__()
    _ns('b_start')
    loads = []
    for i, (off, n, r) in enumerate(SECTIONS):
        cl = pltpu.make_async_copy(l_hbm.at[pl.ds(off, n)], lv.at[pl.ds(off, n)], isem.at[2 * i])
        cr = pltpu.make_async_copy(r_hbm.at[r], rv.at[r], isem.at[2 * i + 1])
        cl.start()
        cr.start()
        loads.append((cl, cr))
    passes = [(y_in, yv, y_out), (gx_in, gxv, gx_out), (gbu_in, gv, gbu_out)]
    srcs = (yv, gxv, gv.at[0])
    pin = [pltpu.make_async_copy(a, b, psem.at[i]) for i, (a, b, _) in enumerate(passes)]
    pin.append(pltpu.make_async_copy(vec_in, vv, psem.at[3]))
    for c in pin:
        c.start()
    douts = (dwd, dwu, dwq, dwo)
    step = 0

    def out_copy(slot, dst, r0):
        return pltpu.make_async_copy(st.at[slot], dst.at[pl.ds(r0, GR)], ssem.at[slot])
    smalls = []
    for i, (off, n, r) in enumerate(SECTIONS):
        _ns('b_load%d' % i)
        loads[i][0].wait()
        loads[i][1].wait()
        dst = douts[i]
        _ns('b_sec%d' % i)
        r0 = 0
        for gr, times in PIECES[i]:
            if gr < GR:
                e = len(smalls)

                def small(m, carry, off=off + r0, gr=gr, e=e, r=r):
                    st2[e, 0:gr] = dot(lv[pl.ds(pl.multiple_of(off + m * gr, 32), gr), :], rv[r], NN).astype(BF16)
                    return carry
                lax.fori_loop(0, 1, small, 0)
                smalls.append(pltpu.make_async_copy(st2.at[e, pl.ds(0, gr)], dst.at[pl.ds(r0, gr)], ssem2.at[e]))
                smalls[-1].start()
            else:
                def body(m, carry, off=off + r0, r=r, dst=dst, step=step, r0=r0):
                    slot = lax.rem(m + step, SLOTS)

                    @pl.when(m + step >= SLOTS)
                    def _():
                        out_copy(slot, dwd, 0).wait()
                    st[slot] = dot(lv[pl.ds(pl.multiple_of(off + m * GR, 64), GR), :], rv[r], NN).astype(BF16)
                    out_copy(slot, dst, pl.multiple_of(r0 + m * GR, 64)).start()
                    return carry
                lax.fori_loop(0, times, body, 0)
                step += times
            r0 += gr * times
        if i == 2:
            ones = jnp.ones((16, SEQ), BF16)
            for h in range(NH):
                for t in range(3):
                    q0 = OFF_QKV + h * 3 * HD + t * HD
                    gbq[t, h:h + 1, :] = dot(ones, lv[q0:q0 + HD, :], NT)[0:1]
    _ns('b_tail')
    for c in pin:
        c.wait()
    done = []
    for i, (_, _, o) in enumerate(passes):
        done.append(pltpu.make_async_copy(srcs[i], o, osem.at[i]))
    for i, o in enumerate((v0, v1, v2, v3, v4, v5)):
        done.append(pltpu.make_async_copy(vv.at[i, 0], o, osem.at[3 + i]))
    done.append(pltpu.make_async_copy(gbq, gbq_hbm, osem.at[9]))
    for c in done:
        c.start()
    _ns('b_flush')
    for slot in range(SLOTS):
        out_copy(slot, dwd, 0).wait()
    for c in smalls:
        c.wait()
    for c in done:
        c.wait()
    _ns(None)


def solution(mesh):
    def local_step(x, ln1_gamma, ln1_beta, w_qkv, b_qkv, w_out, b_out, ln2_gamma, ln2_beta, w_up, b_up, w_down, b_down, grad_y):
        wqt = jnp.transpose(w_qkv, (1, 2, 3, 0)).reshape(QKV, D)
        any_spec = pl.BlockSpec(memory_space=pl.ANY)
        sds = jax.ShapeDtypeStruct
        y, gx, vec, gbu, lmat, rmat = pl.pallas_call(
            block_kernel,
            name='block',
            out_shape=(sds((ROWS, D), BF16), sds((ROWS, D), BF16), sds((6, 1, D), F32), sds((1, FF), F32),
                       sds((LROWS, SEQ), BF16), sds((4, SEQ, D), BF16)),
            in_specs=[any_spec] * 14,
            out_specs=(any_spec,) * 6,
            scratch_shapes=[
                pltpu.VMEM((QKV, D), BF16), pltpu.VMEM((CTX, D), BF16), pltpu.VMEM((D, FF), BF16), pltpu.VMEM((FF, D), BF16),
                pltpu.VMEM((2, ROWS, D), BF16),
                pltpu.VMEM((1, D), F32), pltpu.VMEM((1, D), F32), pltpu.VMEM((3, NH, HD), F32), pltpu.VMEM((1, QKV), F32),
                pltpu.VMEM((1, D), F32), pltpu.VMEM((1, D), F32), pltpu.VMEM((1, D), F32), pltpu.VMEM((1, FF), F32), pltpu.VMEM((1, D), F32),
                pltpu.VMEM((4, SEQ, D), BF16), pltpu.VMEM((LROWS, SEQ), BF16), pltpu.VMEM((SEQ, D), BF16),
                pltpu.VMEM((QKV, SEQ), BF16), pltpu.VMEM((SEQ, QKV), BF16), pltpu.VMEM((SEQ, CTX), BF16),
                pltpu.VMEM((CTX, SEQ), BF16), pltpu.VMEM((NH, SEQ, SEQ), F32),
                pltpu.VMEM((SEQ, FF), BF16), pltpu.VMEM((SEQ, FF), BF16),
                pltpu.VMEM((ROWS, D), F32), pltpu.VMEM((ROWS, D), F32), pltpu.VMEM((2, ROWS, D), F32), pltpu.VMEM((3, ROWS, 128), F32),
                pltpu.VMEM((ROWS, D), F32), pltpu.VMEM((2, ROWS, D), BF16),
                pltpu.VMEM((1, FF), F32),
                pltpu.VMEM((TP, 4, D), F32), pltpu.VMEM((TP, 2, D), F32), pltpu.VMEM((6, 1, D), F32),
                pltpu.VMEM((4, 2, 2, ROWS, D), BF16), pltpu.VMEM((4, 2, ROWS, D), BF16),
                pltpu.VMEM((4, 2, ROWS, D), BF16), pltpu.VMEM((4, 2, ROWS, D), BF16),
                pltpu.SemaphoreType.DMA((4,)), pltpu.SemaphoreType.DMA((10,)), pltpu.SemaphoreType.DMA((10,)),
                pltpu.SemaphoreType.DMA((NSEM,)), pltpu.SemaphoreType.DMA((NSEM,)),
            ],
            compiler_params=pltpu.CompilerParams(collective_id=0, has_side_effects=True, vmem_limit_bytes=66_000_000),
            cost_estimate=pl.CostEstimate(flops=10_000_000_000, bytes_accessed=45_000_000, transcendentals=1_000_000),
        )(x[0], grad_y[0], wqt, w_out, w_up, w_down, ln1_gamma, ln1_beta, jnp.transpose(b_qkv, (1, 0, 2)), b_out,
          ln2_gamma, ln2_beta, b_up, b_down)
        y, gx, v0, v1, v2, v3, v4, v5, gbq, gbu, dwq, dwo, dwu, dwd = pl.pallas_call(
            grad_kernel,
            name='weight_grads',
            out_shape=(sds((ROWS, D), BF16), sds((ROWS, D), BF16)) + (sds((D,), F32),) * 6 + (
                sds((3, NH, HD), F32), sds((FF,), F32), sds((QKV, D), BF16), sds((CTX, D), BF16), sds((D, FF), BF16), sds((FF, D), BF16)),
            in_specs=[any_spec] * 6,
            out_specs=(any_spec,) * 14,
            scratch_shapes=[
                pltpu.VMEM((LROWS, SEQ), BF16), pltpu.VMEM((4, SEQ, D), BF16), pltpu.VMEM((SLOTS, GR, D), BF16), pltpu.VMEM((SMALL, 320, D), BF16),
                pltpu.VMEM((ROWS, D), BF16), pltpu.VMEM((ROWS, D), BF16), pltpu.VMEM((6, 1, D), F32), pltpu.VMEM((1, FF), F32),
                pltpu.VMEM((3, NH, HD), F32),
                pltpu.SemaphoreType.DMA((8,)), pltpu.SemaphoreType.DMA((SLOTS,)), pltpu.SemaphoreType.DMA((SMALL,)), pltpu.SemaphoreType.DMA((4,)), pltpu.SemaphoreType.DMA((10,)),
            ],
            compiler_params=pltpu.CompilerParams(vmem_limit_bytes=66_000_000),
            cost_estimate=pl.CostEstimate(flops=5_000_000_000, bytes_accessed=44_000_000, transcendentals=0),
        )(y, gx, vec, gbu, lmat, rmat)
        g_wqkv = jnp.transpose(dwq.reshape(NH, 3, HD, D), (3, 0, 1, 2))
        g_ln2g, g_ln2b, g_bo, g_bd, g_ln1g, g_ln1b = v0, v1, v2, v3, v4, v5
        return (y[None], gx[None], g_ln1g, g_ln1b, g_wqkv, jnp.transpose(gbq, (1, 0, 2)), dwo, g_bo,
                g_ln2g, g_ln2b, dwu, gbu, dwd, g_bd)

    row_spec = P('dp', 'tp', None)
    in_specs = (row_spec, P(), P(), P(None, 'tp', None, None), P('tp', None, None), P('tp', None), P(), P(), P(),
                P(None, 'tp'), P('tp'), P('tp', None), P(), row_spec)
    out_specs = (row_spec, row_spec, P('dp'), P('dp'), P('dp', 'tp', None, None), P(('dp', 'tp'), None, None),
                 P(('dp', 'tp'), None), P('dp'), P('dp'), P('dp'), P('dp', 'tp'), P(('dp', 'tp')), P(('dp', 'tp'), None), P('dp'))
    return jax.shard_map(local_step, mesh=mesh, in_specs=in_specs, out_specs=out_specs, check_vma=False)
```

```python
import jax
import jax.numpy as jnp
from jax import lax
from jax.experimental import pallas as pl
from jax.experimental.pallas import tpu as pltpu
from jax.sharding import PartitionSpec as P

EPS = 1e-5
MASK_VALUE = -1e30
MESH = pl.DeviceIdType.MESH
F32 = jnp.float32
BF16 = jnp.bfloat16

D = 2560
SEQ = 128
TP = 4
ROWS = SEQ // TP
NH = 8
HD = 80
QKV = NH * 3 * HD
CTX = NH * HD
FF = 2560
AGC = 4
NSEM = 80
AGW = D // AGC
CHUNKS = (256, 256, 512, 512, 512, 256, 256)
RSC = len(CHUNKS)
STARTS = tuple(sum(CHUNKS[:i]) for i in range(RSC))
OFF_G, OFF_ACT, OFF_QKV, OFF_O = 0, D, D + FF, D + FF + QKV
LROWS = D + FF + QKV + CTX
SLOPES = [2.0 ** (-(h + 1) / 4.0) for h in range(NH)]
NT = (((1,), (1,)), ((), ()))
NN = (((1,), (0,)), ((), ()))
TN = (((0,), (0,)), ((), ()))


def dot(a, b, dims):
    return lax.dot_general(a, b, dims, preferred_element_type=F32)


def ln_stats(v):
    mean = jnp.mean(v, axis=-1, keepdims=True)
    cen = v - mean
    var = jnp.mean(cen * cen, axis=-1, keepdims=True)
    rstd = lax.rsqrt(var + EPS)
    return cen * rstd, rstd


def ln_grad(dy, xhat, rstd, gain):
    dxh = dy * gain
    m1 = jnp.mean(dxh, axis=-1, keepdims=True)
    m2 = jnp.mean(dxh * xhat, axis=-1, keepdims=True)
    return rstd * (dxh - m1 - xhat * m2)


def block_kernel(x_hbm, gy_hbm, wq_hbm, wo_hbm, wu_hbm, wd_hbm, g1_hbm, b1_hbm, bq_hbm, bo_hbm, g2_hbm, b2_hbm, bu_hbm,
                 bd_hbm, y_hbm, gx_hbm, vec_hbm, gbu_hbm, l_hbm, r_hbm,
                 wq, wo, wu, wd, xh, g1, b1, bqv, bq, bo, g2, b2, bu, bd,
                 rbuf, lbuf, gbuf, qkvt, dqkv, ctx, dctxt, prob, act, dact, x1, xn1, xn2, rs, dmid, outb, gbu, va, vb, vo,
                 pb, rx1, sb, rx2, wsem, lsem, osem, ssem, rsem):
    me = lax.axis_index('tp')
    ax = lax.div(me, 2)
    ak = lax.rem(me, 2)
    partner = 2 * ax + (1 - ak)
    cross = 2 * (1 - ax) + ak
    diag = 2 * (1 - ax) + (1 - ak)
    peers = (partner, cross, diag)

    def rows(i):
        return pl.ds(pl.multiple_of(i * ROWS, ROWS), ROWS)

    def block_rows(b):
        return rows(2 * b + ak)

    count = {'s': 0, 'r': 0}
    _cur = []

    def _ns(name):
        if _cur:
            _cur.pop().__exit__(None, None, None)
        if name:
            _cur.append(jax.named_scope(name))
            _cur[-1].__enter__()
    _ns('start')

    def alloc(kind, n=1):
        base = count[kind]
        count[kind] += n
        return base

    def remote(src, dst, si, ri, dev):
        return pltpu.make_async_remote_copy(src_ref=src, dst_ref=dst, send_sem=ssem.at[si], recv_sem=rsem.at[ri],
                                            device_id={'tp': dev}, device_id_type=MESH)

    x_load = pltpu.make_async_copy(x_hbm, xh.at[ax], lsem.at[0])
    x_load.start()
    small = [(g1_hbm, g1.at[0]), (b1_hbm, b1.at[0]), (bq_hbm, bqv), (bo_hbm, bo.at[0]), (g2_hbm, g2.at[0]), (b2_hbm, b2.at[0]),
             (bu_hbm, bu.at[0]), (bd_hbm, bd.at[0])]
    loads = [pltpu.make_async_copy(s, d, lsem.at[1 + i]) for i, (s, d) in enumerate(small)]
    for c in loads:
        c.start()
    gy_load = pltpu.make_async_copy(gy_hbm, rbuf.at[1, rows(me)], lsem.at[1 + len(small)])
    gy_load.start()
    wcopies = [pltpu.make_async_copy(s, d, wsem.at[i])
               for i, (s, d) in enumerate([(wq_hbm, wq), (wo_hbm, wo), (wd_hbm, wd), (wu_hbm, wu)])]

    bar = pltpu.get_barrier_semaphore()
    for dev in peers:
        pl.semaphore_signal(bar, inc=1, device_id={'tp': dev}, device_id_type=MESH)
    wcopies[0].start()
    wcopies[1].start()

    class Gather:
        def __init__(self, full):
            self.full = full
            self.s = alloc('s', 2 * AGC + 1)
            self.r = alloc('r', 2 * AGC + 1)

        def chunk(self, dev, c):
            return self.full.at[rows(dev), pl.ds(c * AGW, AGW)]

        def cross_copy(self, dev, c):
            ref = self.chunk(dev, c)
            return remote(ref, ref, self.s + c, self.r + c, cross)

        def fwd_copy(self, dev, c):
            ref = self.chunk(dev, c)
            return remote(ref, ref, self.s + AGC + c, self.r + AGC + c, partner)

        def own_copy(self, dev):
            ref = self.full.at[rows(dev)]
            return remote(ref, ref, self.s + 2 * AGC, self.r + 2 * AGC, partner)

        def start(self):
            for c in range(AGC):
                self.cross_copy(me, c).start()
            self.own_copy(me).start()

        def forward(self, c):
            self.cross_copy(cross, c).wait_recv()
            self.fwd_copy(cross, c).start()

        def finish(self):
            self.own_copy(partner).wait_recv()
            for c in range(AGC):
                self.fwd_copy(diag, c).wait_recv()

        def drain(self):
            for c in range(AGC):
                self.cross_copy(me, c).wait_send()
                self.fwd_copy(cross, c).wait_send()
            self.own_copy(me).wait_send()

    class Share:
        def __init__(self, full):
            self.full = full
            self.s = alloc('s', 2)
            self.r = alloc('r', 2)

        def copy(self, b, k, i):
            ref = self.full.at[rows(2 * b + k)]
            return remote(ref, ref, self.s + i, self.r + i, partner)

        def send(self, b, i):
            self.copy(b, ak, i).start()

        def finish(self, b, i):
            self.copy(b, 1 - ak, i).wait_recv()

        def drain(self):
            self.copy(ax, ak, 0).wait_send()
            self.copy(1 - ax, ak, 1).wait_send()

    class Reduce:
        def __init__(self, i, both):
            self.p, self.x1, self.sb, self.x2 = pb.at[i], rx1.at[i], sb.at[i], rx2.at[i]
            self.both = both
            self.s = alloc('s', 2 * RSC)
            self.r = alloc('r', 2 * RSC)

        def cols(self, n):
            return pl.ds(STARTS[n], CHUNKS[n])

        def pair(self, n):
            return remote(self.p.at[:, 1 - ak, :, self.cols(n)], self.x1.at[:, :, self.cols(n)], self.s + n, self.r + n, partner)

        def over(self, n):
            if self.both:
                src, dst = self.sb.at[:, :, self.cols(n)], self.x2.at[:, :, self.cols(n)]
            else:
                src, dst = self.sb.at[0, :, self.cols(n)], self.x2.at[0, :, self.cols(n)]
            return remote(src, dst, self.s + RSC + n, self.r + RSC + n, cross)

        def produce(self, n, val):
            self.p[:, :, :, self.cols(n)] = val.astype(BF16).reshape(2, 2, ROWS, CHUNKS[n])
            self.pair(n).start()

        def relay(self, n):
            self.pair(n).wait_recv()
            c = self.cols(n)
            if self.both:
                self.sb[:, :, c] = (self.p[:, ak, :, c].astype(F32) + self.x1[:, :, c].astype(F32)).astype(BF16)
            else:
                self.sb[0, :, c] = (self.p[1 - ax, ak, :, c].astype(F32) + self.x1[1 - ax, :, c].astype(F32)).astype(BF16)
            self.over(n).start()

        def run(self, fn, lag, also=None):
            for n in range(RSC):
                self.produce(n, fn(self.cols(n)))
                if n >= lag:
                    self.relay(n - lag)
                if also is not None:
                    also(n)

        def relay_from(self, first):
            for n in range(first, RSC):
                self.relay(n)

        def arrive(self):
            for n in range(RSC):
                self.over(n).wait_recv()

        def block(self, b):
            return (self.sb[b].astype(F32) + self.x2[b].astype(F32)).astype(BF16).astype(F32)

        def own(self):
            v = self.p[ax, ak].astype(F32) + self.x1[ax].astype(F32) + self.x2[0].astype(F32)
            return v.astype(BF16).astype(F32)

        def drain(self):
            for n in range(RSC):
                self.pair(n).wait_send()
                self.over(n).wait_send()

    gat_m = Gather(rbuf.at[1])
    sh_h, sh_g, sh_a = Share(rbuf.at[2]), Share(gbuf), Share(rbuf.at[3])
    sc_a, sc_g, sc_y, sc_h = Reduce(0, True), Reduce(1, True), Reduce(2, False), Reduce(3, False)
    blocks = ((ax, 0), (1 - ax, 1))
    outs = []

    def emit(src, dst):
        c = pltpu.make_async_copy(src, dst, osem.at[len(outs)])
        c.start()
        outs.append(c)

    sx, rx = alloc('s'), alloc('r')
    _ns('barrier')
    x_load.wait()
    pl.semaphore_wait(bar, 3)
    _ns('xsend')
    remote(xh.at[ax], xh.at[ax], sx, rx, cross).start()
    for c in loads:
        c.wait()
    bq[...] = jnp.concatenate([bqv[t, h:h + 1, :] for h in range(NH) for t in range(3)], axis=1)
    for b, i in blocks:
        if i == 1:
            remote(xh.at[1 - ax], xh.at[1 - ax], sx, rx, cross).wait_recv()
        xhat, rstd = ln_stats(xh[b].astype(F32))
        if i == 0:
            xn1[...] = xhat
            rs[2] = jnp.broadcast_to(rstd, (ROWS, 128))
        rbuf[2, block_rows(b), :] = (xhat * g1[...] + b1[...]).astype(BF16)
        sh_h.send(b, i)
    _ns('hshare')
    gy_load.wait()
    gat_m.start()
    wcopies[2].start()
    wcopies[3].start()
    wcopies[0].wait()
    for b, i in blocks:
        sh_h.finish(b, i)
    emit(rbuf.at[2], r_hbm.at[2])

    _ns('qkv')
    QC = 640

    def qkv_body(n, carry):
        r0 = pl.multiple_of(n * QC, QC)
        v = dot(rbuf[2], wq[pl.ds(r0, QC), :], NT) + bq[:, pl.ds(r0, QC)]
        qkvt[pl.ds(r0, QC), :] = v.astype(BF16).T
        return carry
    lax.fori_loop(0, QKV // QC, qkv_body, 0)

    _ns('attn')
    scale = HD ** -0.5
    jpos = lax.broadcasted_iota(jnp.int32, (SEQ, SEQ), 0)
    ipos = lax.broadcasted_iota(jnp.int32, (SEQ, SEQ), 1)
    causal = jpos <= ipos
    jf = jpos.astype(F32)
    base = jnp.where(me == 0, 1.0, jnp.where(me == 1, 0.25, jnp.where(me == 2, 0.0625, 0.015625))).astype(F32)

    def head(h, t):
        r0 = h * 3 * HD + t * HD
        return qkvt[r0:r0 + HD, :]

    for h in range(NH):
        s = dot(head(h, 1), head(h, 0), TN) * scale + (base * SLOPES[h]) * jf
        s = jnp.where(causal, s, MASK_VALUE)
        e = jnp.exp(s - jnp.max(s, axis=0, keepdims=True))
        p = e * (1.0 / jnp.sum(e, axis=0, keepdims=True))
        prob[h] = p
        lbuf[OFF_O + h * HD:OFF_O + (h + 1) * HD, :] = dot(head(h, 2), p.astype(BF16), NN).astype(BF16)
    for t in range(CTX // 128):
        ctx[:, t * 128:(t + 1) * 128] = lbuf[OFF_O + t * 128:OFF_O + (t + 1) * 128, :].T

    _ns('outproj')
    wcopies[1].wait()
    sc_a.run(lambda cols: dot(ctx[...], wo[:, cols], NN), 3)
    _ns('arelay')
    sc_a.relay_from(RSC - 3)

    _ns('gm_fwd')
    for c in range(AGC):
        gat_m.forward(c)
    wcopies[2].wait()
    gat_m.finish()
    emit(rbuf.at[1], r_hbm.at[1])
    _ns('dact')
    FC = 512

    def dact_body(n, carry):
        f0 = pl.multiple_of(n * FC, FC)
        dact[:, pl.ds(f0, FC)] = dot(rbuf[1], wd[pl.ds(f0, FC), :], NT).astype(BF16)
        return carry
    lax.fori_loop(0, FF // FC, dact_body, 0)

    _ns('a_wait')
    sc_a.arrive()
    _ns('ln2')
    for b, i in blocks:
        xm = xh[b].astype(F32) + sc_a.block(b) + bo[...]
        if i == 0:
            x1[...] = xm
        xhat, rstd = ln_stats(xm)
        xn2[b] = xhat
        rs[b] = jnp.broadcast_to(rstd, (ROWS, 128))
        gbuf[block_rows(b), :] = (xhat * g2[...] + b2[...]).astype(BF16)
        sh_g.send(b, i)
    _ns('g_share')
    wcopies[3].wait()
    for b, i in blocks:
        sh_g.finish(b, i)

    _ns('up')
    UC = 512
    k0 = 0.7978845608028654
    k1 = 0.044715

    for f0 in range(0, FF, UC):
        cols = pl.ds(f0, UC)
        v = dot(gbuf[...], wu[:, cols], NN) + bu[:, cols]
        v2 = v * v
        t = jnp.tanh(k0 * (v + k1 * (v2 * v)))
        hp = 0.5 * (1.0 + t)
        act[:, cols] = (v * hp).astype(BF16)
        dg = hp + (0.5 * k0) * v * (1.0 - t * t) * (1.0 + (3.0 * k1) * v2)
        dpre = dact[:, cols].astype(F32) * dg
        gbu[:, cols] = jnp.sum(dpre, axis=0, keepdims=True)
        rbuf[0, :, cols] = dpre.astype(BF16)
    emit(rbuf.at[0], r_hbm.at[0])
    emit(gbu, gbu_hbm)

    _ns('dg')
    def dg_chunk(cols):
        return dot(rbuf[0], wu[cols, :], NT)
    sc_g.run(dg_chunk, 1)

    _ns('down')
    def rest(n):
        if n == 1:
            sc_g.relay(RSC - 1)
    sc_y.run(lambda cols: dot(act[...], wd[:, cols], NN), RSC, rest)
    _ns('yrelay')
    sc_y.relay_from(0)

    _ns('vecy')
    va[me, 3:4, :] = jnp.sum(rbuf[1, rows(me), :].astype(F32), axis=0, keepdims=True)

    _ns('g_wait')
    sc_g.arrive()
    _ns('ln2b')
    for b, i in blocks:
        dgl = sc_g.block(b)
        xhat, rstd = xn2[b], rs[b, :, 0:1]
        dm = rbuf[1, block_rows(b), :].astype(F32) + ln_grad(dgl, xhat, rstd, g2[...])
        rbuf[3, block_rows(b), :] = dm.astype(BF16)
        sh_a.send(b, i)
        if i == 0:
            dmid[...] = dm
    va[me, 2:3, :] = jnp.sum(dmid[...], axis=0, keepdims=True)
    dgl = sc_g.block(ax)
    va[me, 0:1, :] = jnp.sum(dgl * xn2[ax], axis=0, keepdims=True)
    va[me, 1:2, :] = jnp.sum(dgl, axis=0, keepdims=True)

    sva, rva = alloc('s', 3), alloc('r', 3)

    def vec_copy(buf, s, r, i, owner, dev):
        return remote(buf.at[owner], buf.at[owner], s + i, r + i, dev)
    for i, dev in enumerate(peers):
        vec_copy(va, sva, rva, i, me, dev).start()
    _ns('a_share')
    for b, i in blocks:
        sh_a.finish(b, i)
    emit(rbuf.at[3], r_hbm.at[3])

    _ns('attnb')
    ctx[...] = dot(rbuf[3], wo[...], NT).astype(BF16)
    for t in range(CTX // 128):
        dctxt[t * 128:(t + 1) * 128, :] = ctx[:, t * 128:(t + 1) * 128].T

    for h in range(NH):
        dot_h = dctxt[h * HD:(h + 1) * HD, :]
        p = prob[h]
        dp = dot(head(h, 2), dot_h, TN).astype(BF16).astype(F32)
        ds = (p * (dp - jnp.sum(dp * p, axis=0, keepdims=True))).astype(BF16)
        r0 = OFF_QKV + h * 3 * HD
        lbuf[r0:r0 + HD, :] = (dot(head(h, 1), ds, NN) * scale).astype(BF16)
        lbuf[r0 + HD:r0 + 2 * HD, :] = (dot(head(h, 0), ds, NT) * scale).astype(BF16)
        lbuf[r0 + 2 * HD:r0 + 3 * HD, :] = dot(dot_h, p.astype(BF16), NT).astype(BF16)
    for t in range(QKV // 128):
        dqkv[:, t * 128:(t + 1) * 128] = lbuf[OFF_QKV + t * 128:OFF_QKV + (t + 1) * 128, :].T
    emit(lbuf.at[pl.ds(OFF_QKV, QKV + CTX)], l_hbm.at[pl.ds(OFF_QKV, QKV + CTX)])

    _ns('dh')
    sc_h.run(lambda cols: dot(dqkv[...], wq[:, cols], NN), 2)
    _ns('hrelay')
    sc_h.relay_from(RSC - 2)

    _ns('y')
    sc_y.arrive()
    outb[0] = (x1[...] + sc_y.own() + bd[...]).astype(BF16)
    emit(outb.at[0], y_hbm)
    for i, dev in enumerate(peers):
        vec_copy(va, sva, rva, i, dev, dev).wait_recv()
    tot = (va[0] + va[1]) + (va[2] + va[3])
    for i in range(4):
        vo[i] = tot[i:i + 1]

    _ns('transp')
    def tr_body(src, off):
        def body(n, carry):
            r0 = pl.multiple_of(n * 128, 128)
            lbuf[pl.ds(off + r0, 128), :] = src[:, pl.ds(r0, 128)].T
            return carry
        return body
    lax.fori_loop(0, FF // 128, tr_body(act, OFF_ACT), 0)
    lax.fori_loop(0, D // 128, tr_body(gbuf, OFF_G), 0)
    emit(lbuf.at[pl.ds(0, OFF_QKV)], l_hbm.at[pl.ds(0, OFF_QKV)])

    _ns('h_wait')
    sc_h.arrive()
    _ns('ln1b')
    dhl = sc_h.own()
    xhat1, rstd1 = xn1[...], rs[2, :, 0:1]
    vb[me, 0:1, :] = jnp.sum(dhl * xhat1, axis=0, keepdims=True)
    vb[me, 1:2, :] = jnp.sum(dhl, axis=0, keepdims=True)
    svb, rvb = alloc('s', 3), alloc('r', 3)
    for i, dev in enumerate(peers):
        vec_copy(vb, svb, rvb, i, me, dev).start()
    outb[1] = (dmid[...] + ln_grad(dhl, xhat1, rstd1, g1[...])).astype(BF16)
    emit(outb.at[1], gx_hbm)
    _ns('drain')
    remote(xh.at[ax], xh.at[ax], sx, rx, cross).wait_send()
    gat_m.drain()
    for g in (sh_h, sh_g, sh_a, sc_a, sc_g, sc_y, sc_h):
        g.drain()
    for i, dev in enumerate(peers):
        vec_copy(va, sva, rva, i, me, dev).wait_send()
    _ns('vecwait')
    for i, dev in enumerate(peers):
        vec_copy(vb, svb, rvb, i, dev, dev).wait_recv()
    tot = (vb[0] + vb[1]) + (vb[2] + vb[3])
    for i in range(2):
        vo[4 + i] = tot[i:i + 1]
    _ns('final')
    emit(vo, vec_hbm)
    for i, dev in enumerate(peers):
        vec_copy(vb, svb, rvb, i, me, dev).wait_send()
    for c in outs:
        c.wait()
    _ns(None)
    assert max(count.values()) <= NSEM


GR = 640
SLOTS = 4
SECTIONS = ((OFF_ACT, FF, 1), (OFF_G, D, 0), (OFF_QKV, QKV, 2), (OFF_O, CTX, 3))
PIECES = (((160, 1), (160, 1), (320, 1), (GR, 3)), ((GR, 4),), ((GR, 3),), ((320, 1), (160, 1), (160, 1)))
SMALL = 6


def grad_kernel(y_in, gx_in, vec_in, gbu_in, l_hbm, r_hbm, y_out, gx_out, v0, v1, v2, v3, v4, v5, gbq_hbm, gbu_out,
                dwq, dwo, dwu, dwd, lv, rv, st, st2, yv, gxv, vv, gv, gbq, isem, ssem, ssem2, psem, osem):
    _cur = []

    def _ns(name):
        if _cur:
            _cur.pop().__exit__(None, None, None)
        if name:
            _cur.append(jax.named_scope(name))
            _cur[-1].__enter__()
    _ns('b_start')
    loads = []
    for i, (off, n, r) in enumerate(SECTIONS):
        cl = pltpu.make_async_copy(l_hbm.at[pl.ds(off, n)], lv.at[pl.ds(off, n)], isem.at[2 * i])
        cr = pltpu.make_async_copy(r_hbm.at[r], rv.at[r], isem.at[2 * i + 1])
        cl.start()
        cr.start()
        loads.append((cl, cr))
    passes = [(y_in, yv, y_out), (gx_in, gxv, gx_out), (gbu_in, gv, gbu_out)]
    srcs = (yv, gxv, gv.at[0])
    pin = [pltpu.make_async_copy(a, b, psem.at[i]) for i, (a, b, _) in enumerate(passes)]
    pin.append(pltpu.make_async_copy(vec_in, vv, psem.at[3]))
    for c in pin:
        c.start()
    douts = (dwd, dwu, dwq, dwo)
    step = 0

    def out_copy(slot, dst, r0):
        return pltpu.make_async_copy(st.at[slot], dst.at[pl.ds(r0, GR)], ssem.at[slot])
    smalls = []
    for i, (off, n, r) in enumerate(SECTIONS):
        _ns('b_load%d' % i)
        loads[i][0].wait()
        loads[i][1].wait()
        dst = douts[i]
        _ns('b_sec%d' % i)
        r0 = 0
        for gr, times in PIECES[i]:
            if gr < GR:
                e = len(smalls)

                def small(m, carry, off=off + r0, gr=gr, e=e, r=r):
                    st2[e, 0:gr] = dot(lv[pl.ds(pl.multiple_of(off + m * gr, 32), gr), :], rv[r], NN).astype(BF16)
                    return carry
                lax.fori_loop(0, 1, small, 0)
                smalls.append(pltpu.make_async_copy(st2.at[e, pl.ds(0, gr)], dst.at[pl.ds(r0, gr)], ssem2.at[e]))
                smalls[-1].start()
            else:
                def body(m, carry, off=off + r0, r=r, dst=dst, step=step, r0=r0):
                    slot = lax.rem(m + step, SLOTS)

                    @pl.when(m + step >= SLOTS)
                    def _():
                        out_copy(slot, dwd, 0).wait()
                    st[slot] = dot(lv[pl.ds(pl.multiple_of(off + m * GR, 64), GR), :], rv[r], NN).astype(BF16)
                    out_copy(slot, dst, pl.multiple_of(r0 + m * GR, 64)).start()
                    return carry
                lax.fori_loop(0, times, body, 0)
                step += times
            r0 += gr * times
        if i == 2:
            ones = jnp.ones((16, SEQ), BF16)
            for h in range(NH):
                for t in range(3):
                    q0 = OFF_QKV + h * 3 * HD + t * HD
                    gbq[t, h:h + 1, :] = dot(ones, lv[q0:q0 + HD, :], NT)[0:1]
    _ns('b_tail')
    for c in pin:
        c.wait()
    done = []
    for i, (_, _, o) in enumerate(passes):
        done.append(pltpu.make_async_copy(srcs[i], o, osem.at[i]))
    for i, o in enumerate((v0, v1, v2, v3, v4, v5)):
        done.append(pltpu.make_async_copy(vv.at[i, 0], o, osem.at[3 + i]))
    done.append(pltpu.make_async_copy(gbq, gbq_hbm, osem.at[9]))
    for c in done:
        c.start()
    _ns('b_flush')
    for slot in range(SLOTS):
        out_copy(slot, dwd, 0).wait()
    for c in smalls:
        c.wait()
    for c in done:
        c.wait()
    _ns(None)


def solution(mesh):
    def local_step(x, ln1_gamma, ln1_beta, w_qkv, b_qkv, w_out, b_out, ln2_gamma, ln2_beta, w_up, b_up, w_down, b_down, grad_y):
        wqt = jnp.transpose(w_qkv, (1, 2, 3, 0)).reshape(QKV, D)
        any_spec = pl.BlockSpec(memory_space=pl.ANY)
        sds = jax.ShapeDtypeStruct
        y, gx, vec, gbu, lmat, rmat = pl.pallas_call(
            block_kernel,
            name='block',
            out_shape=(sds((ROWS, D), BF16), sds((ROWS, D), BF16), sds((6, 1, D), F32), sds((1, FF), F32),
                       sds((LROWS, SEQ), BF16), sds((4, SEQ, D), BF16)),
            in_specs=[any_spec] * 14,
            out_specs=(any_spec,) * 6,
            scratch_shapes=[
                pltpu.VMEM((QKV, D), BF16), pltpu.VMEM((CTX, D), BF16), pltpu.VMEM((D, FF), BF16), pltpu.VMEM((FF, D), BF16),
                pltpu.VMEM((2, ROWS, D), BF16),
                pltpu.VMEM((1, D), F32), pltpu.VMEM((1, D), F32), pltpu.VMEM((3, NH, HD), F32), pltpu.VMEM((1, QKV), F32),
                pltpu.VMEM((1, D), F32), pltpu.VMEM((1, D), F32), pltpu.VMEM((1, D), F32), pltpu.VMEM((1, FF), F32), pltpu.VMEM((1, D), F32),
                pltpu.VMEM((4, SEQ, D), BF16), pltpu.VMEM((LROWS, SEQ), BF16), pltpu.VMEM((SEQ, D), BF16),
                pltpu.VMEM((QKV, SEQ), BF16), pltpu.VMEM((SEQ, QKV), BF16), pltpu.VMEM((SEQ, CTX), BF16),
                pltpu.VMEM((CTX, SEQ), BF16), pltpu.VMEM((NH, SEQ, SEQ), F32),
                pltpu.VMEM((SEQ, FF), BF16), pltpu.VMEM((SEQ, FF), BF16),
                pltpu.VMEM((ROWS, D), F32), pltpu.VMEM((ROWS, D), F32), pltpu.VMEM((2, ROWS, D), F32), pltpu.VMEM((3, ROWS, 128), F32),
                pltpu.VMEM((ROWS, D), F32), pltpu.VMEM((2, ROWS, D), BF16),
                pltpu.VMEM((1, FF), F32),
                pltpu.VMEM((TP, 4, D), F32), pltpu.VMEM((TP, 2, D), F32), pltpu.VMEM((6, 1, D), F32),
                pltpu.VMEM((4, 2, 2, ROWS, D), BF16), pltpu.VMEM((4, 2, ROWS, D), BF16),
                pltpu.VMEM((4, 2, ROWS, D), BF16), pltpu.VMEM((4, 2, ROWS, D), BF16),
                pltpu.SemaphoreType.DMA((4,)), pltpu.SemaphoreType.DMA((10,)), pltpu.SemaphoreType.DMA((10,)),
                pltpu.SemaphoreType.DMA((NSEM,)), pltpu.SemaphoreType.DMA((NSEM,)),
            ],
            compiler_params=pltpu.CompilerParams(collective_id=0, has_side_effects=True, vmem_limit_bytes=66_000_000),
            cost_estimate=pl.CostEstimate(flops=10_000_000_000, bytes_accessed=45_000_000, transcendentals=1_000_000),
        )(x[0], grad_y[0], wqt, w_out, w_up, w_down, ln1_gamma, ln1_beta, jnp.transpose(b_qkv, (1, 0, 2)), b_out,
          ln2_gamma, ln2_beta, b_up, b_down)
        y, gx, v0, v1, v2, v3, v4, v5, gbq, gbu, dwq, dwo, dwu, dwd = pl.pallas_call(
            grad_kernel,
            name='weight_grads',
            out_shape=(sds((ROWS, D), BF16), sds((ROWS, D), BF16)) + (sds((D,), F32),) * 6 + (
                sds((3, NH, HD), F32), sds((FF,), F32), sds((QKV, D), BF16), sds((CTX, D), BF16), sds((D, FF), BF16), sds((FF, D), BF16)),
            in_specs=[any_spec] * 6,
            out_specs=(any_spec,) * 14,
            scratch_shapes=[
                pltpu.VMEM((LROWS, SEQ), BF16), pltpu.VMEM((4, SEQ, D), BF16), pltpu.VMEM((SLOTS, GR, D), BF16), pltpu.VMEM((SMALL, 320, D), BF16),
                pltpu.VMEM((ROWS, D), BF16), pltpu.VMEM((ROWS, D), BF16), pltpu.VMEM((6, 1, D), F32), pltpu.VMEM((1, FF), F32),
                pltpu.VMEM((3, NH, HD), F32),
                pltpu.SemaphoreType.DMA((8,)), pltpu.SemaphoreType.DMA((SLOTS,)), pltpu.SemaphoreType.DMA((SMALL,)), pltpu.SemaphoreType.DMA((4,)), pltpu.SemaphoreType.DMA((10,)),
            ],
            compiler_params=pltpu.CompilerParams(vmem_limit_bytes=66_000_000),
            cost_estimate=pl.CostEstimate(flops=5_000_000_000, bytes_accessed=44_000_000, transcendentals=0),
        )(y, gx, vec, gbu, lmat, rmat)
        g_wqkv = jnp.transpose(dwq.reshape(NH, 3, HD, D), (3, 0, 1, 2))
        g_ln2g, g_ln2b, g_bo, g_bd, g_ln1g, g_ln1b = v0, v1, v2, v3, v4, v5
        return (y[None], gx[None], g_ln1g, g_ln1b, g_wqkv, jnp.transpose(gbq, (1, 0, 2)), dwo, g_bo,
                g_ln2g, g_ln2b, dwu, gbu, dwd, g_bd)

    row_spec = P('dp', 'tp', None)
    in_specs = (row_spec, P(), P(), P(None, 'tp', None, None), P('tp', None, None), P('tp', None), P(), P(), P(),
                P(None, 'tp'), P('tp'), P('tp', None), P(), row_spec)
    out_specs = (row_spec, row_spec, P('dp'), P('dp'), P('dp', 'tp', None, None), P(('dp', 'tp'), None, None),
                 P(('dp', 'tp'), None), P('dp'), P('dp'), P('dp'), P('dp', 'tp'), P(('dp', 'tp')), P(('dp', 'tp'), None), P('dp'))
    return jax.shard_map(local_step, mesh=mesh, in_specs=in_specs, out_specs=out_specs, check_vma=False)
```

```python
import jax
import jax.numpy as jnp
from jax import lax
from jax.experimental import pallas as pl
from jax.experimental.pallas import tpu as pltpu
from jax.sharding import PartitionSpec as P

EPS = 1e-5
MASK_VALUE = -1e30
MESH = pl.DeviceIdType.MESH
F32 = jnp.float32
BF16 = jnp.bfloat16

D = 2560
SEQ = 128
TP = 4
ROWS = SEQ // TP
NH = 8
HD = 80
QKV = NH * 3 * HD
CTX = NH * HD
FF = 2560
AGC = 4
NSEM = 80
AGW = D // AGC
CHUNKS = (256, 256, 512, 512, 512, 256, 256)
Y_CHUNKS = (640,) * 4
OFF_G, OFF_ACT, OFF_QKV, OFF_O = 0, D, D + FF, D + FF + QKV
LROWS = D + FF + QKV + CTX
SLOPES = [2.0 ** (-(h + 1) / 4.0) for h in range(NH)]
NT = (((1,), (1,)), ((), ()))
NN = (((1,), (0,)), ((), ()))
TN = (((0,), (0,)), ((), ()))


def dot(a, b, dims):
    return lax.dot_general(a, b, dims, preferred_element_type=F32)


def ln_stats(v):
    mean = jnp.mean(v, axis=-1, keepdims=True)
    cen = v - mean
    var = jnp.mean(cen * cen, axis=-1, keepdims=True)
    rstd = lax.rsqrt(var + EPS)
    return cen * rstd, rstd


def ln_grad(dy, xhat, rstd, gain):
    dxh = dy * gain
    m1 = jnp.mean(dxh, axis=-1, keepdims=True)
    m2 = jnp.mean(dxh * xhat, axis=-1, keepdims=True)
    return rstd * (dxh - m1 - xhat * m2)


def block_kernel(x_hbm, gy_hbm, wq_hbm, wo_hbm, wu_hbm, wd_hbm, g1_hbm, b1_hbm, bq_hbm, bo_hbm, g2_hbm, b2_hbm, bu_hbm,
                 bd_hbm, y_hbm, gx_hbm, va_hbm, vb_hbm, gbu_hbm, l_hbm, r_hbm,
                 wq, wo, wu, wd, xh, g1, b1, bqv, bq, bo, g2, b2, bu, bd,
                 rbuf, lbuf, gbuf, qkvt, dqkv, ctx, dctxt, prob, act, dact, x1, xn1, xn2, rs, dmid, outb, gbu, va, vb,
                 pb, rx1, sb, rx2, wsem, lsem, osem, ssem, rsem):
    me = lax.axis_index('tp')
    ax = lax.div(me, 2)
    ak = lax.rem(me, 2)
    partner = 2 * ax + (1 - ak)
    cross = 2 * (1 - ax) + ak
    diag = 2 * (1 - ax) + (1 - ak)
    peers = (partner, cross, diag)

    def rows(i):
        return pl.ds(pl.multiple_of(i * ROWS, ROWS), ROWS)

    def block_rows(b):
        return rows(2 * b + ak)

    count = {'s': 0, 'r': 0}
    _cur = []

    def _ns(name):
        if _cur:
            _cur.pop().__exit__(None, None, None)
        if name:
            _cur.append(jax.named_scope(name))
            _cur[-1].__enter__()
    _ns('start')

    def alloc(kind, n=1):
        base = count[kind]
        count[kind] += n
        return base

    def remote(src, dst, si, ri, dev):
        return pltpu.make_async_remote_copy(src_ref=src, dst_ref=dst, send_sem=ssem.at[si], recv_sem=rsem.at[ri],
                                            device_id={'tp': dev}, device_id_type=MESH)

    x_load = pltpu.make_async_copy(x_hbm, xh.at[ax], lsem.at[0])
    x_load.start()
    small = [(g1_hbm, g1.at[0]), (b1_hbm, b1.at[0]), (bq_hbm, bqv), (bo_hbm, bo.at[0]), (g2_hbm, g2.at[0]), (b2_hbm, b2.at[0]),
             (bu_hbm, bu.at[0]), (bd_hbm, bd.at[0])]
    loads = [pltpu.make_async_copy(s, d, lsem.at[1 + i]) for i, (s, d) in enumerate(small)]
    for c in loads:
        c.start()
    gy_load = pltpu.make_async_copy(gy_hbm, rbuf.at[1, rows(me)], lsem.at[1 + len(small)])
    gy_load.start()
    wcopies = [pltpu.make_async_copy(s, d, wsem.at[i])
               for i, (s, d) in enumerate([(wq_hbm, wq), (wo_hbm, wo), (wd_hbm, wd), (wu_hbm, wu)])]

    bar = pltpu.get_barrier_semaphore()
    for dev in peers:
        pl.semaphore_signal(bar, inc=1, device_id={'tp': dev}, device_id_type=MESH)
    wcopies[0].start()
    wcopies[1].start()

    class Gather:
        def __init__(self, full):
            self.full = full
            self.s = alloc('s', 2 * AGC + 1)
            self.r = alloc('r', 2 * AGC + 1)

        def chunk(self, dev, c):
            return self.full.at[rows(dev), pl.ds(c * AGW, AGW)]

        def cross_copy(self, dev, c):
            ref = self.chunk(dev, c)
            return remote(ref, ref, self.s + c, self.r + c, cross)

        def fwd_copy(self, dev, c):
            ref = self.chunk(dev, c)
            return remote(ref, ref, self.s + AGC + c, self.r + AGC + c, partner)

        def own_copy(self, dev):
            ref = self.full.at[rows(dev)]
            return remote(ref, ref, self.s + 2 * AGC, self.r + 2 * AGC, partner)

        def start(self):
            for c in range(AGC):
                self.cross_copy(me, c).start()
            self.own_copy(me).start()

        def forward(self, c):
            self.cross_copy(cross, c).wait_recv()
            self.fwd_copy(cross, c).start()

        def finish(self):
            self.own_copy(partner).wait_recv()
            for c in range(AGC):
                self.fwd_copy(diag, c).wait_recv()

        def drain(self):
            for c in range(AGC):
                self.cross_copy(me, c).wait_send()
                self.fwd_copy(cross, c).wait_send()
            self.own_copy(me).wait_send()

    class Share:
        def __init__(self, full):
            self.full = full
            self.s = alloc('s', 2)
            self.r = alloc('r', 2)

        def copy(self, b, k, i):
            ref = self.full.at[rows(2 * b + k)]
            return remote(ref, ref, self.s + i, self.r + i, partner)

        def send(self, b, i):
            self.copy(b, ak, i).start()

        def finish(self, b, i):
            self.copy(b, 1 - ak, i).wait_recv()

        def drain(self):
            self.copy(ax, ak, 0).wait_send()
            self.copy(1 - ax, ak, 1).wait_send()

    class Reduce:
        def __init__(self, i, both, chunks=CHUNKS):
            self.p, self.x1, self.sb, self.x2 = pb.at[i], rx1.at[i], sb.at[i], rx2.at[i]
            self.both = both
            self.chunks = chunks
            self.n = len(chunks)
            self.s = alloc('s', 2 * self.n)
            self.r = alloc('r', 2 * self.n)

        def cols(self, n):
            return pl.ds(sum(self.chunks[:n]), self.chunks[n])

        def pair(self, n):
            return remote(self.p.at[:, 1 - ak, :, self.cols(n)], self.x1.at[:, :, self.cols(n)], self.s + n, self.r + n, partner)

        def over(self, n):
            if self.both:
                src, dst = self.sb.at[:, :, self.cols(n)], self.x2.at[:, :, self.cols(n)]
            else:
                src, dst = self.sb.at[0, :, self.cols(n)], self.x2.at[0, :, self.cols(n)]
            return remote(src, dst, self.s + self.n + n, self.r + self.n + n, cross)

        def produce(self, n, val):
            self.p[:, :, :, self.cols(n)] = val.astype(BF16).reshape(2, 2, ROWS, self.chunks[n])
            self.pair(n).start()

        def relay(self, n):
            self.pair(n).wait_recv()
            c = self.cols(n)
            if self.both:
                self.sb[:, :, c] = (self.p[:, ak, :, c].astype(F32) + self.x1[:, :, c].astype(F32)).astype(BF16)
            else:
                self.sb[0, :, c] = (self.p[1 - ax, ak, :, c].astype(F32) + self.x1[1 - ax, :, c].astype(F32)).astype(BF16)
            self.over(n).start()

        def run(self, fn, lag, also=None):
            for n in range(self.n):
                self.produce(n, fn(self.cols(n)))
                if n >= lag:
                    self.relay(n - lag)
                if also is not None:
                    also(n)

        def relay_from(self, first):
            for n in range(first, self.n):
                self.relay(n)

        def arrive(self):
            for n in range(self.n):
                self.over(n).wait_recv()

        def block(self, b):
            return (self.sb[b].astype(F32) + self.x2[b].astype(F32)).astype(BF16).astype(F32)

        def own(self):
            v = self.p[ax, ak].astype(F32) + self.x1[ax].astype(F32) + self.x2[0].astype(F32)
            return v.astype(BF16).astype(F32)

        def drain(self):
            for n in range(self.n):
                self.pair(n).wait_send()
                self.over(n).wait_send()

    gat_m = Gather(rbuf.at[1])
    sh_h, sh_g, sh_a = Share(rbuf.at[2]), Share(gbuf), Share(rbuf.at[3])
    sc_a, sc_g, sc_y, sc_h = Reduce(0, True), Reduce(1, True), Reduce(2, False, Y_CHUNKS), Reduce(3, False)
    blocks = ((ax, 0), (1 - ax, 1))
    outs = []

    def emit(src, dst):
        c = pltpu.make_async_copy(src, dst, osem.at[len(outs)])
        c.start()
        outs.append(c)

    sx, rx = alloc('s'), alloc('r')
    _ns('barrier')
    x_load.wait()
    pl.semaphore_wait(bar, 3)
    _ns('xsend')
    remote(xh.at[ax], xh.at[ax], sx, rx, cross).start()
    for c in loads:
        c.wait()
    bq[...] = jnp.concatenate([bqv[t, h:h + 1, :] for h in range(NH) for t in range(3)], axis=1)
    for b, i in blocks:
        if i == 1:
            remote(xh.at[1 - ax], xh.at[1 - ax], sx, rx, cross).wait_recv()
        xhat, rstd = ln_stats(xh[b].astype(F32))
        if i == 0:
            xn1[...] = xhat
            rs[2] = jnp.broadcast_to(rstd, (ROWS, 128))
        rbuf[2, block_rows(b), :] = (xhat * g1[...] + b1[...]).astype(BF16)
        sh_h.send(b, i)
    _ns('hshare')
    gy_load.wait()
    gat_m.start()
    wcopies[2].start()
    wcopies[3].start()
    wcopies[0].wait()
    for b, i in blocks:
        sh_h.finish(b, i)
    emit(rbuf.at[2], r_hbm.at[2])

    _ns('qkv')
    QC = 640

    def qkv_body(n, carry):
        r0 = pl.multiple_of(n * QC, QC)
        v = dot(rbuf[2], wq[pl.ds(r0, QC), :], NT) + bq[:, pl.ds(r0, QC)]
        qkvt[pl.ds(r0, QC), :] = v.astype(BF16).T
        return carry
    lax.fori_loop(0, QKV // QC, qkv_body, 0)

    _ns('attn')
    scale = HD ** -0.5
    jpos = lax.broadcasted_iota(jnp.int32, (SEQ, SEQ), 0)
    ipos = lax.broadcasted_iota(jnp.int32, (SEQ, SEQ), 1)
    causal = jpos <= ipos
    jf = jpos.astype(F32)
    base = jnp.where(me == 0, 1.0, jnp.where(me == 1, 0.25, jnp.where(me == 2, 0.0625, 0.015625))).astype(F32)

    def head(h, t):
        r0 = h * 3 * HD + t * HD
        return qkvt[r0:r0 + HD, :]

    for h in range(NH):
        s = dot(head(h, 1), head(h, 0), TN) * scale + (base * SLOPES[h]) * jf
        s = jnp.where(causal, s, MASK_VALUE)
        e = jnp.exp(s - jnp.max(s, axis=0, keepdims=True))
        p = e * (1.0 / jnp.sum(e, axis=0, keepdims=True))
        prob[h] = p
        lbuf[OFF_O + h * HD:OFF_O + (h + 1) * HD, :] = dot(head(h, 2), p.astype(BF16), NN).astype(BF16)
    for t in range(CTX // 128):
        ctx[:, t * 128:(t + 1) * 128] = lbuf[OFF_O + t * 128:OFF_O + (t + 1) * 128, :].T

    _ns('outproj')
    wcopies[1].wait()
    sc_a.run(lambda cols: dot(ctx[...], wo[:, cols], NN), 3)
    _ns('arelay')
    sc_a.relay_from(sc_a.n - 3)

    _ns('gm_fwd')
    for c in range(AGC):
        gat_m.forward(c)
    wcopies[2].wait()
    gat_m.finish()
    emit(rbuf.at[1], r_hbm.at[1])
    _ns('dact')
    FC = 512

    def dact_body(n, carry):
        f0 = pl.multiple_of(n * FC, FC)
        dact[:, pl.ds(f0, FC)] = dot(rbuf[1], wd[pl.ds(f0, FC), :], NT).astype(BF16)
        return carry
    lax.fori_loop(0, FF // FC, dact_body, 0)

    _ns('a_wait')
    sc_a.arrive()
    _ns('ln2')
    for b, i in blocks:
        xm = xh[b].astype(F32) + sc_a.block(b) + bo[...]
        if i == 0:
            x1[...] = xm
        xhat, rstd = ln_stats(xm)
        xn2[b] = xhat
        rs[b] = jnp.broadcast_to(rstd, (ROWS, 128))
        gbuf[block_rows(b), :] = (xhat * g2[...] + b2[...]).astype(BF16)
        sh_g.send(b, i)
    _ns('g_share')
    wcopies[3].wait()
    for b, i in blocks:
        sh_g.finish(b, i)

    _ns('up')
    UC = 512
    k0 = 0.7978845608028654
    k1 = 0.044715

    for f0 in range(0, FF, UC):
        cols = pl.ds(f0, UC)
        v = dot(gbuf[...], wu[:, cols], NN) + bu[:, cols]
        v2 = v * v
        t = jnp.tanh(k0 * (v + k1 * (v2 * v)))
        hp = 0.5 * (1.0 + t)
        act[:, cols] = (v * hp).astype(BF16)
        dg = hp + (0.5 * k0) * v * (1.0 - t * t) * (1.0 + (3.0 * k1) * v2)
        dpre = dact[:, cols].astype(F32) * dg
        gbu[:, cols] = jnp.sum(dpre, axis=0, keepdims=True)
        rbuf[0, :, cols] = dpre.astype(BF16)
    emit(rbuf.at[0], r_hbm.at[0])
    emit(gbu, gbu_hbm)

    _ns('dg')
    def dg_chunk(cols):
        return dot(rbuf[0], wu[cols, :], NT)
    sc_g.run(dg_chunk, 1)

    _ns('down')
    def rest(n):
        if n == 0:
            sc_g.relay(sc_g.n - 1)
    sc_y.run(lambda cols: dot(act[...], wd[:, cols], NN), sc_y.n, rest)
    va[3:4, :] = jnp.sum(rbuf[1, rows(me), :].astype(F32), axis=0, keepdims=True)

    _ns('g_wait')
    sc_g.arrive()
    _ns('ln2b')
    for b, i in blocks:
        dgl = sc_g.block(b)
        xhat, rstd = xn2[b], rs[b, :, 0:1]
        dm = rbuf[1, block_rows(b), :].astype(F32) + ln_grad(dgl, xhat, rstd, g2[...])
        rbuf[3, block_rows(b), :] = dm.astype(BF16)
        sh_a.send(b, i)
        if i == 0:
            dmid[...] = dm
    va[2:3, :] = jnp.sum(dmid[...], axis=0, keepdims=True)
    dgl = sc_g.block(ax)
    va[0:1, :] = jnp.sum(dgl * xn2[ax], axis=0, keepdims=True)
    va[1:2, :] = jnp.sum(dgl, axis=0, keepdims=True)

    sva, rva = alloc('s', 3), alloc('r', 3)

    def vec_copy(buf, hbm, s, r, i, owner, dev):
        return remote(buf, hbm.at[owner], s + i, r + i, dev)
    _ns('yrelay')
    sc_y.relay_from(0)
    for i, dev in enumerate(peers):
        vec_copy(va, va_hbm, sva, rva, i, me, dev).start()
    emit(va, va_hbm.at[me])
    _ns('a_share')
    for b, i in blocks:
        sh_a.finish(b, i)
    emit(rbuf.at[3], r_hbm.at[3])

    _ns('attnb')
    ctx[...] = dot(rbuf[3], wo[...], NT).astype(BF16)
    for t in range(CTX // 128):
        dctxt[t * 128:(t + 1) * 128, :] = ctx[:, t * 128:(t + 1) * 128].T

    for h in range(NH):
        dot_h = dctxt[h * HD:(h + 1) * HD, :]
        p = prob[h]
        dp = dot(head(h, 2), dot_h, TN).astype(BF16).astype(F32)
        ds = (p * (dp - jnp.sum(dp * p, axis=0, keepdims=True))).astype(BF16)
        r0 = OFF_QKV + h * 3 * HD
        lbuf[r0:r0 + HD, :] = (dot(head(h, 1), ds, NN) * scale).astype(BF16)
        lbuf[r0 + HD:r0 + 2 * HD, :] = (dot(head(h, 0), ds, NT) * scale).astype(BF16)
        lbuf[r0 + 2 * HD:r0 + 3 * HD, :] = dot(dot_h, p.astype(BF16), NT).astype(BF16)
    for t in range(QKV // 128):
        dqkv[:, t * 128:(t + 1) * 128] = lbuf[OFF_QKV + t * 128:OFF_QKV + (t + 1) * 128, :].T
    emit(lbuf.at[pl.ds(OFF_QKV, QKV + CTX)], l_hbm.at[pl.ds(OFF_QKV, QKV + CTX)])

    _ns('dh')
    sc_h.run(lambda cols: dot(dqkv[...], wq[:, cols], NN), 2)
    _ns('hrelay')
    sc_h.relay_from(sc_h.n - 2)

    _ns('y')
    sc_y.arrive()
    outb[0] = (x1[...] + sc_y.own() + bd[...]).astype(BF16)
    emit(outb.at[0], y_hbm)
    _ns('transp')
    def tr_body(src, off):
        def body(n, carry):
            r0 = pl.multiple_of(n * 512, 512)
            lbuf[pl.ds(off + r0, 512), :] = src[:, pl.ds(r0, 512)].T
            return carry
        return body
    lax.fori_loop(0, FF // 512, tr_body(act, OFF_ACT), 0)
    lax.fori_loop(0, D // 512, tr_body(gbuf, OFF_G), 0)
    emit(lbuf.at[pl.ds(0, OFF_QKV)], l_hbm.at[pl.ds(0, OFF_QKV)])

    _ns('h_wait')
    sc_h.arrive()
    _ns('ln1b')
    dhl = sc_h.own()
    xhat1, rstd1 = xn1[...], rs[2, :, 0:1]
    vb[0:1, :] = jnp.sum(dhl * xhat1, axis=0, keepdims=True)
    vb[1:2, :] = jnp.sum(dhl, axis=0, keepdims=True)
    svb, rvb = alloc('s', 3), alloc('r', 3)
    for i, dev in enumerate(peers):
        vec_copy(vb, vb_hbm, svb, rvb, i, me, dev).start()
    emit(vb, vb_hbm.at[me])
    outb[1] = (dmid[...] + ln_grad(dhl, xhat1, rstd1, g1[...])).astype(BF16)
    emit(outb.at[1], gx_hbm)
    _ns('drain')
    remote(xh.at[ax], xh.at[ax], sx, rx, cross).wait_send()
    gat_m.drain()
    for g in (sh_h, sh_g, sh_a, sc_a, sc_g, sc_y, sc_h):
        g.drain()
    for i, dev in enumerate(peers):
        vec_copy(va, va_hbm, sva, rva, i, me, dev).wait_send()
        vec_copy(va, va_hbm, sva, rva, i, dev, dev).wait_recv()
    _ns('vecwait')
    for i, dev in enumerate(peers):
        vec_copy(vb, vb_hbm, svb, rvb, i, dev, dev).wait_recv()
    for i, dev in enumerate(peers):
        vec_copy(vb, vb_hbm, svb, rvb, i, me, dev).wait_send()
    for c in outs:
        c.wait()
    _ns(None)
    assert max(count.values()) <= NSEM


GR = 640
SLOTS = 4
SECTIONS = ((OFF_ACT, FF, 1), (OFF_G, D, 0), (OFF_QKV, QKV, 2), (OFF_O, CTX, 3))
PIECES = (((160, 1), (160, 1), (320, 1), (GR, 3)), ((GR, 4),), ((GR, 3),), ((320, 1), (160, 1), (160, 1)))
SMALL = 6


def grad_kernel(y_in, gx_in, va_in, vb_in, gbu_in, l_hbm, r_hbm, y_out, gx_out, v0, v1, v2, v3, v4, v5, gbq_hbm, gbu_out,
                dwq, dwo, dwu, dwd, lv, rv, st, st2, yv, gxv, vav, vbv, vv, gv, gbq, isem, ssem, ssem2, psem, osem):
    _cur = []

    def _ns(name):
        if _cur:
            _cur.pop().__exit__(None, None, None)
        if name:
            _cur.append(jax.named_scope(name))
            _cur[-1].__enter__()
    _ns('b_start')
    loads = []
    for i, (off, n, r) in enumerate(SECTIONS):
        cl = pltpu.make_async_copy(l_hbm.at[pl.ds(off, n)], lv.at[pl.ds(off, n)], isem.at[2 * i])
        cr = pltpu.make_async_copy(r_hbm.at[r], rv.at[r], isem.at[2 * i + 1])
        cl.start()
        cr.start()
        loads.append((cl, cr))
    passes = [(y_in, yv, y_out), (gx_in, gxv, gx_out), (gbu_in, gv, gbu_out)]
    srcs = (yv, gxv, gv.at[0])
    pin = [pltpu.make_async_copy(a, b, psem.at[i]) for i, (a, b, _) in enumerate(passes)]
    pin.append(pltpu.make_async_copy(va_in, vav, psem.at[3]))
    pin.append(pltpu.make_async_copy(vb_in, vbv, psem.at[4]))
    for c in pin:
        c.start()
    douts = (dwd, dwu, dwq, dwo)
    step = 0

    def out_copy(slot, dst, r0):
        return pltpu.make_async_copy(st.at[slot], dst.at[pl.ds(r0, GR)], ssem.at[slot])
    smalls = []
    for i, (off, n, r) in enumerate(SECTIONS):
        _ns('b_load%d' % i)
        loads[i][0].wait()
        loads[i][1].wait()
        dst = douts[i]
        _ns('b_sec%d' % i)
        r0 = 0
        for gr, times in PIECES[i]:
            if gr < GR:
                e = len(smalls)

                def small(m, carry, off=off + r0, gr=gr, e=e, r=r):
                    st2[e, 0:gr] = dot(lv[pl.ds(pl.multiple_of(off + m * gr, 32), gr), :], rv[r], NN).astype(BF16)
                    return carry
                lax.fori_loop(0, 1, small, 0)
                smalls.append(pltpu.make_async_copy(st2.at[e, pl.ds(0, gr)], dst.at[pl.ds(r0, gr)], ssem2.at[e]))
                smalls[-1].start()
            else:
                def body(m, carry, off=off + r0, r=r, dst=dst, step=step, r0=r0):
                    slot = lax.rem(m + step, SLOTS)

                    @pl.when(m + step >= SLOTS)
                    def _():
                        out_copy(slot, dwd, 0).wait()
                    st[slot] = dot(lv[pl.ds(pl.multiple_of(off + m * GR, 64), GR), :], rv[r], NN).astype(BF16)
                    out_copy(slot, dst, pl.multiple_of(r0 + m * GR, 64)).start()
                    return carry
                lax.fori_loop(0, times, body, 0)
                step += times
            r0 += gr * times
        if i == 0:
            for c in pin:
                c.wait()
            for buf, first, n in ((vav, 0, 4), (vbv, 4, 2)):
                tot = (buf[0] + buf[1]) + (buf[2] + buf[3])
                for j in range(n):
                    vv[first + j] = tot[j:j + 1]
        if i == 2:
            ones = jnp.ones((16, SEQ), BF16)
            for h in range(NH):
                for t in range(3):
                    q0 = OFF_QKV + h * 3 * HD + t * HD
                    gbq[t, h:h + 1, :] = dot(ones, lv[q0:q0 + HD, :], NT)[0:1]
    _ns('b_tail')
    done = []
    for i, (_, _, o) in enumerate(passes):
        done.append(pltpu.make_async_copy(srcs[i], o, osem.at[i]))
    for i, o in enumerate((v0, v1, v2, v3, v4, v5)):
        done.append(pltpu.make_async_copy(vv.at[i, 0], o, osem.at[3 + i]))
    done.append(pltpu.make_async_copy(gbq, gbq_hbm, osem.at[9]))
    for c in done:
        c.start()
    _ns('b_flush')
    for slot in range(SLOTS):
        out_copy(slot, dwd, 0).wait()
    for c in smalls:
        c.wait()
    for c in done:
        c.wait()
    _ns(None)


def solution(mesh):
    def local_step(x, ln1_gamma, ln1_beta, w_qkv, b_qkv, w_out, b_out, ln2_gamma, ln2_beta, w_up, b_up, w_down, b_down, grad_y):
        wqt = jnp.transpose(w_qkv, (1, 2, 3, 0)).reshape(QKV, D)
        any_spec = pl.BlockSpec(memory_space=pl.ANY)
        sds = jax.ShapeDtypeStruct
        y, gx, pva, pvb, gbu, lmat, rmat = pl.pallas_call(
            block_kernel,
            name='block',
            out_shape=(sds((ROWS, D), BF16), sds((ROWS, D), BF16), sds((TP, 4, D), F32), sds((TP, 2, D), F32), sds((1, FF), F32),
                       sds((LROWS, SEQ), BF16), sds((4, SEQ, D), BF16)),
            in_specs=[any_spec] * 14,
            out_specs=(any_spec,) * 7,
            scratch_shapes=[
                pltpu.VMEM((QKV, D), BF16), pltpu.VMEM((CTX, D), BF16), pltpu.VMEM((D, FF), BF16), pltpu.VMEM((FF, D), BF16),
                pltpu.VMEM((2, ROWS, D), BF16),
                pltpu.VMEM((1, D), F32), pltpu.VMEM((1, D), F32), pltpu.VMEM((3, NH, HD), F32), pltpu.VMEM((1, QKV), F32),
                pltpu.VMEM((1, D), F32), pltpu.VMEM((1, D), F32), pltpu.VMEM((1, D), F32), pltpu.VMEM((1, FF), F32), pltpu.VMEM((1, D), F32),
                pltpu.VMEM((4, SEQ, D), BF16), pltpu.VMEM((LROWS, SEQ), BF16), pltpu.VMEM((SEQ, D), BF16),
                pltpu.VMEM((QKV, SEQ), BF16), pltpu.VMEM((SEQ, QKV), BF16), pltpu.VMEM((SEQ, CTX), BF16),
                pltpu.VMEM((CTX, SEQ), BF16), pltpu.VMEM((NH, SEQ, SEQ), F32),
                pltpu.VMEM((SEQ, FF), BF16), pltpu.VMEM((SEQ, FF), BF16),
                pltpu.VMEM((ROWS, D), F32), pltpu.VMEM((ROWS, D), F32), pltpu.VMEM((2, ROWS, D), F32), pltpu.VMEM((3, ROWS, 128), F32),
                pltpu.VMEM((ROWS, D), F32), pltpu.VMEM((2, ROWS, D), BF16),
                pltpu.VMEM((1, FF), F32),
                pltpu.VMEM((4, D), F32), pltpu.VMEM((2, D), F32),
                pltpu.VMEM((4, 2, 2, ROWS, D), BF16), pltpu.VMEM((4, 2, ROWS, D), BF16),
                pltpu.VMEM((4, 2, ROWS, D), BF16), pltpu.VMEM((4, 2, ROWS, D), BF16),
                pltpu.SemaphoreType.DMA((4,)), pltpu.SemaphoreType.DMA((10,)), pltpu.SemaphoreType.DMA((11,)),
                pltpu.SemaphoreType.DMA((NSEM,)), pltpu.SemaphoreType.DMA((NSEM,)),
            ],
            compiler_params=pltpu.CompilerParams(collective_id=0, has_side_effects=True, vmem_limit_bytes=66_000_000),
            cost_estimate=pl.CostEstimate(flops=10_000_000_000, bytes_accessed=45_000_000, transcendentals=1_000_000),
        )(x[0], grad_y[0], wqt, w_out, w_up, w_down, ln1_gamma, ln1_beta, jnp.transpose(b_qkv, (1, 0, 2)), b_out,
          ln2_gamma, ln2_beta, b_up, b_down)
        y, gx, v0, v1, v2, v3, v4, v5, gbq, gbu, dwq, dwo, dwu, dwd = pl.pallas_call(
            grad_kernel,
            name='weight_grads',
            out_shape=(sds((ROWS, D), BF16), sds((ROWS, D), BF16)) + (sds((D,), F32),) * 6 + (
                sds((3, NH, HD), F32), sds((FF,), F32), sds((QKV, D), BF16), sds((CTX, D), BF16), sds((D, FF), BF16), sds((FF, D), BF16)),
            in_specs=[any_spec] * 7,
            out_specs=(any_spec,) * 14,
            scratch_shapes=[
                pltpu.VMEM((LROWS, SEQ), BF16), pltpu.VMEM((4, SEQ, D), BF16), pltpu.VMEM((SLOTS, GR, D), BF16), pltpu.VMEM((SMALL, 320, D), BF16),
                pltpu.VMEM((ROWS, D), BF16), pltpu.VMEM((ROWS, D), BF16), pltpu.VMEM((TP, 4, D), F32), pltpu.VMEM((TP, 2, D), F32),
                pltpu.VMEM((6, 1, D), F32), pltpu.VMEM((1, FF), F32),
                pltpu.VMEM((3, NH, HD), F32),
                pltpu.SemaphoreType.DMA((8,)), pltpu.SemaphoreType.DMA((SLOTS,)), pltpu.SemaphoreType.DMA((SMALL,)), pltpu.SemaphoreType.DMA((5,)), pltpu.SemaphoreType.DMA((10,)),
            ],
            compiler_params=pltpu.CompilerParams(vmem_limit_bytes=66_000_000),
            cost_estimate=pl.CostEstimate(flops=5_000_000_000, bytes_accessed=44_000_000, transcendentals=0),
        )(y, gx, pva, pvb, gbu, lmat, rmat)
        g_wqkv = jnp.transpose(dwq.reshape(NH, 3, HD, D), (3, 0, 1, 2))
        g_ln2g, g_ln2b, g_bo, g_bd, g_ln1g, g_ln1b = v0, v1, v2, v3, v4, v5
        return (y[None], gx[None], g_ln1g, g_ln1b, g_wqkv, jnp.transpose(gbq, (1, 0, 2)), dwo, g_bo,
                g_ln2g, g_ln2b, dwu, gbu, dwd, g_bd)

    row_spec = P('dp', 'tp', None)
    in_specs = (row_spec, P(), P(), P(None, 'tp', None, None), P('tp', None, None), P('tp', None), P(), P(), P(),
                P(None, 'tp'), P('tp'), P('tp', None), P(), row_spec)
    out_specs = (row_spec, row_spec, P('dp'), P('dp'), P('dp', 'tp', None, None), P(('dp', 'tp'), None, None),
                 P(('dp', 'tp'), None), P('dp'), P('dp'), P('dp'), P('dp', 'tp'), P(('dp', 'tp')), P(('dp', 'tp'), None), P('dp'))
    return jax.shard_map(local_step, mesh=mesh, in_specs=in_specs, out_specs=out_specs, check_vma=False)
```

```python
import jax
import jax.numpy as jnp
from jax import lax
from jax.experimental import pallas as pl
from jax.experimental.pallas import tpu as pltpu
from jax.sharding import PartitionSpec as P

EPS = 1e-5
MASK_VALUE = -1e30
MESH = pl.DeviceIdType.MESH
F32 = jnp.float32
BF16 = jnp.bfloat16

D = 2560
SEQ = 128
TP = 4
ROWS = SEQ // TP
NH = 8
HD = 80
QKV = NH * 3 * HD
CTX = NH * HD
FF = 2560
AGC = 4
NSEM = 80
AGW = D // AGC
CHUNKS = (256, 256, 512, 512, 512, 256, 256)
Y_CHUNKS = (640,) * 4
OFF_G, OFF_ACT, OFF_QKV, OFF_O = 0, D, D + FF, D + FF + QKV
LROWS = D + FF + QKV + CTX
SLOPES = [2.0 ** (-(h + 1) / 4.0) for h in range(NH)]
NT = (((1,), (1,)), ((), ()))
NN = (((1,), (0,)), ((), ()))
TN = (((0,), (0,)), ((), ()))


def dot(a, b, dims):
    return lax.dot_general(a, b, dims, preferred_element_type=F32)


def ln_stats(v):
    mean = jnp.mean(v, axis=-1, keepdims=True)
    cen = v - mean
    var = jnp.mean(cen * cen, axis=-1, keepdims=True)
    rstd = lax.rsqrt(var + EPS)
    return cen * rstd, rstd


def ln_grad(dy, xhat, rstd, gain):
    dxh = dy * gain
    m1 = jnp.mean(dxh, axis=-1, keepdims=True)
    m2 = jnp.mean(dxh * xhat, axis=-1, keepdims=True)
    return rstd * (dxh - m1 - xhat * m2)


def block_kernel(x_hbm, gy_hbm, wq_hbm, wo_hbm, wu_hbm, wd_hbm, g1_hbm, b1_hbm, bq_hbm, bo_hbm, g2_hbm, b2_hbm, bu_hbm,
                 bd_hbm, y_hbm, gx_hbm, va_hbm, vb_hbm, gbu_hbm, l_hbm, r_hbm,
                 wq, wo, wu, wd, xh, g1, b1, bqv, bq, bo, g2, b2, bu, bd,
                 rbuf, lbuf, gbuf, qkvt, dqkv, ctx, dctxt, prob, act, dact, x1, xn1, xn2, rs, dmid, outb, gbu, va, vb,
                 pb, rx1, sb, rx2, wsem, lsem, osem, ssem, rsem):
    me = lax.axis_index('tp')
    ax = lax.div(me, 2)
    ak = lax.rem(me, 2)
    partner = 2 * ax + (1 - ak)
    cross = 2 * (1 - ax) + ak
    diag = 2 * (1 - ax) + (1 - ak)
    peers = (partner, cross, diag)

    def rows(i):
        return pl.ds(pl.multiple_of(i * ROWS, ROWS), ROWS)

    def block_rows(b):
        return rows(2 * b + ak)

    count = {'s': 0, 'r': 0}
    _cur = []

    def _ns(name):
        if _cur:
            _cur.pop().__exit__(None, None, None)
        if name:
            _cur.append(jax.named_scope(name))
            _cur[-1].__enter__()
    _ns('start')

    def alloc(kind, n=1):
        base = count[kind]
        count[kind] += n
        return base

    def remote(src, dst, si, ri, dev):
        return pltpu.make_async_remote_copy(src_ref=src, dst_ref=dst, send_sem=ssem.at[si], recv_sem=rsem.at[ri],
                                            device_id={'tp': dev}, device_id_type=MESH)

    x_load = pltpu.make_async_copy(x_hbm, xh.at[ax], lsem.at[0])
    x_load.start()
    small = [(g1_hbm, g1.at[0]), (b1_hbm, b1.at[0]), (bq_hbm, bqv), (bo_hbm, bo.at[0]), (g2_hbm, g2.at[0]), (b2_hbm, b2.at[0]),
             (bu_hbm, bu.at[0]), (bd_hbm, bd.at[0])]
    loads = [pltpu.make_async_copy(s, d, lsem.at[1 + i]) for i, (s, d) in enumerate(small)]
    for c in loads:
        c.start()
    gy_load = pltpu.make_async_copy(gy_hbm, rbuf.at[1, rows(me)], lsem.at[1 + len(small)])
    gy_load.start()
    wcopies = [pltpu.make_async_copy(s, d, wsem.at[i])
               for i, (s, d) in enumerate([(wq_hbm, wq), (wo_hbm, wo), (wd_hbm, wd), (wu_hbm, wu)])]

    bar = pltpu.get_barrier_semaphore()
    for dev in peers:
        pl.semaphore_signal(bar, inc=1, device_id={'tp': dev}, device_id_type=MESH)
    wcopies[0].start()
    wcopies[1].start()

    class Gather:
        def __init__(self, full):
            self.full = full
            self.s = alloc('s', 2 * AGC + 1)
            self.r = alloc('r', 2 * AGC + 1)

        def chunk(self, dev, c):
            return self.full.at[rows(dev), pl.ds(c * AGW, AGW)]

        def cross_copy(self, dev, c):
            ref = self.chunk(dev, c)
            return remote(ref, ref, self.s + c, self.r + c, cross)

        def fwd_copy(self, dev, c):
            ref = self.chunk(dev, c)
            return remote(ref, ref, self.s + AGC + c, self.r + AGC + c, partner)

        def own_copy(self, dev):
            ref = self.full.at[rows(dev)]
            return remote(ref, ref, self.s + 2 * AGC, self.r + 2 * AGC, partner)

        def start(self):
            for c in range(AGC):
                self.cross_copy(me, c).start()
            self.own_copy(me).start()

        def forward(self, c):
            self.cross_copy(cross, c).wait_recv()
            self.fwd_copy(cross, c).start()

        def finish(self):
            self.own_copy(partner).wait_recv()
            for c in range(AGC):
                self.fwd_copy(diag, c).wait_recv()

        def drain(self):
            for c in range(AGC):
                self.cross_copy(me, c).wait_send()
                self.fwd_copy(cross, c).wait_send()
            self.own_copy(me).wait_send()

    class Share:
        def __init__(self, full):
            self.full = full
            self.s = alloc('s', 2)
            self.r = alloc('r', 2)

        def copy(self, b, k, i):
            ref = self.full.at[rows(2 * b + k)]
            return remote(ref, ref, self.s + i, self.r + i, partner)

        def send(self, b, i):
            self.copy(b, ak, i).start()

        def finish(self, b, i):
            self.copy(b, 1 - ak, i).wait_recv()

        def drain(self):
            self.copy(ax, ak, 0).wait_send()
            self.copy(1 - ax, ak, 1).wait_send()

    class Reduce:
        def __init__(self, i, both, chunks=CHUNKS):
            self.p, self.x1, self.sb, self.x2 = pb.at[i], rx1.at[i], sb.at[i], rx2.at[i]
            self.both = both
            self.chunks = chunks
            self.n = len(chunks)
            self.s = alloc('s', 2 * self.n)
            self.r = alloc('r', 2 * self.n)

        def cols(self, n):
            return pl.ds(sum(self.chunks[:n]), self.chunks[n])

        def pair(self, n):
            return remote(self.p.at[:, 1 - ak, :, self.cols(n)], self.x1.at[:, :, self.cols(n)], self.s + n, self.r + n, partner)

        def over(self, n):
            if self.both:
                src, dst = self.sb.at[:, :, self.cols(n)], self.x2.at[:, :, self.cols(n)]
            else:
                src, dst = self.sb.at[0, :, self.cols(n)], self.x2.at[0, :, self.cols(n)]
            return remote(src, dst, self.s + self.n + n, self.r + self.n + n, cross)

        def produce(self, n, val):
            self.p[:, :, :, self.cols(n)] = val.astype(BF16).reshape(2, 2, ROWS, self.chunks[n])
            self.pair(n).start()

        def relay(self, n):
            self.pair(n).wait_recv()
            c = self.cols(n)
            if self.both:
                self.sb[:, :, c] = (self.p[:, ak, :, c].astype(F32) + self.x1[:, :, c].astype(F32)).astype(BF16)
            else:
                self.sb[0, :, c] = (self.p[1 - ax, ak, :, c].astype(F32) + self.x1[1 - ax, :, c].astype(F32)).astype(BF16)
            self.over(n).start()

        def run(self, fn, lag, late=0, also=None):
            for n in range(self.n):
                self.produce(n, fn(self.cols(n)))
                self.step(n - lag, n - lag - late)
                if also is not None:
                    also(n)

        def step(self, n0, n1):
            for core, n in ((0, n0), (1, n1)):
                if 0 <= n < self.n:
                    @pl.when(ak == core)
                    def _():
                        self.relay(n)

        def rest(self, lag, late=0):
            for i in range(lag + late):
                self.step(self.n - lag + i, self.n - lag - late + i)

        def relay_all(self):
            for n in range(self.n):
                self.relay(n)

        def arrive(self):
            for n in range(self.n):
                self.over(n).wait_recv()

        def block(self, b):
            return (self.sb[b].astype(F32) + self.x2[b].astype(F32)).astype(BF16).astype(F32)

        def own(self):
            v = self.p[ax, ak].astype(F32) + self.x1[ax].astype(F32) + self.x2[0].astype(F32)
            return v.astype(BF16).astype(F32)

        def drain(self):
            for n in range(self.n):
                self.pair(n).wait_send()
                self.over(n).wait_send()

    gat_m = Gather(rbuf.at[1])
    sh_h, sh_g, sh_a = Share(rbuf.at[2]), Share(gbuf), Share(rbuf.at[3])
    sc_a, sc_g, sc_y, sc_h = Reduce(0, True), Reduce(1, True), Reduce(2, False, Y_CHUNKS), Reduce(3, False)
    blocks = ((ax, 0), (1 - ax, 1))
    outs = []

    def emit(src, dst):
        c = pltpu.make_async_copy(src, dst, osem.at[len(outs)])
        c.start()
        outs.append(c)

    sx, rx = alloc('s'), alloc('r')
    _ns('barrier')
    x_load.wait()
    pl.semaphore_wait(bar, 3)

    def x_start(core):
        @pl.when(ak == core)
        def _():
            remote(xh.at[ax], xh.at[ax], sx, rx, cross).start()
    _ns('xsend')
    x_start(0)
    for c in loads:
        c.wait()
    bq[...] = jnp.concatenate([bqv[t, h:h + 1, :] for h in range(NH) for t in range(3)], axis=1)
    for b, i in blocks:
        if i == 1:
            remote(xh.at[1 - ax], xh.at[1 - ax], sx, rx, cross).wait_recv()
        xhat, rstd = ln_stats(xh[b].astype(F32))
        if i == 0:
            xn1[...] = xhat
            rs[2] = jnp.broadcast_to(rstd, (ROWS, 128))
        rbuf[2, block_rows(b), :] = (xhat * g1[...] + b1[...]).astype(BF16)
        sh_h.send(b, i)
        if i == 0:
            x_start(1)
    _ns('hshare')
    gy_load.wait()
    gat_m.start()
    wcopies[2].start()
    wcopies[3].start()
    wcopies[0].wait()
    for b, i in blocks:
        sh_h.finish(b, i)
    emit(rbuf.at[2], r_hbm.at[2])

    _ns('qkv')
    QC = 640

    def qkv_body(n, carry):
        r0 = pl.multiple_of(n * QC, QC)
        v = dot(rbuf[2], wq[pl.ds(r0, QC), :], NT) + bq[:, pl.ds(r0, QC)]
        qkvt[pl.ds(r0, QC), :] = v.astype(BF16).T
        return carry
    lax.fori_loop(0, QKV // QC, qkv_body, 0)

    _ns('attn')
    scale = HD ** -0.5
    jpos = lax.broadcasted_iota(jnp.int32, (SEQ, SEQ), 0)
    ipos = lax.broadcasted_iota(jnp.int32, (SEQ, SEQ), 1)
    causal = jpos <= ipos
    jf = jpos.astype(F32)
    base = jnp.where(me == 0, 1.0, jnp.where(me == 1, 0.25, jnp.where(me == 2, 0.0625, 0.015625))).astype(F32)

    def head(h, t):
        r0 = h * 3 * HD + t * HD
        return qkvt[r0:r0 + HD, :]

    for h in range(NH):
        s = dot(head(h, 1), head(h, 0), TN) * scale + (base * SLOPES[h]) * jf
        s = jnp.where(causal, s, MASK_VALUE)
        e = jnp.exp(s - jnp.max(s, axis=0, keepdims=True))
        p = e * (1.0 / jnp.sum(e, axis=0, keepdims=True))
        prob[h] = p
        lbuf[OFF_O + h * HD:OFF_O + (h + 1) * HD, :] = dot(head(h, 2), p.astype(BF16), NN).astype(BF16)
    for t in range(CTX // 128):
        ctx[:, t * 128:(t + 1) * 128] = lbuf[OFF_O + t * 128:OFF_O + (t + 1) * 128, :].T

    _ns('outproj')
    wcopies[1].wait()
    sc_a.run(lambda cols: dot(ctx[...], wo[:, cols], NN), 3, 3)
    _ns('arelay')
    sc_a.rest(3, 3)

    _ns('gm_fwd')
    for c in range(AGC):
        gat_m.forward(c)
    wcopies[2].wait()
    gat_m.finish()
    emit(rbuf.at[1], r_hbm.at[1])
    _ns('dact')
    FC = 512

    def dact_body(n, carry):
        f0 = pl.multiple_of(n * FC, FC)
        dact[:, pl.ds(f0, FC)] = dot(rbuf[1], wd[pl.ds(f0, FC), :], NT).astype(BF16)
        return carry
    lax.fori_loop(0, FF // FC, dact_body, 0)

    _ns('a_wait')
    sc_a.arrive()
    _ns('ln2')
    for b, i in blocks:
        xm = xh[b].astype(F32) + sc_a.block(b) + bo[...]
        if i == 0:
            x1[...] = xm
        xhat, rstd = ln_stats(xm)
        xn2[b] = xhat
        rs[b] = jnp.broadcast_to(rstd, (ROWS, 128))
        gbuf[block_rows(b), :] = (xhat * g2[...] + b2[...]).astype(BF16)
        sh_g.send(b, i)
    _ns('g_share')
    wcopies[3].wait()
    for b, i in blocks:
        sh_g.finish(b, i)

    _ns('up')
    UC = 512
    k0 = 0.7978845608028654
    k1 = 0.044715

    for f0 in range(0, FF, UC):
        cols = pl.ds(f0, UC)
        v = dot(gbuf[...], wu[:, cols], NN) + bu[:, cols]
        v2 = v * v
        t = jnp.tanh(k0 * (v + k1 * (v2 * v)))
        hp = 0.5 * (1.0 + t)
        act[:, cols] = (v * hp).astype(BF16)
        dg = hp + (0.5 * k0) * v * (1.0 - t * t) * (1.0 + (3.0 * k1) * v2)
        dpre = dact[:, cols].astype(F32) * dg
        gbu[:, cols] = jnp.sum(dpre, axis=0, keepdims=True)
        rbuf[0, :, cols] = dpre.astype(BF16)
    emit(rbuf.at[0], r_hbm.at[0])
    emit(gbu, gbu_hbm)

    _ns('dg')
    def dg_chunk(cols):
        return dot(rbuf[0], wu[cols, :], NT)
    sc_g.run(dg_chunk, 1, 1)

    _ns('down')
    def rest(n):
        if n == 0:
            sc_g.rest(1, 1)
    sc_y.run(lambda cols: dot(act[...], wd[:, cols], NN), sc_y.n, 0, rest)
    va[3:4, :] = jnp.sum(rbuf[1, rows(me), :].astype(F32), axis=0, keepdims=True)

    _ns('g_wait')
    sc_g.arrive()
    _ns('ln2b')
    for b, i in blocks:
        dgl = sc_g.block(b)
        xhat, rstd = xn2[b], rs[b, :, 0:1]
        dm = rbuf[1, block_rows(b), :].astype(F32) + ln_grad(dgl, xhat, rstd, g2[...])
        rbuf[3, block_rows(b), :] = dm.astype(BF16)
        sh_a.send(b, i)
        if i == 0:
            dmid[...] = dm
    va[2:3, :] = jnp.sum(dmid[...], axis=0, keepdims=True)
    dgl = sc_g.block(ax)
    va[0:1, :] = jnp.sum(dgl * xn2[ax], axis=0, keepdims=True)
    va[1:2, :] = jnp.sum(dgl, axis=0, keepdims=True)

    sva, rva = alloc('s', 3), alloc('r', 3)

    def vec_copy(buf, hbm, s, r, i, owner, dev):
        return remote(buf, hbm.at[owner], s + i, r + i, dev)
    _ns('yrelay')
    sc_y.relay_all()
    for i, dev in enumerate(peers):
        vec_copy(va, va_hbm, sva, rva, i, me, dev).start()
    emit(va, va_hbm.at[me])
    _ns('a_share')
    for b, i in blocks:
        sh_a.finish(b, i)
    emit(rbuf.at[3], r_hbm.at[3])

    _ns('attnb')
    ctx[...] = dot(rbuf[3], wo[...], NT).astype(BF16)
    for t in range(CTX // 128):
        dctxt[t * 128:(t + 1) * 128, :] = ctx[:, t * 128:(t + 1) * 128].T

    for h in range(NH):
        dot_h = dctxt[h * HD:(h + 1) * HD, :]
        p = prob[h]
        dp = dot(head(h, 2), dot_h, TN).astype(BF16).astype(F32)
        ds = (p * (dp - jnp.sum(dp * p, axis=0, keepdims=True))).astype(BF16)
        r0 = OFF_QKV + h * 3 * HD
        lbuf[r0:r0 + HD, :] = (dot(head(h, 1), ds, NN) * scale).astype(BF16)
        lbuf[r0 + HD:r0 + 2 * HD, :] = (dot(head(h, 0), ds, NT) * scale).astype(BF16)
        lbuf[r0 + 2 * HD:r0 + 3 * HD, :] = dot(dot_h, p.astype(BF16), NT).astype(BF16)
    for t in range(QKV // 128):
        dqkv[:, t * 128:(t + 1) * 128] = lbuf[OFF_QKV + t * 128:OFF_QKV + (t + 1) * 128, :].T
    emit(lbuf.at[pl.ds(OFF_QKV, QKV + CTX)], l_hbm.at[pl.ds(OFF_QKV, QKV + CTX)])

    _ns('dh')
    sc_h.run(lambda cols: dot(dqkv[...], wq[:, cols], NN), 2, 2)
    _ns('hrelay')
    sc_h.rest(2, 2)

    _ns('y')
    sc_y.arrive()
    outb[0] = (x1[...] + sc_y.own() + bd[...]).astype(BF16)
    emit(outb.at[0], y_hbm)
    _ns('transp')
    def tr_body(src, off):
        def body(n, carry):
            r0 = pl.multiple_of(n * 512, 512)
            lbuf[pl.ds(off + r0, 512), :] = src[:, pl.ds(r0, 512)].T
            return carry
        return body
    lax.fori_loop(0, FF // 512, tr_body(act, OFF_ACT), 0)
    lax.fori_loop(0, D // 512, tr_body(gbuf, OFF_G), 0)
    emit(lbuf.at[pl.ds(0, OFF_QKV)], l_hbm.at[pl.ds(0, OFF_QKV)])

    _ns('h_wait')
    sc_h.arrive()
    _ns('ln1b')
    dhl = sc_h.own()
    xhat1, rstd1 = xn1[...], rs[2, :, 0:1]
    vb[0:1, :] = jnp.sum(dhl * xhat1, axis=0, keepdims=True)
    vb[1:2, :] = jnp.sum(dhl, axis=0, keepdims=True)
    svb, rvb = alloc('s', 3), alloc('r', 3)
    for i, dev in enumerate(peers):
        vec_copy(vb, vb_hbm, svb, rvb, i, me, dev).start()
    emit(vb, vb_hbm.at[me])
    outb[1] = (dmid[...] + ln_grad(dhl, xhat1, rstd1, g1[...])).astype(BF16)
    emit(outb.at[1], gx_hbm)
    _ns('drain')
    remote(xh.at[ax], xh.at[ax], sx, rx, cross).wait_send()
    gat_m.drain()
    for g in (sh_h, sh_g, sh_a, sc_a, sc_g, sc_y, sc_h):
        g.drain()
    for i, dev in enumerate(peers):
        vec_copy(va, va_hbm, sva, rva, i, me, dev).wait_send()
        vec_copy(va, va_hbm, sva, rva, i, dev, dev).wait_recv()
    _ns('vecwait')
    for i, dev in enumerate(peers):
        vec_copy(vb, vb_hbm, svb, rvb, i, dev, dev).wait_recv()
    for i, dev in enumerate(peers):
        vec_copy(vb, vb_hbm, svb, rvb, i, me, dev).wait_send()
    for c in outs:
        c.wait()
    _ns(None)
    assert max(count.values()) <= NSEM


GR = 640
SLOTS = 4
SECTIONS = ((OFF_ACT, FF, 1), (OFF_G, D, 0), (OFF_QKV, QKV, 2), (OFF_O, CTX, 3))
PIECES = (((160, 1), (160, 1), (320, 1), (GR, 3)), ((GR, 4),), ((GR, 3),), ((320, 1), (160, 1), (160, 1)))
SMALL = 6


def grad_kernel(y_in, gx_in, va_in, vb_in, gbu_in, l_hbm, r_hbm, y_out, gx_out, v0, v1, v2, v3, v4, v5, gbq_hbm, gbu_out,
                dwq, dwo, dwu, dwd, lv, rv, st, st2, yv, gxv, vav, vbv, vv, gv, gbq, isem, ssem, ssem2, psem, osem):
    _cur = []

    def _ns(name):
        if _cur:
            _cur.pop().__exit__(None, None, None)
        if name:
            _cur.append(jax.named_scope(name))
            _cur[-1].__enter__()
    _ns('b_start')
    loads = []
    for i, (off, n, r) in enumerate(SECTIONS):
        cl = pltpu.make_async_copy(l_hbm.at[pl.ds(off, n)], lv.at[pl.ds(off, n)], isem.at[2 * i])
        cr = pltpu.make_async_copy(r_hbm.at[r], rv.at[r], isem.at[2 * i + 1])
        cl.start()
        cr.start()
        loads.append((cl, cr))
    passes = [(y_in, yv, y_out), (gx_in, gxv, gx_out), (gbu_in, gv, gbu_out)]
    srcs = (yv, gxv, gv.at[0])
    pin = [pltpu.make_async_copy(a, b, psem.at[i]) for i, (a, b, _) in enumerate(passes)]
    pin.append(pltpu.make_async_copy(va_in, vav, psem.at[3]))
    pin.append(pltpu.make_async_copy(vb_in, vbv, psem.at[4]))
    for c in pin:
        c.start()
    douts = (dwd, dwu, dwq, dwo)
    step = 0

    def out_copy(slot, dst, r0):
        return pltpu.make_async_copy(st.at[slot], dst.at[pl.ds(r0, GR)], ssem.at[slot])
    smalls = []
    for i, (off, n, r) in enumerate(SECTIONS):
        _ns('b_load%d' % i)
        loads[i][0].wait()
        loads[i][1].wait()
        dst = douts[i]
        _ns('b_sec%d' % i)
        r0 = 0
        for gr, times in PIECES[i]:
            if gr < GR:
                e = len(smalls)

                def small(m, carry, off=off + r0, gr=gr, e=e, r=r):
                    st2[e, 0:gr] = dot(lv[pl.ds(pl.multiple_of(off + m * gr, 32), gr), :], rv[r], NN).astype(BF16)
                    return carry
                lax.fori_loop(0, 1, small, 0)
                smalls.append(pltpu.make_async_copy(st2.at[e, pl.ds(0, gr)], dst.at[pl.ds(r0, gr)], ssem2.at[e]))
                smalls[-1].start()
            else:
                def body(m, carry, off=off + r0, r=r, dst=dst, step=step, r0=r0):
                    slot = lax.rem(m + step, SLOTS)

                    @pl.when(m + step >= SLOTS)
                    def _():
                        out_copy(slot, dwd, 0).wait()
                    st[slot] = dot(lv[pl.ds(pl.multiple_of(off + m * GR, 64), GR), :], rv[r], NN).astype(BF16)
                    out_copy(slot, dst, pl.multiple_of(r0 + m * GR, 64)).start()
                    return carry
                lax.fori_loop(0, times, body, 0)
                step += times
            r0 += gr * times
        if i == 0:
            for c in pin:
                c.wait()
            for buf, first, n in ((vav, 0, 4), (vbv, 4, 2)):
                tot = (buf[0] + buf[1]) + (buf[2] + buf[3])
                for j in range(n):
                    vv[first + j] = tot[j:j + 1]
        if i == 2:
            ones = jnp.ones((16, SEQ), BF16)
            for h in range(NH):
                for t in range(3):
                    q0 = OFF_QKV + h * 3 * HD + t * HD
                    gbq[t, h:h + 1, :] = dot(ones, lv[q0:q0 + HD, :], NT)[0:1]
    _ns('b_tail')
    done = []
    for i, (_, _, o) in enumerate(passes):
        done.append(pltpu.make_async_copy(srcs[i], o, osem.at[i]))
    for i, o in enumerate((v0, v1, v2, v3, v4, v5)):
        done.append(pltpu.make_async_copy(vv.at[i, 0], o, osem.at[3 + i]))
    done.append(pltpu.make_async_copy(gbq, gbq_hbm, osem.at[9]))
    for c in done:
        c.start()
    _ns('b_flush')
    for slot in range(SLOTS):
        out_copy(slot, dwd, 0).wait()
    for c in smalls:
        c.wait()
    for c in done:
        c.wait()
    _ns(None)


def solution(mesh):
    def local_step(x, ln1_gamma, ln1_beta, w_qkv, b_qkv, w_out, b_out, ln2_gamma, ln2_beta, w_up, b_up, w_down, b_down, grad_y):
        wqt = jnp.transpose(w_qkv, (1, 2, 3, 0)).reshape(QKV, D)
        any_spec = pl.BlockSpec(memory_space=pl.ANY)
        sds = jax.ShapeDtypeStruct
        y, gx, pva, pvb, gbu, lmat, rmat = pl.pallas_call(
            block_kernel,
            name='block',
            out_shape=(sds((ROWS, D), BF16), sds((ROWS, D), BF16), sds((TP, 4, D), F32), sds((TP, 2, D), F32), sds((1, FF), F32),
                       sds((LROWS, SEQ), BF16), sds((4, SEQ, D), BF16)),
            in_specs=[any_spec] * 14,
            out_specs=(any_spec,) * 7,
            scratch_shapes=[
                pltpu.VMEM((QKV, D), BF16), pltpu.VMEM((CTX, D), BF16), pltpu.VMEM((D, FF), BF16), pltpu.VMEM((FF, D), BF16),
                pltpu.VMEM((2, ROWS, D), BF16),
                pltpu.VMEM((1, D), F32), pltpu.VMEM((1, D), F32), pltpu.VMEM((3, NH, HD), F32), pltpu.VMEM((1, QKV), F32),
                pltpu.VMEM((1, D), F32), pltpu.VMEM((1, D), F32), pltpu.VMEM((1, D), F32), pltpu.VMEM((1, FF), F32), pltpu.VMEM((1, D), F32),
                pltpu.VMEM((4, SEQ, D), BF16), pltpu.VMEM((LROWS, SEQ), BF16), pltpu.VMEM((SEQ, D), BF16),
                pltpu.VMEM((QKV, SEQ), BF16), pltpu.VMEM((SEQ, QKV), BF16), pltpu.VMEM((SEQ, CTX), BF16),
                pltpu.VMEM((CTX, SEQ), BF16), pltpu.VMEM((NH, SEQ, SEQ), F32),
                pltpu.VMEM((SEQ, FF), BF16), pltpu.VMEM((SEQ, FF), BF16),
                pltpu.VMEM((ROWS, D), F32), pltpu.VMEM((ROWS, D), F32), pltpu.VMEM((2, ROWS, D), F32), pltpu.VMEM((3, ROWS, 128), F32),
                pltpu.VMEM((ROWS, D), F32), pltpu.VMEM((2, ROWS, D), BF16),
                pltpu.VMEM((1, FF), F32),
                pltpu.VMEM((4, D), F32), pltpu.VMEM((2, D), F32),
                pltpu.VMEM((4, 2, 2, ROWS, D), BF16), pltpu.VMEM((4, 2, ROWS, D), BF16),
                pltpu.VMEM((4, 2, ROWS, D), BF16), pltpu.VMEM((4, 2, ROWS, D), BF16),
                pltpu.SemaphoreType.DMA((4,)), pltpu.SemaphoreType.DMA((10,)), pltpu.SemaphoreType.DMA((11,)),
                pltpu.SemaphoreType.DMA((NSEM,)), pltpu.SemaphoreType.DMA((NSEM,)),
            ],
            compiler_params=pltpu.CompilerParams(collective_id=0, has_side_effects=True, vmem_limit_bytes=66_000_000),
            cost_estimate=pl.CostEstimate(flops=10_000_000_000, bytes_accessed=45_000_000, transcendentals=1_000_000),
        )(x[0], grad_y[0], wqt, w_out, w_up, w_down, ln1_gamma, ln1_beta, jnp.transpose(b_qkv, (1, 0, 2)), b_out,
          ln2_gamma, ln2_beta, b_up, b_down)
        y, gx, v0, v1, v2, v3, v4, v5, gbq, gbu, dwq, dwo, dwu, dwd = pl.pallas_call(
            grad_kernel,
            name='weight_grads',
            out_shape=(sds((ROWS, D), BF16), sds((ROWS, D), BF16)) + (sds((D,), F32),) * 6 + (
                sds((3, NH, HD), F32), sds((FF,), F32), sds((QKV, D), BF16), sds((CTX, D), BF16), sds((D, FF), BF16), sds((FF, D), BF16)),
            in_specs=[any_spec] * 7,
            out_specs=(any_spec,) * 14,
            scratch_shapes=[
                pltpu.VMEM((LROWS, SEQ), BF16), pltpu.VMEM((4, SEQ, D), BF16), pltpu.VMEM((SLOTS, GR, D), BF16), pltpu.VMEM((SMALL, 320, D), BF16),
                pltpu.VMEM((ROWS, D), BF16), pltpu.VMEM((ROWS, D), BF16), pltpu.VMEM((TP, 4, D), F32), pltpu.VMEM((TP, 2, D), F32),
                pltpu.VMEM((6, 1, D), F32), pltpu.VMEM((1, FF), F32),
                pltpu.VMEM((3, NH, HD), F32),
                pltpu.SemaphoreType.DMA((8,)), pltpu.SemaphoreType.DMA((SLOTS,)), pltpu.SemaphoreType.DMA((SMALL,)), pltpu.SemaphoreType.DMA((5,)), pltpu.SemaphoreType.DMA((10,)),
            ],
            compiler_params=pltpu.CompilerParams(vmem_limit_bytes=66_000_000),
            cost_estimate=pl.CostEstimate(flops=5_000_000_000, bytes_accessed=44_000_000, transcendentals=0),
        )(y, gx, pva, pvb, gbu, lmat, rmat)
        g_wqkv = jnp.transpose(dwq.reshape(NH, 3, HD, D), (3, 0, 1, 2))
        g_ln2g, g_ln2b, g_bo, g_bd, g_ln1g, g_ln1b = v0, v1, v2, v3, v4, v5
        return (y[None], gx[None], g_ln1g, g_ln1b, g_wqkv, jnp.transpose(gbq, (1, 0, 2)), dwo, g_bo,
                g_ln2g, g_ln2b, dwu, gbu, dwd, g_bd)

    row_spec = P('dp', 'tp', None)
    in_specs = (row_spec, P(), P(), P(None, 'tp', None, None), P('tp', None, None), P('tp', None), P(), P(), P(),
                P(None, 'tp'), P('tp'), P('tp', None), P(), row_spec)
    out_specs = (row_spec, row_spec, P('dp'), P('dp'), P('dp', 'tp', None, None), P(('dp', 'tp'), None, None),
                 P(('dp', 'tp'), None), P('dp'), P('dp'), P('dp'), P('dp', 'tp'), P(('dp', 'tp')), P(('dp', 'tp'), None), P('dp'))
    return jax.shard_map(local_step, mesh=mesh, in_specs=in_specs, out_specs=out_specs, check_vma=False)
```

```python
import jax
import jax.numpy as jnp
from jax import lax
from jax.experimental import pallas as pl
from jax.experimental.pallas import tpu as pltpu
from jax.sharding import PartitionSpec as P

EPS = 1e-5
MASK_VALUE = -1e30
MESH = pl.DeviceIdType.MESH
F32 = jnp.float32
BF16 = jnp.bfloat16

D = 2560
SEQ = 128
TP = 4
ROWS = SEQ // TP
NH = 8
HD = 80
QKV = NH * 3 * HD
CTX = NH * HD
FF = 2560
AGC = 4
NS, NR = 24, 48
AGW = D // AGC
CHUNKS = (256, 256, 512, 512, 512, 256, 256)
Y_CHUNKS = (640,) * 4
OFF_G, OFF_ACT, OFF_QKV, OFF_O = 0, D, D + FF, D + FF + QKV
LROWS = D + FF + QKV + CTX
SLOPES = [2.0 ** (-(h + 1) / 4.0) for h in range(NH)]
NT = (((1,), (1,)), ((), ()))
NN = (((1,), (0,)), ((), ()))
TN = (((0,), (0,)), ((), ()))


def dot(a, b, dims):
    return lax.dot_general(a, b, dims, preferred_element_type=F32)


def ln_stats(v):
    mean = jnp.mean(v, axis=-1, keepdims=True)
    cen = v - mean
    var = jnp.mean(cen * cen, axis=-1, keepdims=True)
    rstd = lax.rsqrt(var + EPS)
    return cen * rstd, rstd


def ln_grad(dy, xhat, rstd, gain):
    dxh = dy * gain
    m1 = jnp.mean(dxh, axis=-1, keepdims=True)
    m2 = jnp.mean(dxh * xhat, axis=-1, keepdims=True)
    return rstd * (dxh - m1 - xhat * m2)


def block_kernel(x_hbm, gy_hbm, wq_hbm, wo_hbm, wu_hbm, wd_hbm, g1_hbm, b1_hbm, bq_hbm, bo_hbm, g2_hbm, b2_hbm, bu_hbm,
                 bd_hbm, y_hbm, gx_hbm, va_hbm, vb_hbm, gbu_hbm, l_hbm, r_hbm,
                 wq, wo, wu, wd, xh, g1, b1, bqv, bq, bo, g2, b2, bu, bd,
                 rbuf, lbuf, gbuf, qkvt, dqkv, ctx, dctxt, prob, act, dact, x1, xn1, xn2, rs, dmid, outb, gbu, va, vb,
                 pb, rx1, sb, rx2, wsem, lsem, osem, ssem, rsem):
    me = lax.axis_index('tp')
    ax = lax.div(me, 2)
    ak = lax.rem(me, 2)
    partner = 2 * ax + (1 - ak)
    cross = 2 * (1 - ax) + ak
    diag = 2 * (1 - ax) + (1 - ak)
    peers = (partner, cross, diag)

    def rows(i):
        return pl.ds(pl.multiple_of(i * ROWS, ROWS), ROWS)

    def block_rows(b):
        return rows(2 * b + ak)

    count = {'s': 0, 'r': 0}

    def alloc(kind, n=1):
        base = count[kind]
        count[kind] += n
        return base

    def remote(src, dst, si, ri, dev):
        return pltpu.make_async_remote_copy(src_ref=src, dst_ref=dst, send_sem=ssem.at[si], recv_sem=rsem.at[ri],
                                            device_id={'tp': dev}, device_id_type=MESH)

    x_load = pltpu.make_async_copy(x_hbm, xh.at[ax], lsem.at[0])
    x_load.start()
    small = [(g1_hbm, g1.at[0]), (b1_hbm, b1.at[0]), (bq_hbm, bqv), (bo_hbm, bo.at[0]), (g2_hbm, g2.at[0]), (b2_hbm, b2.at[0]),
             (bu_hbm, bu.at[0]), (bd_hbm, bd.at[0])]
    loads = [pltpu.make_async_copy(s, d, lsem.at[1 + i]) for i, (s, d) in enumerate(small)]
    for c in loads:
        c.start()
    gy_load = pltpu.make_async_copy(gy_hbm, rbuf.at[1, rows(me)], lsem.at[1 + len(small)])
    gy_load.start()
    wcopies = [pltpu.make_async_copy(s, d, wsem.at[i])
               for i, (s, d) in enumerate([(wq_hbm, wq), (wo_hbm, wo), (wd_hbm, wd), (wu_hbm, wu)])]

    bar = pltpu.get_barrier_semaphore()
    for dev in peers:
        pl.semaphore_signal(bar, inc=1, device_id={'tp': dev}, device_id_type=MESH)
    wcopies[0].start()
    wcopies[1].start()

    class Gather:
        def __init__(self, full):
            self.full = full
            self.s = alloc('s', 3)
            self.r = alloc('r', AGC + 2)

        def chunk(self, dev, c):
            return self.full.at[rows(dev), pl.ds(c * AGW, AGW)]

        def cross_copy(self, dev, c):
            ref = self.chunk(dev, c)
            return remote(ref, ref, self.s, self.r + c, cross)

        def fwd_copy(self, dev, c):
            ref = self.chunk(dev, c)
            return remote(ref, ref, self.s + 1, self.r + AGC, partner)

        def whole(self, dev, i, j, to):
            ref = self.full.at[rows(dev)]
            return remote(ref, ref, self.s + i, self.r + j, to)

        def own_copy(self, dev):
            return self.whole(dev, 2, AGC + 1, partner)

        def start(self):
            for c in range(AGC):
                self.cross_copy(me, c).start()
            self.own_copy(me).start()

        def forward(self, c):
            self.cross_copy(cross, c).wait_recv()
            self.fwd_copy(cross, c).start()

        def finish(self):
            self.own_copy(partner).wait_recv()
            self.whole(diag, 1, AGC, partner).wait_recv()

        def drain(self):
            self.whole(me, 0, 0, cross).wait_send()
            self.whole(cross, 1, AGC, partner).wait_send()
            self.own_copy(me).wait_send()

    class Share:
        def __init__(self, full):
            self.full = full
            self.s = alloc('s', 2)
            self.r = alloc('r', 2)

        def copy(self, b, k, i):
            ref = self.full.at[rows(2 * b + k)]
            return remote(ref, ref, self.s + i, self.r + i, partner)

        def send(self, b, i):
            self.copy(b, ak, i).start()

        def finish(self, b, i):
            self.copy(b, 1 - ak, i).wait_recv()

        def drain(self):
            self.copy(ax, ak, 0).wait_send()
            self.copy(1 - ax, ak, 1).wait_send()

    class Reduce:
        def __init__(self, i, both, chunks=CHUNKS):
            self.p, self.x1, self.sb, self.x2 = pb.at[i], rx1.at[i], sb.at[i], rx2.at[i]
            self.both = both
            self.chunks = chunks
            self.n = len(chunks)
            self.s = alloc('s', 2)
            self.r = alloc('r', self.n + 1)

        def cols(self, n):
            return pl.ds(sum(self.chunks[:n]), self.chunks[n])

        def pair(self, n):
            return remote(self.p.at[:, 1 - ak, :, self.cols(n)], self.x1.at[:, :, self.cols(n)], self.s, self.r + n, partner)

        def over(self, c):
            if self.both:
                src, dst = self.sb.at[:, :, c], self.x2.at[:, :, c]
            else:
                src, dst = self.sb.at[0, :, c], self.x2.at[0, :, c]
            return remote(src, dst, self.s + 1, self.r + self.n, cross)

        def produce(self, n, val):
            self.p[:, :, :, self.cols(n)] = val.astype(BF16).reshape(2, 2, ROWS, self.chunks[n])
            self.pair(n).start()

        def relay(self, n):
            self.pair(n).wait_recv()
            c = self.cols(n)
            if self.both:
                self.sb[:, :, c] = (self.p[:, ak, :, c].astype(F32) + self.x1[:, :, c].astype(F32)).astype(BF16)
            else:
                self.sb[0, :, c] = (self.p[1 - ax, ak, :, c].astype(F32) + self.x1[1 - ax, :, c].astype(F32)).astype(BF16)
            self.over(c).start()

        def run(self, fn, lag, also=None):
            for n in range(self.n):
                self.produce(n, fn(self.cols(n)))
                if n >= lag:
                    self.relay(n - lag)
                if also is not None:
                    also(n)

        def relay_from(self, first):
            for n in range(first, self.n):
                self.relay(n)

        def arrive(self):
            self.over(slice(None)).wait_recv()

        def block(self, b):
            return (self.sb[b].astype(F32) + self.x2[b].astype(F32)).astype(BF16).astype(F32)

        def own(self):
            v = self.p[ax, ak].astype(F32) + self.x1[ax].astype(F32) + self.x2[0].astype(F32)
            return v.astype(BF16).astype(F32)

        def drain(self):
            remote(self.p.at[:, 1 - ak], self.x1, self.s, self.r, partner).wait_send()
            self.over(slice(None)).wait_send()

    gat_m = Gather(rbuf.at[1])
    sh_h, sh_g, sh_a = Share(rbuf.at[2]), Share(gbuf), Share(rbuf.at[3])
    sc_a, sc_g, sc_y, sc_h = Reduce(0, True), Reduce(1, True), Reduce(2, False, Y_CHUNKS), Reduce(3, False)
    blocks = ((ax, 0), (1 - ax, 1))
    outs = []

    def emit(src, dst):
        c = pltpu.make_async_copy(src, dst, osem.at[len(outs)])
        c.start()
        outs.append(c)

    sx, rx = alloc('s'), alloc('r')
    x_load.wait()
    pl.semaphore_wait(bar, 3)
    remote(xh.at[ax], xh.at[ax], sx, rx, cross).start()
    for c in loads:
        c.wait()
    bq[...] = jnp.concatenate([bqv[t, h:h + 1, :] for h in range(NH) for t in range(3)], axis=1)
    for b, i in blocks:
        if i == 1:
            remote(xh.at[1 - ax], xh.at[1 - ax], sx, rx, cross).wait_recv()
        xhat, rstd = ln_stats(xh[b].astype(F32))
        if i == 0:
            xn1[...] = xhat
            rs[2] = jnp.broadcast_to(rstd, (ROWS, 128))
        rbuf[2, block_rows(b), :] = (xhat * g1[...] + b1[...]).astype(BF16)
        sh_h.send(b, i)
    gy_load.wait()
    gat_m.start()
    wcopies[2].start()
    wcopies[3].start()
    wcopies[0].wait()
    for b, i in blocks:
        sh_h.finish(b, i)
    emit(rbuf.at[2], r_hbm.at[2])

    QC = 640

    def qkv_body(n, carry):
        r0 = pl.multiple_of(n * QC, QC)
        v = dot(rbuf[2], wq[pl.ds(r0, QC), :], NT) + bq[:, pl.ds(r0, QC)]
        qkvt[pl.ds(r0, QC), :] = v.astype(BF16).T
        return carry
    lax.fori_loop(0, QKV // QC, qkv_body, 0)

    scale = HD ** -0.5
    jpos = lax.broadcasted_iota(jnp.int32, (SEQ, SEQ), 0)
    ipos = lax.broadcasted_iota(jnp.int32, (SEQ, SEQ), 1)
    causal = jpos <= ipos
    jf = jpos.astype(F32)
    base = jnp.where(me == 0, 1.0, jnp.where(me == 1, 0.25, jnp.where(me == 2, 0.0625, 0.015625))).astype(F32)

    def head(h, t):
        r0 = h * 3 * HD + t * HD
        return qkvt[r0:r0 + HD, :]

    for h in range(NH):
        s = dot(head(h, 1), head(h, 0), TN) * scale + (base * SLOPES[h]) * jf
        s = jnp.where(causal, s, MASK_VALUE)
        e = jnp.exp(s - jnp.max(s, axis=0, keepdims=True))
        p = e * (1.0 / jnp.sum(e, axis=0, keepdims=True))
        prob[h] = p
        lbuf[OFF_O + h * HD:OFF_O + (h + 1) * HD, :] = dot(head(h, 2), p.astype(BF16), NN).astype(BF16)
    for t in range(CTX // 128):
        ctx[:, t * 128:(t + 1) * 128] = lbuf[OFF_O + t * 128:OFF_O + (t + 1) * 128, :].T

    wcopies[1].wait()
    sc_a.run(lambda cols: dot(ctx[...], wo[:, cols], NN), 3)
    sc_a.relay_from(sc_a.n - 3)

    for c in range(AGC):
        gat_m.forward(c)
    wcopies[2].wait()
    gat_m.finish()
    emit(rbuf.at[1], r_hbm.at[1])
    FC = 512

    def dact_body(n, carry):
        f0 = pl.multiple_of(n * FC, FC)
        dact[:, pl.ds(f0, FC)] = dot(rbuf[1], wd[pl.ds(f0, FC), :], NT).astype(BF16)
        return carry
    lax.fori_loop(0, FF // FC, dact_body, 0)

    sc_a.arrive()
    for b, i in blocks:
        xm = xh[b].astype(F32) + sc_a.block(b) + bo[...]
        if i == 0:
            x1[...] = xm
        xhat, rstd = ln_stats(xm)
        xn2[b] = xhat
        rs[b] = jnp.broadcast_to(rstd, (ROWS, 128))
        gbuf[block_rows(b), :] = (xhat * g2[...] + b2[...]).astype(BF16)
        sh_g.send(b, i)
    wcopies[3].wait()
    for b, i in blocks:
        sh_g.finish(b, i)

    UC = 512
    k0 = 0.7978845608028654
    k1 = 0.044715

    for f0 in range(0, FF, UC):
        cols = pl.ds(f0, UC)
        v = dot(gbuf[...], wu[:, cols], NN) + bu[:, cols]
        v2 = v * v
        t = jnp.tanh(k0 * (v + k1 * (v2 * v)))
        hp = 0.5 * (1.0 + t)
        act[:, cols] = (v * hp).astype(BF16)
        dg = hp + (0.5 * k0) * v * (1.0 - t * t) * (1.0 + (3.0 * k1) * v2)
        dpre = dact[:, cols].astype(F32) * dg
        gbu[:, cols] = jnp.sum(dpre, axis=0, keepdims=True)
        rbuf[0, :, cols] = dpre.astype(BF16)
    emit(rbuf.at[0], r_hbm.at[0])
    emit(gbu, gbu_hbm)

    def dg_chunk(cols):
        return dot(rbuf[0], wu[cols, :], NT)
    sc_g.run(dg_chunk, 1)

    def rest(n):
        if n == 0:
            sc_g.relay(sc_g.n - 1)
    sc_y.run(lambda cols: dot(act[...], wd[:, cols], NN), sc_y.n, rest)
    va[3:4, :] = jnp.sum(rbuf[1, rows(me), :].astype(F32), axis=0, keepdims=True)

    sc_g.arrive()
    for b, i in blocks:
        dgl = sc_g.block(b)
        xhat, rstd = xn2[b], rs[b, :, 0:1]
        dm = rbuf[1, block_rows(b), :].astype(F32) + ln_grad(dgl, xhat, rstd, g2[...])
        rbuf[3, block_rows(b), :] = dm.astype(BF16)
        sh_a.send(b, i)
        if i == 0:
            dmid[...] = dm
    va[2:3, :] = jnp.sum(dmid[...], axis=0, keepdims=True)
    dgl = sc_g.block(ax)
    va[0:1, :] = jnp.sum(dgl * xn2[ax], axis=0, keepdims=True)
    va[1:2, :] = jnp.sum(dgl, axis=0, keepdims=True)

    sva, rva = alloc('s', 3), alloc('r', 3)

    def vec_copy(buf, hbm, s, r, i, owner, dev):
        return remote(buf, hbm.at[owner], s + i, r + i, dev)
    sc_y.relay_from(0)
    for i, dev in enumerate(peers):
        vec_copy(va, va_hbm, sva, rva, i, me, dev).start()
    emit(va, va_hbm.at[me])
    for b, i in blocks:
        sh_a.finish(b, i)
    emit(rbuf.at[3], r_hbm.at[3])

    ctx[...] = dot(rbuf[3], wo[...], NT).astype(BF16)
    for t in range(CTX // 128):
        dctxt[t * 128:(t + 1) * 128, :] = ctx[:, t * 128:(t + 1) * 128].T

    for h in range(NH):
        dot_h = dctxt[h * HD:(h + 1) * HD, :]
        p = prob[h]
        dp = dot(head(h, 2), dot_h, TN).astype(BF16).astype(F32)
        ds = (p * (dp - jnp.sum(dp * p, axis=0, keepdims=True))).astype(BF16)
        r0 = OFF_QKV + h * 3 * HD
        lbuf[r0:r0 + HD, :] = (dot(head(h, 1), ds, NN) * scale).astype(BF16)
        lbuf[r0 + HD:r0 + 2 * HD, :] = (dot(head(h, 0), ds, NT) * scale).astype(BF16)
        lbuf[r0 + 2 * HD:r0 + 3 * HD, :] = dot(dot_h, p.astype(BF16), NT).astype(BF16)
    for t in range(QKV // 128):
        dqkv[:, t * 128:(t + 1) * 128] = lbuf[OFF_QKV + t * 128:OFF_QKV + (t + 1) * 128, :].T
    emit(lbuf.at[pl.ds(OFF_QKV, QKV + CTX)], l_hbm.at[pl.ds(OFF_QKV, QKV + CTX)])

    sc_h.run(lambda cols: dot(dqkv[...], wq[:, cols], NN), 2)
    sc_h.relay_from(sc_h.n - 2)

    sc_y.arrive()
    outb[0] = (x1[...] + sc_y.own() + bd[...]).astype(BF16)
    emit(outb.at[0], y_hbm)
    def tr_body(src, off):
        def body(n, carry):
            r0 = pl.multiple_of(n * 512, 512)
            lbuf[pl.ds(off + r0, 512), :] = src[:, pl.ds(r0, 512)].T
            return carry
        return body
    lax.fori_loop(0, FF // 512, tr_body(act, OFF_ACT), 0)
    lax.fori_loop(0, D // 512, tr_body(gbuf, OFF_G), 0)
    emit(lbuf.at[pl.ds(0, OFF_QKV)], l_hbm.at[pl.ds(0, OFF_QKV)])

    sc_h.arrive()
    dhl = sc_h.own()
    xhat1, rstd1 = xn1[...], rs[2, :, 0:1]
    vb[0:1, :] = jnp.sum(dhl * xhat1, axis=0, keepdims=True)
    vb[1:2, :] = jnp.sum(dhl, axis=0, keepdims=True)
    svb, rvb = alloc('s', 3), alloc('r', 3)
    for i, dev in enumerate(peers):
        vec_copy(vb, vb_hbm, svb, rvb, i, me, dev).start()
    emit(vb, vb_hbm.at[me])
    outb[1] = (dmid[...] + ln_grad(dhl, xhat1, rstd1, g1[...])).astype(BF16)
    emit(outb.at[1], gx_hbm)
    remote(xh.at[ax], xh.at[ax], sx, rx, cross).wait_send()
    gat_m.drain()
    for g in (sh_h, sh_g, sh_a, sc_a, sc_g, sc_y, sc_h):
        g.drain()
    for i, dev in enumerate(peers):
        vec_copy(va, va_hbm, sva, rva, i, me, dev).wait_send()
        vec_copy(va, va_hbm, sva, rva, i, dev, dev).wait_recv()
    for i, dev in enumerate(peers):
        vec_copy(vb, vb_hbm, svb, rvb, i, dev, dev).wait_recv()
    for i, dev in enumerate(peers):
        vec_copy(vb, vb_hbm, svb, rvb, i, me, dev).wait_send()
    for c in outs:
        c.wait()
    assert (count['s'], count['r']) == (NS, NR), count


GR = 1280
SLOTS = 3
SECTIONS = ((OFF_ACT, FF, 1), (OFF_G, D, 0), (OFF_QKV, QKV, 2), (OFF_O, CTX, 3))
PIECES = (((160, 1), (160, 1), (320, 1), (640, 1), (GR, 1)), ((GR, 2),), ((GR, 1), (640, 1)), ((320, 1), (160, 1), (160, 1)))
SMALL = 8


def grad_kernel(y_in, gx_in, va_in, vb_in, gbu_in, l_hbm, r_hbm, y_out, gx_out, v0, v1, v2, v3, v4, v5, gbq_hbm, gbu_out,
                dwq, dwo, dwu, dwd, lv, rv, st, st2, yv, gxv, vav, vbv, vv, gv, gbq, isem, ssem, ssem2, psem, osem):
    loads = []
    for i, (off, n, r) in enumerate(SECTIONS):
        cl = pltpu.make_async_copy(l_hbm.at[pl.ds(off, n)], lv.at[pl.ds(off, n)], isem.at[2 * i])
        cr = pltpu.make_async_copy(r_hbm.at[r], rv.at[r], isem.at[2 * i + 1])
        cl.start()
        cr.start()
        loads.append((cl, cr))
    passes = [(y_in, yv, y_out), (gx_in, gxv, gx_out), (gbu_in, gv, gbu_out)]
    srcs = (yv, gxv, gv.at[0])
    pin = [pltpu.make_async_copy(a, b, psem.at[i]) for i, (a, b, _) in enumerate(passes)]
    pin.append(pltpu.make_async_copy(va_in, vav, psem.at[3]))
    pin.append(pltpu.make_async_copy(vb_in, vbv, psem.at[4]))
    for c in pin:
        c.start()
    douts = (dwd, dwu, dwq, dwo)
    step = 0

    def out_copy(slot, dst, r0):
        return pltpu.make_async_copy(st.at[slot], dst.at[pl.ds(r0, GR)], ssem.at[slot])
    smalls = []
    for i, (off, n, r) in enumerate(SECTIONS):
        loads[i][0].wait()
        loads[i][1].wait()
        dst = douts[i]
        r0 = 0
        for gr, times in PIECES[i]:
            if gr < GR:
                e = len(smalls)

                def small(m, carry, off=off + r0, gr=gr, e=e, r=r):
                    st2[e, 0:gr] = dot(lv[pl.ds(pl.multiple_of(off + m * gr, 32), gr), :], rv[r], NN).astype(BF16)
                    return carry
                lax.fori_loop(0, 1, small, 0)
                smalls.append(pltpu.make_async_copy(st2.at[e, pl.ds(0, gr)], dst.at[pl.ds(r0, gr)], ssem2.at[e]))
                smalls[-1].start()
            else:
                def body(m, carry, off=off + r0, r=r, dst=dst, step=step, r0=r0):
                    slot = lax.rem(m + step, SLOTS)

                    @pl.when(m + step >= SLOTS)
                    def _():
                        out_copy(slot, dwd, 0).wait()
                    st[slot] = dot(lv[pl.ds(pl.multiple_of(off + m * GR, 64), GR), :], rv[r], NN).astype(BF16)
                    out_copy(slot, dst, pl.multiple_of(r0 + m * GR, 64)).start()
                    return carry
                lax.fori_loop(0, times, body, 0)
                step += times
            r0 += gr * times
        if i == 0:
            for c in pin:
                c.wait()
            for buf, first, n in ((vav, 0, 4), (vbv, 4, 2)):
                tot = (buf[0] + buf[1]) + (buf[2] + buf[3])
                for j in range(n):
                    vv[first + j] = tot[j:j + 1]
        if i == 2:
            ones = jnp.ones((16, SEQ), BF16)
            for h in range(NH):
                for t in range(3):
                    q0 = OFF_QKV + h * 3 * HD + t * HD
                    gbq[t, h:h + 1, :] = dot(ones, lv[q0:q0 + HD, :], NT)[0:1]
    done = []
    for i, (_, _, o) in enumerate(passes):
        done.append(pltpu.make_async_copy(srcs[i], o, osem.at[i]))
    for i, o in enumerate((v0, v1, v2, v3, v4, v5)):
        done.append(pltpu.make_async_copy(vv.at[i, 0], o, osem.at[3 + i]))
    done.append(pltpu.make_async_copy(gbq, gbq_hbm, osem.at[9]))
    for c in done:
        c.start()
    for slot in range(SLOTS):
        out_copy(slot, dwd, 0).wait()
    for c in smalls:
        c.wait()
    for c in done:
        c.wait()


def solution(mesh):
    def local_step(x, ln1_gamma, ln1_beta, w_qkv, b_qkv, w_out, b_out, ln2_gamma, ln2_beta, w_up, b_up, w_down, b_down, grad_y):
        wqt = jnp.transpose(w_qkv, (1, 2, 3, 0)).reshape(QKV, D)
        any_spec = pl.BlockSpec(memory_space=pl.ANY)
        sds = jax.ShapeDtypeStruct
        y, gx, pva, pvb, gbu, lmat, rmat = pl.pallas_call(
            block_kernel,
            name='block',
            out_shape=(sds((ROWS, D), BF16), sds((ROWS, D), BF16), sds((TP, 4, D), F32), sds((TP, 2, D), F32), sds((1, FF), F32),
                       sds((LROWS, SEQ), BF16), sds((4, SEQ, D), BF16)),
            in_specs=[any_spec] * 14,
            out_specs=(any_spec,) * 7,
            scratch_shapes=[
                pltpu.VMEM((QKV, D), BF16), pltpu.VMEM((CTX, D), BF16), pltpu.VMEM((D, FF), BF16), pltpu.VMEM((FF, D), BF16),
                pltpu.VMEM((2, ROWS, D), BF16),
                pltpu.VMEM((1, D), F32), pltpu.VMEM((1, D), F32), pltpu.VMEM((3, NH, HD), F32), pltpu.VMEM((1, QKV), F32),
                pltpu.VMEM((1, D), F32), pltpu.VMEM((1, D), F32), pltpu.VMEM((1, D), F32), pltpu.VMEM((1, FF), F32), pltpu.VMEM((1, D), F32),
                pltpu.VMEM((4, SEQ, D), BF16), pltpu.VMEM((LROWS, SEQ), BF16), pltpu.VMEM((SEQ, D), BF16),
                pltpu.VMEM((QKV, SEQ), BF16), pltpu.VMEM((SEQ, QKV), BF16), pltpu.VMEM((SEQ, CTX), BF16),
                pltpu.VMEM((CTX, SEQ), BF16), pltpu.VMEM((NH, SEQ, SEQ), F32),
                pltpu.VMEM((SEQ, FF), BF16), pltpu.VMEM((SEQ, FF), BF16),
                pltpu.VMEM((ROWS, D), F32), pltpu.VMEM((ROWS, D), F32), pltpu.VMEM((2, ROWS, D), F32), pltpu.VMEM((3, ROWS, 128), F32),
                pltpu.VMEM((ROWS, D), F32), pltpu.VMEM((2, ROWS, D), BF16),
                pltpu.VMEM((1, FF), F32),
                pltpu.VMEM((4, D), F32), pltpu.VMEM((2, D), F32),
                pltpu.VMEM((4, 2, 2, ROWS, D), BF16), pltpu.VMEM((4, 2, ROWS, D), BF16),
                pltpu.VMEM((4, 2, ROWS, D), BF16), pltpu.VMEM((4, 2, ROWS, D), BF16),
                pltpu.SemaphoreType.DMA((4,)), pltpu.SemaphoreType.DMA((10,)), pltpu.SemaphoreType.DMA((11,)),
                pltpu.SemaphoreType.DMA((NS,)), pltpu.SemaphoreType.DMA((NR,)),
            ],
            compiler_params=pltpu.CompilerParams(collective_id=0, has_side_effects=True, vmem_limit_bytes=66_000_000),
            cost_estimate=pl.CostEstimate(flops=10_000_000_000, bytes_accessed=45_000_000, transcendentals=1_000_000),
        )(x[0], grad_y[0], wqt, w_out, w_up, w_down, ln1_gamma, ln1_beta, jnp.transpose(b_qkv, (1, 0, 2)), b_out,
          ln2_gamma, ln2_beta, b_up, b_down)
        y, gx, v0, v1, v2, v3, v4, v5, gbq, gbu, dwq, dwo, dwu, dwd = pl.pallas_call(
            grad_kernel,
            name='weight_grads',
            out_shape=(sds((ROWS, D), BF16), sds((ROWS, D), BF16)) + (sds((D,), F32),) * 6 + (
                sds((3, NH, HD), F32), sds((FF,), F32), sds((QKV, D), BF16), sds((CTX, D), BF16), sds((D, FF), BF16), sds((FF, D), BF16)),
            in_specs=[any_spec] * 7,
            out_specs=(any_spec,) * 14,
            scratch_shapes=[
                pltpu.VMEM((LROWS, SEQ), BF16), pltpu.VMEM((4, SEQ, D), BF16), pltpu.VMEM((SLOTS, GR, D), BF16), pltpu.VMEM((SMALL, 640, D), BF16),
                pltpu.VMEM((ROWS, D), BF16), pltpu.VMEM((ROWS, D), BF16), pltpu.VMEM((TP, 4, D), F32), pltpu.VMEM((TP, 2, D), F32),
                pltpu.VMEM((6, 1, D), F32), pltpu.VMEM((1, FF), F32),
                pltpu.VMEM((3, NH, HD), F32),
                pltpu.SemaphoreType.DMA((8,)), pltpu.SemaphoreType.DMA((SLOTS,)), pltpu.SemaphoreType.DMA((SMALL,)), pltpu.SemaphoreType.DMA((5,)), pltpu.SemaphoreType.DMA((10,)),
            ],
            compiler_params=pltpu.CompilerParams(vmem_limit_bytes=66_000_000),
            cost_estimate=pl.CostEstimate(flops=5_000_000_000, bytes_accessed=44_000_000, transcendentals=0),
        )(y, gx, pva, pvb, gbu, lmat, rmat)
        g_wqkv = jnp.transpose(dwq.reshape(NH, 3, HD, D), (3, 0, 1, 2))
        g_ln2g, g_ln2b, g_bo, g_bd, g_ln1g, g_ln1b = v0, v1, v2, v3, v4, v5
        return (y[None], gx[None], g_ln1g, g_ln1b, g_wqkv, jnp.transpose(gbq, (1, 0, 2)), dwo, g_bo,
                g_ln2g, g_ln2b, dwu, gbu, dwd, g_bd)

    row_spec = P('dp', 'tp', None)
    in_specs = (row_spec, P(), P(), P(None, 'tp', None, None), P('tp', None, None), P('tp', None), P(), P(), P(),
                P(None, 'tp'), P('tp'), P('tp', None), P(), row_spec)
    out_specs = (row_spec, row_spec, P('dp'), P('dp'), P('dp', 'tp', None, None), P(('dp', 'tp'), None, None),
                 P(('dp', 'tp'), None), P('dp'), P('dp'), P('dp'), P('dp', 'tp'), P(('dp', 'tp')), P(('dp', 'tp'), None), P('dp'))
    return jax.shard_map(local_step, mesh=mesh, in_specs=in_specs, out_specs=out_specs, check_vma=False)
```

```python
import jax
import jax.numpy as jnp
from jax import lax
from jax.experimental import pallas as pl
from jax.experimental.pallas import tpu as pltpu
from jax.sharding import PartitionSpec as P

EPS = 1e-5
MASK_VALUE = -1e30
MESH = pl.DeviceIdType.MESH
F32 = jnp.float32
BF16 = jnp.bfloat16

D = 2560
SEQ = 128
TP = 4
ROWS = SEQ // TP
NH = 8
HD = 80
QKV = NH * 3 * HD
CTX = NH * HD
FF = 2560
AGC = 4
NS, NR = 24, 48
AGW = D // AGC
CHUNKS = (256, 256, 512, 512, 512, 256, 256)
Y_CHUNKS = (640,) * 4
OFF_G, OFF_ACT, OFF_QKV, OFF_O = 0, D, D + FF, D + FF + QKV
LROWS = D + FF + QKV + CTX
SLOPES = [2.0 ** (-(h + 1) / 4.0) for h in range(NH)]
NT = (((1,), (1,)), ((), ()))
NN = (((1,), (0,)), ((), ()))
TN = (((0,), (0,)), ((), ()))


def dot(a, b, dims):
    return lax.dot_general(a, b, dims, preferred_element_type=F32)


def ln_stats(v):
    mean = jnp.mean(v, axis=-1, keepdims=True)
    cen = v - mean
    var = jnp.mean(cen * cen, axis=-1, keepdims=True)
    rstd = lax.rsqrt(var + EPS)
    return cen * rstd, rstd


def ln_grad(dy, xhat, rstd, gain):
    dxh = dy * gain
    m1 = jnp.mean(dxh, axis=-1, keepdims=True)
    m2 = jnp.mean(dxh * xhat, axis=-1, keepdims=True)
    return rstd * (dxh - m1 - xhat * m2)


def block_kernel(x_hbm, gy_hbm, wq_hbm, wo_hbm, wu_hbm, wd_hbm, g1_hbm, b1_hbm, bq_hbm, bo_hbm, g2_hbm, b2_hbm, bu_hbm,
                 bd_hbm, y_hbm, gx_hbm, va_hbm, vb_hbm, gbu_hbm, l_hbm, r_hbm,
                 wq, wo, wu, wd, xh, g1, b1, bqv, bq, bo, g2, b2, bu, bd,
                 rbuf, lbuf, gbuf, qkvt, dqkv, ctx, dctxt, prob, act, dact, x1, xn1, xn2, rs, dmid, outb, gbu, va, vb,
                 pb, rx1, sb, rx2, wsem, lsem, osem, ssem, rsem):
    me = lax.axis_index('tp')
    ax = lax.div(me, 2)
    ak = lax.rem(me, 2)
    partner = 2 * ax + (1 - ak)
    cross = 2 * (1 - ax) + ak
    diag = 2 * (1 - ax) + (1 - ak)
    peers = (partner, cross, diag)

    def rows(i):
        return pl.ds(pl.multiple_of(i * ROWS, ROWS), ROWS)

    def block_rows(b):
        return rows(2 * b + ak)

    count = {'s': 0, 'r': 0}

    def alloc(kind, n=1):
        base = count[kind]
        count[kind] += n
        return base

    def remote(src, dst, si, ri, dev):
        return pltpu.make_async_remote_copy(src_ref=src, dst_ref=dst, send_sem=ssem.at[si], recv_sem=rsem.at[ri],
                                            device_id={'tp': dev}, device_id_type=MESH)

    x_load = pltpu.make_async_copy(x_hbm, xh.at[ax], lsem.at[0])
    x_load.start()
    small = [(g1_hbm, g1.at[0]), (b1_hbm, b1.at[0]), (bq_hbm, bqv), (bo_hbm, bo.at[0]), (g2_hbm, g2.at[0]), (b2_hbm, b2.at[0]),
             (bu_hbm, bu.at[0]), (bd_hbm, bd.at[0])]
    loads = [pltpu.make_async_copy(s, d, lsem.at[1 + i]) for i, (s, d) in enumerate(small)]
    for c in loads:
        c.start()
    gy_load = pltpu.make_async_copy(gy_hbm, rbuf.at[1, rows(me)], lsem.at[1 + len(small)])
    gy_load.start()
    wcopies = [pltpu.make_async_copy(s, d, wsem.at[i])
               for i, (s, d) in enumerate([(wq_hbm, wq), (wo_hbm, wo), (wd_hbm, wd), (wu_hbm, wu)])]

    bar = pltpu.get_barrier_semaphore()
    for dev in peers:
        pl.semaphore_signal(bar, inc=1, device_id={'tp': dev}, device_id_type=MESH)
    wcopies[0].start()
    wcopies[1].start()

    class Gather:
        def __init__(self, full):
            self.full = full
            self.s = alloc('s', 3)
            self.r = alloc('r', AGC + 2)

        def chunk(self, dev, c):
            return self.full.at[rows(dev), pl.ds(c * AGW, AGW)]

        def cross_copy(self, dev, c):
            ref = self.chunk(dev, c)
            return remote(ref, ref, self.s, self.r + c, cross)

        def fwd_copy(self, dev, c):
            ref = self.chunk(dev, c)
            return remote(ref, ref, self.s + 1, self.r + AGC, partner)

        def whole(self, dev, i, j, to):
            ref = self.full.at[rows(dev)]
            return remote(ref, ref, self.s + i, self.r + j, to)

        def own_copy(self, dev):
            return self.whole(dev, 2, AGC + 1, partner)

        def start(self):
            for c in range(AGC):
                self.cross_copy(me, c).start()
            self.own_copy(me).start()

        def forward(self, c):
            self.cross_copy(cross, c).wait_recv()
            self.fwd_copy(cross, c).start()

        def finish(self):
            self.own_copy(partner).wait_recv()
            self.whole(diag, 1, AGC, partner).wait_recv()

        def drain(self):
            self.whole(me, 0, 0, cross).wait_send()
            self.whole(cross, 1, AGC, partner).wait_send()
            self.own_copy(me).wait_send()

    class Share:
        def __init__(self, full):
            self.full = full
            self.s = alloc('s', 2)
            self.r = alloc('r', 2)

        def copy(self, b, k, i):
            ref = self.full.at[rows(2 * b + k)]
            return remote(ref, ref, self.s + i, self.r + i, partner)

        def send(self, b, i):
            self.copy(b, ak, i).start()

        def finish(self, b, i):
            self.copy(b, 1 - ak, i).wait_recv()

        def drain(self):
            self.copy(ax, ak, 0).wait_send()
            self.copy(1 - ax, ak, 1).wait_send()

    class Reduce:
        def __init__(self, i, both, chunks=CHUNKS):
            self.p, self.x1, self.sb, self.x2 = pb.at[i], rx1.at[i], sb.at[i], rx2.at[i]
            self.both = both
            self.chunks = chunks
            self.n = len(chunks)
            self.s = alloc('s', 2)
            self.r = alloc('r', self.n + 1)

        def cols(self, n):
            return pl.ds(sum(self.chunks[:n]), self.chunks[n])

        def pair(self, n):
            return remote(self.p.at[:, 1 - ak, :, self.cols(n)], self.x1.at[:, :, self.cols(n)], self.s, self.r + n, partner)

        def over(self, c):
            if self.both:
                src, dst = self.sb.at[:, :, c], self.x2.at[:, :, c]
            else:
                src, dst = self.sb.at[0, :, c], self.x2.at[0, :, c]
            return remote(src, dst, self.s + 1, self.r + self.n, cross)

        def produce(self, n, val):
            self.p[:, :, :, self.cols(n)] = val.astype(BF16).reshape(2, 2, ROWS, self.chunks[n])
            self.pair(n).start()

        def relay(self, n):
            self.pair(n).wait_recv()
            c = self.cols(n)
            if self.both:
                self.sb[:, :, c] = (self.p[:, ak, :, c].astype(F32) + self.x1[:, :, c].astype(F32)).astype(BF16)
            else:
                self.sb[0, :, c] = (self.p[1 - ax, ak, :, c].astype(F32) + self.x1[1 - ax, :, c].astype(F32)).astype(BF16)
            self.over(c).start()

        def run(self, fn, lag, also=None):
            for n in range(self.n):
                self.produce(n, fn(self.cols(n)))
                if n >= lag:
                    self.relay(n - lag)
                if also is not None:
                    also(n)

        def relay_from(self, first):
            for n in range(first, self.n):
                self.relay(n)

        def arrive(self):
            self.over(slice(None)).wait_recv()

        def block(self, b):
            return (self.sb[b].astype(F32) + self.x2[b].astype(F32)).astype(BF16).astype(F32)

        def own(self):
            v = self.p[ax, ak].astype(F32) + self.x1[ax].astype(F32) + self.x2[0].astype(F32)
            return v.astype(BF16).astype(F32)

        def drain(self):
            remote(self.p.at[:, 1 - ak], self.x1, self.s, self.r, partner).wait_send()
            self.over(slice(None)).wait_send()

    gat_m = Gather(rbuf.at[1])
    sh_h, sh_g, sh_a = Share(rbuf.at[2]), Share(gbuf), Share(rbuf.at[3])
    sc_a, sc_g, sc_y, sc_h = Reduce(0, True), Reduce(1, True), Reduce(2, False, Y_CHUNKS), Reduce(3, False)
    blocks = ((ax, 0), (1 - ax, 1))
    outs = []

    def emit(src, dst):
        c = pltpu.make_async_copy(src, dst, osem.at[len(outs)])
        c.start()
        outs.append(c)

    sx, rx = alloc('s'), alloc('r')
    x_load.wait()
    pl.semaphore_wait(bar, 3)
    remote(xh.at[ax], xh.at[ax], sx, rx, cross).start()
    for c in loads:
        c.wait()
    bq[...] = jnp.concatenate([bqv[t, h:h + 1, :] for h in range(NH) for t in range(3)], axis=1)
    for b, i in blocks:
        if i == 1:
            remote(xh.at[1 - ax], xh.at[1 - ax], sx, rx, cross).wait_recv()
        xhat, rstd = ln_stats(xh[b].astype(F32))
        if i == 0:
            xn1[...] = xhat
            rs[2] = jnp.broadcast_to(rstd, (ROWS, 128))
        rbuf[2, block_rows(b), :] = (xhat * g1[...] + b1[...]).astype(BF16)
        sh_h.send(b, i)
    gy_load.wait()
    gat_m.start()
    wcopies[2].start()
    wcopies[3].start()
    wcopies[0].wait()
    for b, i in blocks:
        sh_h.finish(b, i)
    emit(rbuf.at[2], r_hbm.at[2])

    QC = 640

    def qkv_body(n, carry):
        r0 = pl.multiple_of(n * QC, QC)
        v = dot(rbuf[2], wq[pl.ds(r0, QC), :], NT) + bq[:, pl.ds(r0, QC)]
        qkvt[pl.ds(r0, QC), :] = v.astype(BF16).T
        return carry
    lax.fori_loop(0, QKV // QC, qkv_body, 0)

    scale = HD ** -0.5
    jpos = lax.broadcasted_iota(jnp.int32, (SEQ, SEQ), 0)
    ipos = lax.broadcasted_iota(jnp.int32, (SEQ, SEQ), 1)
    causal = jpos <= ipos
    jf = jpos.astype(F32)
    base = jnp.where(me == 0, 1.0, jnp.where(me == 1, 0.25, jnp.where(me == 2, 0.0625, 0.015625))).astype(F32)

    def head(h, t):
        r0 = h * 3 * HD + t * HD
        return qkvt[r0:r0 + HD, :]

    for h in range(NH):
        s = dot(head(h, 1), head(h, 0), TN) * scale + (base * SLOPES[h]) * jf
        s = jnp.where(causal, s, MASK_VALUE)
        e = jnp.exp(s - jnp.max(s, axis=0, keepdims=True))
        p = e * (1.0 / jnp.sum(e, axis=0, keepdims=True))
        prob[h] = p
        lbuf[OFF_O + h * HD:OFF_O + (h + 1) * HD, :] = dot(head(h, 2), p.astype(BF16), NN).astype(BF16)
    for t in range(CTX // 128):
        ctx[:, t * 128:(t + 1) * 128] = lbuf[OFF_O + t * 128:OFF_O + (t + 1) * 128, :].T

    wcopies[1].wait()
    sc_a.run(lambda cols: dot(ctx[...], wo[:, cols], NN), 3)
    sc_a.relay_from(sc_a.n - 3)

    for c in range(AGC):
        gat_m.forward(c)
    wcopies[2].wait()
    gat_m.finish()
    emit(rbuf.at[1], r_hbm.at[1])
    FC = 512

    def dact_body(n, carry):
        f0 = pl.multiple_of(n * FC, FC)
        dact[:, pl.ds(f0, FC)] = dot(rbuf[1], wd[pl.ds(f0, FC), :], NT).astype(BF16)
        return carry
    lax.fori_loop(0, FF // FC, dact_body, 0)

    sc_a.arrive()
    for b, i in blocks:
        xm = xh[b].astype(F32) + sc_a.block(b) + bo[...]
        if i == 0:
            x1[...] = xm
        xhat, rstd = ln_stats(xm)
        xn2[b] = xhat
        rs[b] = jnp.broadcast_to(rstd, (ROWS, 128))
        gbuf[block_rows(b), :] = (xhat * g2[...] + b2[...]).astype(BF16)
        sh_g.send(b, i)
    wcopies[3].wait()
    for b, i in blocks:
        sh_g.finish(b, i)

    UC = 512
    k0 = 0.7978845608028654
    k1 = 0.044715

    for f0 in range(0, FF, UC):
        cols = pl.ds(f0, UC)
        v = dot(gbuf[...], wu[:, cols], NN) + bu[:, cols]
        v2 = v * v
        t = jnp.tanh(k0 * (v + k1 * (v2 * v)))
        hp = 0.5 * (1.0 + t)
        act[:, cols] = (v * hp).astype(BF16)
        dg = hp + (0.5 * k0) * v * (1.0 - t * t) * (1.0 + (3.0 * k1) * v2)
        dpre = dact[:, cols].astype(F32) * dg
        gbu[:, cols] = jnp.sum(dpre, axis=0, keepdims=True)
        rbuf[0, :, cols] = dpre.astype(BF16)
    emit(rbuf.at[0], r_hbm.at[0])
    emit(gbu, gbu_hbm)

    def dg_chunk(cols):
        return dot(rbuf[0], wu[cols, :], NT)
    sc_g.run(dg_chunk, 1)

    def rest(n):
        if n == 0:
            sc_g.relay(sc_g.n - 1)
    sc_y.run(lambda cols: dot(act[...], wd[:, cols], NN), sc_y.n, rest)
    va[3:4, :] = jnp.sum(rbuf[1, rows(me), :].astype(F32), axis=0, keepdims=True)

    sc_g.arrive()
    for b, i in blocks:
        dgl = sc_g.block(b)
        xhat, rstd = xn2[b], rs[b, :, 0:1]
        dm = rbuf[1, block_rows(b), :].astype(F32) + ln_grad(dgl, xhat, rstd, g2[...])
        rbuf[3, block_rows(b), :] = dm.astype(BF16)
        sh_a.send(b, i)
        if i == 0:
            dmid[...] = dm
    va[2:3, :] = jnp.sum(dmid[...], axis=0, keepdims=True)
    dgl = sc_g.block(ax)
    va[0:1, :] = jnp.sum(dgl * xn2[ax], axis=0, keepdims=True)
    va[1:2, :] = jnp.sum(dgl, axis=0, keepdims=True)

    sva, rva = alloc('s', 3), alloc('r', 3)

    def vec_copy(buf, hbm, s, r, i, owner, dev):
        return remote(buf, hbm.at[owner], s + i, r + i, dev)
    sc_y.relay_from(0)
    for i, dev in enumerate(peers):
        vec_copy(va, va_hbm, sva, rva, i, me, dev).start()
    emit(va, va_hbm.at[me])
    for b, i in blocks:
        sh_a.finish(b, i)
    emit(rbuf.at[3], r_hbm.at[3])

    ctx[...] = dot(rbuf[3], wo[...], NT).astype(BF16)
    for t in range(CTX // 128):
        dctxt[t * 128:(t + 1) * 128, :] = ctx[:, t * 128:(t + 1) * 128].T

    for h in range(NH):
        dot_h = dctxt[h * HD:(h + 1) * HD, :]
        p = prob[h]
        dp = dot(head(h, 2), dot_h, TN).astype(BF16).astype(F32)
        ds = (p * (dp - jnp.sum(dp * p, axis=0, keepdims=True))).astype(BF16)
        r0 = OFF_QKV + h * 3 * HD
        lbuf[r0:r0 + HD, :] = (dot(head(h, 1), ds, NN) * scale).astype(BF16)
        lbuf[r0 + HD:r0 + 2 * HD, :] = (dot(head(h, 0), ds, NT) * scale).astype(BF16)
        lbuf[r0 + 2 * HD:r0 + 3 * HD, :] = dot(dot_h, p.astype(BF16), NT).astype(BF16)
    for t in range(QKV // 128):
        dqkv[:, t * 128:(t + 1) * 128] = lbuf[OFF_QKV + t * 128:OFF_QKV + (t + 1) * 128, :].T
    emit(lbuf.at[pl.ds(OFF_QKV, QKV + CTX)], l_hbm.at[pl.ds(OFF_QKV, QKV + CTX)])

    sc_h.run(lambda cols: dot(dqkv[...], wq[:, cols], NN), 2)
    sc_h.relay_from(sc_h.n - 2)

    sc_y.arrive()
    outb[0] = (x1[...] + sc_y.own() + bd[...]).astype(BF16)
    emit(outb.at[0], y_hbm)
    def tr_body(src, off):
        def body(n, carry):
            r0 = pl.multiple_of(n * 512, 512)
            lbuf[pl.ds(off + r0, 512), :] = src[:, pl.ds(r0, 512)].T
            return carry
        return body
    lax.fori_loop(0, FF // 512, tr_body(act, OFF_ACT), 0)
    lax.fori_loop(0, D // 512, tr_body(gbuf, OFF_G), 0)
    emit(lbuf.at[pl.ds(0, OFF_QKV)], l_hbm.at[pl.ds(0, OFF_QKV)])

    sc_h.arrive()
    dhl = sc_h.own()
    xhat1, rstd1 = xn1[...], rs[2, :, 0:1]
    vb[0:1, :] = jnp.sum(dhl * xhat1, axis=0, keepdims=True)
    vb[1:2, :] = jnp.sum(dhl, axis=0, keepdims=True)
    svb, rvb = alloc('s', 3), alloc('r', 3)
    for i, dev in enumerate(peers):
        vec_copy(vb, vb_hbm, svb, rvb, i, me, dev).start()
    emit(vb, vb_hbm.at[me])
    outb[1] = (dmid[...] + ln_grad(dhl, xhat1, rstd1, g1[...])).astype(BF16)
    emit(outb.at[1], gx_hbm)
    remote(xh.at[ax], xh.at[ax], sx, rx, cross).wait_send()
    gat_m.drain()
    for g in (sh_h, sh_g, sh_a, sc_a, sc_g, sc_y, sc_h):
        g.drain()
    for i, dev in enumerate(peers):
        vec_copy(va, va_hbm, sva, rva, i, me, dev).wait_send()
        vec_copy(va, va_hbm, sva, rva, i, dev, dev).wait_recv()
    for i, dev in enumerate(peers):
        vec_copy(vb, vb_hbm, svb, rvb, i, dev, dev).wait_recv()
    for i, dev in enumerate(peers):
        vec_copy(vb, vb_hbm, svb, rvb, i, me, dev).wait_send()
    for c in outs:
        c.wait()
    assert (count['s'], count['r']) == (NS, NR), count


GR = 640
SLOTS = 4
SECTIONS = ((OFF_ACT, FF, 1), (OFF_G, D, 0), (OFF_QKV, QKV, 2), (OFF_O, CTX, 3))
PIECES = (((160, 1), (160, 1), (320, 1), (GR, 3)), ((GR, 4),), ((GR, 3),), ((320, 1), (160, 1), (160, 1)))
SMALL = 6


def grad_kernel(y_in, gx_in, va_in, vb_in, gbu_in, l_hbm, r_hbm, y_out, gx_out, v0, v1, v2, v3, v4, v5, gbq_hbm, gbu_out,
                dwq, dwo, dwu, dwd, lv, rv, st, st2, yv, gxv, vav, vbv, vv, gv, gbq, isem, ssem, ssem2, psem, osem):
    loads = []
    for i, (off, n, r) in enumerate(SECTIONS):
        cl = pltpu.make_async_copy(l_hbm.at[pl.ds(off, n)], lv.at[pl.ds(off, n)], isem.at[2 * i])
        cr = pltpu.make_async_copy(r_hbm.at[r], rv.at[r], isem.at[2 * i + 1])
        cl.start()
        cr.start()
        loads.append((cl, cr))
    passes = [(y_in, yv, y_out), (gx_in, gxv, gx_out), (gbu_in, gv, gbu_out)]
    srcs = (yv, gxv, gv.at[0])
    pin = [pltpu.make_async_copy(a, b, psem.at[i]) for i, (a, b, _) in enumerate(passes)]
    pin.append(pltpu.make_async_copy(va_in, vav, psem.at[3]))
    pin.append(pltpu.make_async_copy(vb_in, vbv, psem.at[4]))
    for c in pin:
        c.start()
    douts = (dwd, dwu, dwq, dwo)
    step = 0

    def out_copy(slot, dst, r0):
        return pltpu.make_async_copy(st.at[slot], dst.at[pl.ds(r0, GR)], ssem.at[slot])
    smalls = []
    for i, (off, n, r) in enumerate(SECTIONS):
        loads[i][0].wait()
        loads[i][1].wait()
        dst = douts[i]
        r0 = 0
        for gr, times in PIECES[i]:
            if gr < GR:
                e = len(smalls)

                def small(m, carry, off=off + r0, gr=gr, e=e, r=r):
                    st2[e, 0:gr] = dot(lv[pl.ds(pl.multiple_of(off + m * gr, 32), gr), :], rv[r], NN).astype(BF16)
                    return carry
                lax.fori_loop(0, 1, small, 0)
                smalls.append(pltpu.make_async_copy(st2.at[e, pl.ds(0, gr)], dst.at[pl.ds(r0, gr)], ssem2.at[e]))
                smalls[-1].start()
            else:
                def body(m, carry, off=off + r0, r=r, dst=dst, step=step, r0=r0):
                    slot = lax.rem(m + step, SLOTS)

                    @pl.when(m + step >= SLOTS)
                    def _():
                        out_copy(slot, dwd, 0).wait()
                    st[slot] = dot(lv[pl.ds(pl.multiple_of(off + m * GR, 64), GR), :], rv[r], NN).astype(BF16)
                    out_copy(slot, dst, pl.multiple_of(r0 + m * GR, 64)).start()
                    return carry
                lax.fori_loop(0, times, body, 0)
                step += times
            r0 += gr * times
        if i == 0:
            for c in pin:
                c.wait()
            for buf, first, n in ((vav, 0, 4), (vbv, 4, 2)):
                tot = (buf[0] + buf[1]) + (buf[2] + buf[3])
                for j in range(n):
                    vv[first + j] = tot[j:j + 1]
        if i == 2:
            ones = jnp.ones((16, SEQ), BF16)
            for h in range(NH):
                for t in range(3):
                    q0 = OFF_QKV + h * 3 * HD + t * HD
                    gbq[t, h:h + 1, :] = dot(ones, lv[q0:q0 + HD, :], NT)[0:1]
    done = []
    for i, (_, _, o) in enumerate(passes):
        done.append(pltpu.make_async_copy(srcs[i], o, osem.at[i]))
    for i, o in enumerate((v0, v1, v2, v3, v4, v5)):
        done.append(pltpu.make_async_copy(vv.at[i, 0], o, osem.at[3 + i]))
    done.append(pltpu.make_async_copy(gbq, gbq_hbm, osem.at[9]))
    for c in done:
        c.start()
    for slot in range(SLOTS):
        out_copy(slot, dwd, 0).wait()
    for c in smalls:
        c.wait()
    for c in done:
        c.wait()


def solution(mesh):
    def local_step(x, ln1_gamma, ln1_beta, w_qkv, b_qkv, w_out, b_out, ln2_gamma, ln2_beta, w_up, b_up, w_down, b_down, grad_y):
        wqt = jnp.transpose(w_qkv, (1, 2, 3, 0)).reshape(QKV, D)
        any_spec = pl.BlockSpec(memory_space=pl.ANY)
        sds = jax.ShapeDtypeStruct
        y, gx, pva, pvb, gbu, lmat, rmat = pl.pallas_call(
            block_kernel,
            name='block',
            out_shape=(sds((ROWS, D), BF16), sds((ROWS, D), BF16), sds((TP, 4, D), F32), sds((TP, 2, D), F32), sds((1, FF), F32),
                       sds((LROWS, SEQ), BF16), sds((4, SEQ, D), BF16)),
            in_specs=[any_spec] * 14,
            out_specs=(any_spec,) * 7,
            scratch_shapes=[
                pltpu.VMEM((QKV, D), BF16), pltpu.VMEM((CTX, D), BF16), pltpu.VMEM((D, FF), BF16), pltpu.VMEM((FF, D), BF16),
                pltpu.VMEM((2, ROWS, D), BF16),
                pltpu.VMEM((1, D), F32), pltpu.VMEM((1, D), F32), pltpu.VMEM((3, NH, HD), F32), pltpu.VMEM((1, QKV), F32),
                pltpu.VMEM((1, D), F32), pltpu.VMEM((1, D), F32), pltpu.VMEM((1, D), F32), pltpu.VMEM((1, FF), F32), pltpu.VMEM((1, D), F32),
                pltpu.VMEM((4, SEQ, D), BF16), pltpu.VMEM((LROWS, SEQ), BF16), pltpu.VMEM((SEQ, D), BF16),
                pltpu.VMEM((QKV, SEQ), BF16), pltpu.VMEM((SEQ, QKV), BF16), pltpu.VMEM((SEQ, CTX), BF16),
                pltpu.VMEM((CTX, SEQ), BF16), pltpu.VMEM((NH, SEQ, SEQ), F32),
                pltpu.VMEM((SEQ, FF), BF16), pltpu.VMEM((SEQ, FF), BF16),
                pltpu.VMEM((ROWS, D), F32), pltpu.VMEM((ROWS, D), F32), pltpu.VMEM((2, ROWS, D), F32), pltpu.VMEM((3, ROWS, 128), F32),
                pltpu.VMEM((ROWS, D), F32), pltpu.VMEM((2, ROWS, D), BF16),
                pltpu.VMEM((1, FF), F32),
                pltpu.VMEM((4, D), F32), pltpu.VMEM((2, D), F32),
                pltpu.VMEM((4, 2, 2, ROWS, D), BF16), pltpu.VMEM((4, 2, ROWS, D), BF16),
                pltpu.VMEM((4, 2, ROWS, D), BF16), pltpu.VMEM((4, 2, ROWS, D), BF16),
                pltpu.SemaphoreType.DMA((4,)), pltpu.SemaphoreType.DMA((10,)), pltpu.SemaphoreType.DMA((11,)),
                pltpu.SemaphoreType.DMA((NS,)), pltpu.SemaphoreType.DMA((NR,)),
            ],
            compiler_params=pltpu.CompilerParams(collective_id=0, has_side_effects=True, vmem_limit_bytes=66_000_000),
            cost_estimate=pl.CostEstimate(flops=10_000_000_000, bytes_accessed=45_000_000, transcendentals=1_000_000),
        )(x[0], grad_y[0], wqt, w_out, w_up, w_down, ln1_gamma, ln1_beta, jnp.transpose(b_qkv, (1, 0, 2)), b_out,
          ln2_gamma, ln2_beta, b_up, b_down)
        y, gx, v0, v1, v2, v3, v4, v5, gbq, gbu, dwq, dwo, dwu, dwd = pl.pallas_call(
            grad_kernel,
            name='weight_grads',
            out_shape=(sds((ROWS, D), BF16), sds((ROWS, D), BF16)) + (sds((D,), F32),) * 6 + (
                sds((3, NH, HD), F32), sds((FF,), F32), sds((QKV, D), BF16), sds((CTX, D), BF16), sds((D, FF), BF16), sds((FF, D), BF16)),
            in_specs=[any_spec] * 7,
            out_specs=(any_spec,) * 14,
            scratch_shapes=[
                pltpu.VMEM((LROWS, SEQ), BF16), pltpu.VMEM((4, SEQ, D), BF16), pltpu.VMEM((SLOTS, GR, D), BF16), pltpu.VMEM((SMALL, 320, D), BF16),
                pltpu.VMEM((ROWS, D), BF16), pltpu.VMEM((ROWS, D), BF16), pltpu.VMEM((TP, 4, D), F32), pltpu.VMEM((TP, 2, D), F32),
                pltpu.VMEM((6, 1, D), F32), pltpu.VMEM((1, FF), F32),
                pltpu.VMEM((3, NH, HD), F32),
                pltpu.SemaphoreType.DMA((8,)), pltpu.SemaphoreType.DMA((SLOTS,)), pltpu.SemaphoreType.DMA((SMALL,)), pltpu.SemaphoreType.DMA((5,)), pltpu.SemaphoreType.DMA((10,)),
            ],
            compiler_params=pltpu.CompilerParams(vmem_limit_bytes=66_000_000),
            cost_estimate=pl.CostEstimate(flops=5_000_000_000, bytes_accessed=44_000_000, transcendentals=0),
        )(y, gx, pva, pvb, gbu, lmat, rmat)
        g_wqkv = jnp.transpose(dwq.reshape(NH, 3, HD, D), (3, 0, 1, 2))
        g_ln2g, g_ln2b, g_bo, g_bd, g_ln1g, g_ln1b = v0, v1, v2, v3, v4, v5
        return (y[None], gx[None], g_ln1g, g_ln1b, g_wqkv, jnp.transpose(gbq, (1, 0, 2)), dwo, g_bo,
                g_ln2g, g_ln2b, dwu, gbu, dwd, g_bd)

    row_spec = P('dp', 'tp', None)
    in_specs = (row_spec, P(), P(), P(None, 'tp', None, None), P('tp', None, None), P('tp', None), P(), P(), P(),
                P(None, 'tp'), P('tp'), P('tp', None), P(), row_spec)
    out_specs = (row_spec, row_spec, P('dp'), P('dp'), P('dp', 'tp', None, None), P(('dp', 'tp'), None, None),
                 P(('dp', 'tp'), None), P('dp'), P('dp'), P('dp'), P('dp', 'tp'), P(('dp', 'tp')), P(('dp', 'tp'), None), P('dp'))
    return jax.shard_map(local_step, mesh=mesh, in_specs=in_specs, out_specs=out_specs, check_vma=False)
```
